32 devices in a mesh: pairs: 1 (over z), ho: 4 (over y), tp: 8 (over x, core).
Axes of the slice: x: 4, y: 4, z: 1, core: 2. Of those that a mesh axis runs over, the one named last changes fastest.
The devices are a block of a 4x4x8 slice.
Arguments:
- prompt_a: bfloat16 [4, 512, 3072], P('pairs')
- prompt_b: bfloat16 [4, 512, 3072], P('pairs')
- first_a: bfloat16 [4, 3072], P(('pairs', 'ho'))
- first_b: bfloat16 [4, 3072], P(('pairs', 'ho'))
- w_qkv: bfloat16 [6, 3072, 8, 5, 128], P(None, None, 'tp')
- w_out: bfloat16 [6, 8, 3, 128, 3072], P(None, 'tp')
- w_gate: bfloat16 [6, 3072, 8192], P(None, None, 'tp')
- w_up: bfloat16 [6, 3072, 8192], P(None, None, 'tp')
- w_down: bfloat16 [6, 8192, 3072], P(None, 'tp')
- norm_attn: float32 [6, 3072], replicated
- norm_mlp: float32 [6, 3072], replicated
Outputs:
- output 1: bfloat16 [4, 512, 3072], P(('pairs', 'ho'))
- output 2: bfloat16 [4, 512, 3072], P(('pairs', 'ho'))
- output 3: float32 [4, 3072], P(('pairs', 'ho'))
- output 4: float32 [4, 3072], P(('pairs', 'ho'))
- output 5: bfloat16 [4, 6, 2, 513, 8, 128], P(('pairs', 'ho'), None, None, None, 'tp')
- output 6: bfloat16 [4, 6, 2, 513, 8, 128], P(('pairs', 'ho'), None, None, None, 'tp')
All inputs are finite; a program needn't handle non-finite values.
Results may differ from the reference program's by a relative error of at most 0.02.
Values are sent between devices in bfloat16 or wider.
A program may use at most 768 MiB of HBM per device.

```python
import jax
import jax.numpy as jnp
from jax import lax

HO_DEVICES = 4
TOKENS = 512
LAYERS = 6
MODEL_DIM = 3072
HEADS = 24
KV_HEADS = 8
HEAD_DIM = 128
FFN_DIM = 8192

GROUP_SIZE = HEADS // KV_HEADS


def setup_inputs(seed: int = 0, part: int = 0) -> dict:
    part_keys = jax.random.split(jax.random.fold_in(jax.random.key(seed), part), 6)
    shared_keys = jax.random.split(jax.random.key(seed + 1), 7)

    def draw_prompt(key_common, key_noise):
        common = jax.random.normal(key_common, (HO_DEVICES, 1, MODEL_DIM), jnp.float32)
        noise_part = jax.random.normal(key_noise, (HO_DEVICES, TOKENS, MODEL_DIM), jnp.float32)
        return (common + noise_part).astype(jnp.bfloat16)

    def draw_weight(rng_key, arr_dims, fan_in):
        return (jax.random.normal(rng_key, arr_dims, jnp.float32) * fan_in ** -0.5).astype(jnp.bfloat16)

    return {
        'prompt_a': draw_prompt(part_keys[0], part_keys[1]),
        'prompt_b': draw_prompt(part_keys[2], part_keys[3]),
        'first_a': jax.random.normal(part_keys[4], (HO_DEVICES, MODEL_DIM), jnp.float32).astype(jnp.bfloat16),
        'first_b': jax.random.normal(part_keys[5], (HO_DEVICES, MODEL_DIM), jnp.float32).astype(jnp.bfloat16),
        'w_qkv': draw_weight(shared_keys[0], (LAYERS, MODEL_DIM, KV_HEADS, GROUP_SIZE + 2, HEAD_DIM), MODEL_DIM),
        'w_out': draw_weight(shared_keys[1], (LAYERS, KV_HEADS, GROUP_SIZE, HEAD_DIM, MODEL_DIM), HEADS * HEAD_DIM),
        'w_gate': draw_weight(shared_keys[2], (LAYERS, MODEL_DIM, FFN_DIM), MODEL_DIM),
        'w_up': draw_weight(shared_keys[3], (LAYERS, MODEL_DIM, FFN_DIM), MODEL_DIM),
        'w_down': draw_weight(shared_keys[4], (LAYERS, FFN_DIM, MODEL_DIM), FFN_DIM),
        'norm_attn': jax.random.uniform(shared_keys[5], (LAYERS, MODEL_DIM), jnp.float32, 0.5, 1.5),
        'norm_mlp': jax.random.uniform(shared_keys[6], (LAYERS, MODEL_DIM), jnp.float32, 0.5, 1.5),
    }


def rms_norm(hidden, gain_vec):
    hidden_f = hidden.astype(jnp.float32)
    inv_rms = lax.rsqrt(jnp.mean(hidden_f * hidden_f, axis=-1, keepdims=True) + 1e-5)
    return (hidden_f * inv_rms * gain_vec).astype(jnp.bfloat16)


def causal_attention(q_heads, key_rows, value_rows):
    positions = jnp.arange(TOKENS)
    allowed = positions[:, None] >= positions[None, :]

    def one_group(operands):
        q_group, k_group, v_group = operands
        scores = jnp.einsum('tgc,sc->gts', q_group.astype(jnp.float32), k_group.astype(jnp.float32)) * HEAD_DIM ** -0.5
        scores = jnp.where(allowed, scores, -1e30)
        attn_probs = jax.nn.softmax(scores, axis=-1).astype(jnp.bfloat16)
        mixed_out = jnp.einsum('gts,sc->tgc', attn_probs.astype(jnp.float32), v_group.astype(jnp.float32))
        return mixed_out.astype(jnp.bfloat16)

    mixed_out = lax.map(one_group, (jnp.moveaxis(q_heads, 1, 0), jnp.moveaxis(key_rows, 1, 0), jnp.moveaxis(value_rows, 1, 0)))
    return jnp.moveaxis(mixed_out, 0, 1)


def prefill_layer(hidden, layer_weights):
    w_qkv, w_out, w_gate, w_up, w_down, gain_attn, gain_mlp = layer_weights
    normed = rms_norm(hidden, gain_attn)
    qkv_out = jnp.dot(normed, w_qkv.reshape(MODEL_DIM, -1), preferred_element_type=jnp.float32)
    qkv_out = qkv_out.astype(jnp.bfloat16).reshape(TOKENS, KV_HEADS, GROUP_SIZE + 2, HEAD_DIM)
    key_rows = qkv_out[:, :, GROUP_SIZE]
    value_rows = qkv_out[:, :, GROUP_SIZE + 1]
    mixed_out = causal_attention(qkv_out[:, :, :GROUP_SIZE], key_rows, value_rows)
    attn_out = jnp.dot(mixed_out.reshape(TOKENS, -1), w_out.reshape(-1, MODEL_DIM), preferred_element_type=jnp.float32)
    hidden = (hidden.astype(jnp.float32) + attn_out.astype(jnp.bfloat16).astype(jnp.float32)).astype(jnp.bfloat16)
    normed = rms_norm(hidden, gain_mlp)
    gate_pre = jnp.dot(normed, w_gate, preferred_element_type=jnp.float32)
    up_val = jnp.dot(normed, w_up, preferred_element_type=jnp.float32)
    act_out = (jax.nn.silu(gate_pre) * up_val).astype(jnp.bfloat16)
    mlp_out = jnp.dot(act_out, w_down, preferred_element_type=jnp.float32)
    hidden = (hidden.astype(jnp.float32) + mlp_out.astype(jnp.bfloat16).astype(jnp.float32)).astype(jnp.bfloat16)
    return hidden, jnp.stack([key_rows, value_rows])


def decode_layer(dec_state, layer_inputs):
    w_qkv, w_out, w_gate, w_up, w_down, gain_attn, gain_mlp, kv_layer = layer_inputs
    normed = rms_norm(dec_state, gain_attn)
    qkv_out = jnp.dot(normed[None], w_qkv.reshape(MODEL_DIM, -1), preferred_element_type=jnp.float32)
    qkv_out = qkv_out.astype(jnp.bfloat16).reshape(KV_HEADS, GROUP_SIZE + 2, HEAD_DIM)
    new_kv = jnp.moveaxis(qkv_out[:, GROUP_SIZE:], 1, 0)[:, None]
    full_kv = jnp.concatenate([kv_layer, new_kv], axis=1)
    scores = jnp.einsum('kgc,skc->kgs', qkv_out[:, :GROUP_SIZE].astype(jnp.float32), full_kv[0].astype(jnp.float32)) * HEAD_DIM ** -0.5
    attn_probs = jax.nn.softmax(scores, axis=-1).astype(jnp.bfloat16)
    mixed_out = jnp.einsum('kgs,skc->kgc', attn_probs.astype(jnp.float32), full_kv[1].astype(jnp.float32)).astype(jnp.bfloat16)
    dec_state = dec_state + jnp.dot(mixed_out.reshape(1, -1), w_out.reshape(-1, MODEL_DIM), preferred_element_type=jnp.float32)[0]
    normed = rms_norm(dec_state, gain_mlp)
    gate_pre = jnp.dot(normed[None], w_gate, preferred_element_type=jnp.float32)
    up_val = jnp.dot(normed[None], w_up, preferred_element_type=jnp.float32)
    act_out = (jax.nn.silu(gate_pre) * up_val).astype(jnp.bfloat16)
    dec_state = dec_state + jnp.dot(act_out, w_down, preferred_element_type=jnp.float32)[0]
    return dec_state, full_kv


def reference(prompt_a, prompt_b, first_a, first_b, w_qkv, w_out, w_gate, w_up, w_down, norm_attn, norm_mlp):
    weights = (w_qkv, w_out, w_gate, w_up, w_down, norm_attn, norm_mlp)

    def prefill(prompt):
        return lax.scan(prefill_layer, prompt, weights)

    def decode(operands):
        first_tok, kv_rows = operands
        return lax.scan(decode_layer, first_tok.astype(jnp.float32), weights + (kv_rows,))

    out_a, kv_a = lax.map(prefill, prompt_a)
    out_b, kv_b = lax.map(prefill, prompt_b)
    final_a, cache_a = lax.map(decode, (first_a, jnp.roll(kv_a, 1, axis=0)))
    final_b, cache_b = lax.map(decode, (first_b, jnp.roll(kv_b, 1, axis=0)))
    return out_a, out_b, final_a, final_b, cache_a, cache_b
```

```python
import functools

import jax
import jax.numpy as jnp
from jax import lax
from jax.experimental import pallas as pl
from jax.experimental.pallas import tpu as pltpu
from jax.sharding import PartitionSpec as P

MESH = pl.DeviceIdType.MESH
F32 = jnp.float32
BF16 = jnp.bfloat16
CORES = 2
CHIPS = 4
STREAMS = 4
DEC = 16
PAD = 128


def tile_of(size, most):
    tile = most
    while size % tile:
        tile //= 2
    return tile


def body(cfg, pa, pb, y0, wq, wo, wg, wu, wd, g1, g2, oa, ob, fin, ca, cb,
         H, PB, PR, AR, BC, XR, QS, KV, OS, US, KVR, WQ, WO, WG, WU, WD, DY, DP, DS, DR, DG,
         s_prs, s_prr, s_as, s_ar, s_bs, s_br, s_cs, s_cr, s_gs, s_gr, s_rs, s_rr, s_ds, s_dr,
         s_kvs, s_kvr, s_wa, s_wm, s_in, s_out, s_ko, s_e1s, s_e1r, s_e2s, s_e2r, s_fin):
    n_ho, n_tp, L, T, D, G, hd, F = cfg
    TS = T // 2
    NB = n_tp
    BR = TS // NB
    DH = D // 2
    NS = 8 * L
    SL = D // n_tp
    NQ = SL // hd
    scale = hd ** -0.5
    j = lax.axis_index('ho')
    tp = lax.axis_index('tp')
    X = lax.div(tp, CORES)
    c = lax.rem(tp, CORES)
    R = lax.rem(X + 1, CHIPS)
    O = lax.rem(X + 2, CHIPS)
    Lf = lax.rem(X + 3, CHIPS)
    to_right = {'tp': R * CORES + c}
    to_left = {'tp': Lf * CORES + c}
    to_partner = {'tp': X * CORES + (1 - c)}
    ho_right = lax.rem(j + 1, n_ho)
    ho_left = lax.rem(j + n_ho - 1, n_ho)

    def rc(src, dst, ss, rs, dev):
        return pltpu.make_async_remote_copy(src_ref=src, dst_ref=dst, send_sem=ss, recv_sem=rs,
                                            device_id=dev, device_id_type=MESH)

    def lc(src, dst, sem):
        return pltpu.make_async_copy(src, dst, sem)

    def own_rows(Y):
        return pl.ds(pl.multiple_of((Y * CORES + c) * BR, BR), BR)

    def d_pr(par, h):
        return rc(PB.at[par, h, :, 1 - c], PR.at[par, h], s_prs.at[par, h], s_prr.at[par, h], to_partner)

    def d_a(par, d):
        return rc(PB.at[par, d, O, c], AR.at[par, d], s_as.at[par, d], s_ar.at[par, d], to_left if d else to_right)

    def d_b(par, d):
        return rc(PB.at[par, 1 - d, Lf if d else R, c], BC.at[par, d, 1 - d], s_bs.at[par, d], s_br.at[par, d],
                  to_left if d else to_right)

    def d_c(par, d):
        return rc(PB.at[par, d, Lf if d else R, c], BC.at[par, d, d], s_cs.at[par, d], s_cr.at[par, d],
                  to_left if d else to_right)

    def h_part(s, Y, half):
        return H.at[s, own_rows(Y), pl.ds(half * DH, DH)]

    def d_g(s, par, d, half):
        return rc(h_part(s, X, half), h_part(s, X, half), s_gs.at[par, d, half], s_gr.at[par, d, half],
                  to_left if d else to_right)

    def d_r(s, par, d):
        Y = R if d else Lf
        return rc(h_part(s, Y, d), h_part(s, Y, d), s_rs.at[par, d], s_rr.at[par, d], to_left if d else to_right)

    def d_d(s, Y):
        return rc(H.at[s, own_rows(Y)], H.at[s, own_rows(Y)], s_ds.at[s], s_dr.at[s], to_partner)

    def d_d_all(s):
        return rc(H.at[s, pl.ds(0, CHIPS * BR)], H.at[s, pl.ds(0, CHIPS * BR)], s_ds.at[s], s_dr.at[s], to_partner)

    def d_kv(l, pr):
        return rc(KV.at[pr], KVR.at[l, pr, :, pl.ds(0, T)], s_kvs.at[pr], s_kvr.at[l, pr], {'ho': ho_right})

    def wa_copies(l):
        out = [lc(wq.at[l, i], WQ.at[:, pl.ds(i * hd, hd)], s_wa.at[i]) for i in range(G + 2)]
        return out + [lc(wo.at[l], WO, s_wa.at[G + 2])]

    def wm_copies(l):
        return [lc(wg.at[l], WG, s_wm.at[0]), lc(wu.at[l], WU, s_wm.at[1]), lc(wd.at[l], WD, s_wm.at[2])]

    def prompt_copy(s):
        src = pa if s < 2 else pb
        return lc(src.at[j, pl.ds((s % 2) * TS, TS)], H.at[s, pl.ds(0, TS)], s_in.at[s])

    barrier = pltpu.get_barrier_semaphore()
    for k in range(1, n_tp):
        pl.semaphore_signal(barrier, inc=1, device_id={'tp': lax.rem(tp + k, n_tp)}, device_id_type=MESH)
    for k in (ho_right, ho_left):
        pl.semaphore_signal(barrier, inc=1, device_id={'ho': k}, device_id_type=MESH)

    prompt_copy(0).start()
    for w in wa_copies(0):
        w.start()
    for s in range(1, STREAMS):
        prompt_copy(s).start()
    for w in wm_copies(0):
        w.start()
    KV[...] = jnp.zeros(KV.shape, BF16)
    for s in range(STREAMS):
        H[s, TS:TS + DEC, :] = jnp.zeros((DEC, D), BF16)

    def zero_kvr(l, _):
        for pr in range(2):
            for kv in range(2):
                KVR[l, pr, kv, T:T + PAD, :] = jnp.zeros((PAD, hd), BF16)
        return 0

    lax.fori_loop(0, L, zero_kvr, 0)

    def normed(xf, gain):
        ms = jnp.mean(xf * xf, axis=-1, keepdims=True)
        return xf * lax.rsqrt(ms + 1e-5) * gain

    def decode_norm(gain):
        h = normed(DY[...], gain)
        H[STREAMS - 1, TS:TS + DEC, :] = jnp.concatenate([h, jnp.zeros_like(h)], axis=0).astype(BF16)

    DY[...] = y0[...]
    decode_norm(g1[0:1, :])
    pl.semaphore_wait(barrier, n_tp - 1 + 2)

    def slot(it, _):
        n = it - 1
        m1, m2, m3, mc = n - 1, n - 2, n - 3, n + 1
        live_n = jnp.logical_and(n >= 0, n < NS)
        live_1 = jnp.logical_and(m1 >= 0, m1 < NS)
        live_2 = jnp.logical_and(m2 >= 0, m2 < NS)
        live_3 = jnp.logical_and(m3 >= 0, m3 < NS)
        live_c = mc < NS
        par_n = lax.rem(n + 8, 2)
        par_1 = lax.rem(m1 + 8, 2)

        @pl.when(live_n)
        def _():
            par = par_n
            for h in range(2):
                d_pr(par, h).wait_recv()

            def add(h, Y):
                PB[par, h, Y, c] = PB[par, h, Y, c] + PR[par, h, Y]

            add(0, O)
            add(1, O)
            add(1, R)
            add(0, Lf)
            for d in range(2):
                d_a(par, d).start()
            for d in range(2):
                d_b(par, d).start()
            add(0, R)
            add(1, Lf)
            add(0, X)
            add(1, X)

        @pl.when(live_1)
        def _():
            par = par_1
            s = lax.rem(m1, STREAMS)
            l = lax.div(m1, 8)
            is_attn = lax.rem(lax.div(m1, 4), 2) == 0
            last = m1 >= NS - STREAMS
            for d in range(2):
                d_b(par, d).wait_recv()
            for d in range(2):
                d_c(par, d).wait_recv()
            x_new = []
            ms = jnp.zeros((BR, 1), F32)
            for h in range(2):
                total = PB[par, h, X, c].astype(F32) + (BC[par, 0, h].astype(F32) + BC[par, 1, h].astype(F32))
                x = XR[s, :, h * DH:(h + 1) * DH].astype(F32) + total.astype(BF16).astype(F32)
                x = x.astype(BF16)
                XR[s, :, h * DH:(h + 1) * DH] = x
                x = x.astype(F32)
                ms = ms + jnp.sum(x * x, axis=-1, keepdims=True)
                x_new.append(x)
            inv = lax.rsqrt(ms * (1.0 / D) + 1e-5)
            nl = jnp.minimum(l + 1, L - 1)
            for h in range(2):
                cols = slice(h * DH, (h + 1) * DH)
                gain = jnp.where(is_attn, g2[pl.ds(l, 1), cols], g1[pl.ds(nl, 1), cols])
                hn = x_new[h] * inv * gain
                H[s, own_rows(X), cols] = jnp.where(last, x_new[h], hn).astype(BF16)
            for half in range(2):
                for d in range(2):
                    d_g(s, par, d, half if d == 0 else 1 - half).start()
            d_d(s, X).start()

        @pl.when(live_1)
        def _():
            for h in range(2):
                d_pr(par_1, h).wait_send()
            for d in range(2):
                d_a(par_1, d).wait_send()
                d_b(par_1, d).wait_send()
                d_c(par_1, d).wait_send()

        @pl.when(live_2)
        def _():
            par = lax.rem(m2, 2)
            s = lax.rem(m2, STREAMS)
            d_g(s, par, 0, 1).wait_recv()
            d_d(s, Lf).start()
            d_g(s, par, 1, 0).wait_recv()
            d_d(s, R).start()
            for d in range(2):
                d_r(s, par, d).wait_recv()
            d_d(s, O).start()
            for d in range(2):
                for half in range(2):
                    d_g(s, par, d, half).wait_send()
                d_r(s, par, d).wait_send()

        @pl.when(live_3)
        def _():
            s = lax.rem(m3, STREAMS)
            d_d_all(s).wait_recv()
            d_d_all(s).wait_send()

        for s in range(STREAMS):
            @pl.when(m3 == NS - STREAMS + s)
            def _():
                lc(H.at[s, pl.ds(0, TS)], (oa if s < 2 else ob).at[pl.ds((s % 2) * TS, TS)], s_out.at[s]).start()

        r8 = lax.rem(mc, 8)

        @pl.when(jnp.logical_or(r8 == 5, jnp.logical_and(r8 == 0, mc > 0)))
        def _():
            rc(DS.at[pl.ds(0, n_tp - 1)], DR.at[pl.ds(0, n_tp - 1)], s_e1s, s_e1r, to_partner).wait_recv()
            rc(DS.at[pl.ds(0, n_tp - 1)], DR.at[pl.ds(0, n_tp - 1)], s_e1s, s_e1r, to_partner).wait_send()
            acc = DR[0]
            for k in range(1, n_tp):
                acc = acc + DR[k]
            DG[tp] = acc
            for k in range(1, n_tp):
                rc(DG.at[tp], DG.at[tp], s_e2s, s_e2r, {'tp': lax.rem(tp + k, n_tp)}).start()

        @pl.when(jnp.logical_or(r8 == 6, jnp.logical_and(r8 == 1, mc > 8)))
        def _():
            rc(DG.at[pl.ds(0, n_tp - 1)], DG.at[pl.ds(0, n_tp - 1)], s_e2s, s_e2r, to_partner).wait_recv()
            rc(DG.at[pl.ds(0, n_tp - 1)], DG.at[pl.ds(0, n_tp - 1)], s_e2s, s_e2r, to_partner).wait_send()
            rows = lax.broadcasted_iota(jnp.int32, (8, hd), 0)
            for k in range(n_tp):
                block = DG[k]
                for q in range(NQ):
                    part = block if q == 0 else pltpu.roll(block, 8 - 2 * q, axis=0)
                    cols = slice(k * SL + q * hd, k * SL + (q + 1) * hd)
                    DY[:, cols] = DY[:, cols] + jnp.where(rows < 2, part, 0.0)
            lq = lax.div(mc, 8)

            @pl.when(r8 == 6)
            def _():
                decode_norm(g2[pl.ds(lq, 1), :])

            @pl.when(jnp.logical_and(r8 == 1, mc < NS))
            def _():
                decode_norm(g1[pl.ds(jnp.minimum(lq, L - 1), 1), :])

        def decode_send():
            for k in range(n_tp):
                acc = DP[:, k * SL:k * SL + hd]
                for q in range(1, NQ):
                    acc = acc + pltpu.roll(DP[:, k * SL + q * hd:k * SL + (q + 1) * hd], 2 * q, axis=0)
                DS[k] = acc
            DR[tp] = DS[tp]
            for k in range(1, n_tp):
                to = lax.rem(tp + k, n_tp)
                rc(DS.at[to], DR.at[tp], s_e1s, s_e1r, {'tp': to}).start()

        par_c = lax.rem(mc, 2)
        sc = lax.rem(mc, STREAMS)
        lc_ = jnp.minimum(lax.div(mc, 8), L - 1)
        attn_c = jnp.logical_and(live_c, r8 < 4)
        mlp_c = jnp.logical_and(live_c, r8 >= 4)
        hi = lax.rem(sc, 2)
        pr_c = lax.div(sc, 2)

        for s in range(STREAMS):
            @pl.when(mc == s)
            def _():
                prompt_copy(s).wait()

                def first_rows(i, _):
                    rows = pl.ds(pl.multiple_of(i * BR, BR), BR)
                    hn = normed(H[s, rows, :].astype(F32), g1[0:1, :])
                    H[s, rows, :] = hn.astype(BF16)
                    return 0

                XR[s] = H[s, own_rows(X), :]
                lax.fori_loop(0, NB, first_rows, 0)

        @pl.when(attn_c)
        def _():
            @pl.when(sc == 0)
            def _():
                for w in wa_copies(lc_):
                    w.wait()

            c0 = 0
            while c0 < (G + 2) * hd:
                c1 = min(c0 + 2 * hd, (G + 2) * hd)
                QS[:, c0:c1] = jnp.dot(H[sc], WQ[:, c0:c1], preferred_element_type=F32).astype(BF16)
                c0 = c1
            rows = pl.ds(pl.multiple_of(hi * TS, TS), TS)
            for kv in range(2):
                KV[pr_c, kv, rows, :] = QS[0:TS, (G + kv) * hd:(G + kv + 1) * hd]

            @pl.when(hi == 1)
            def _():
                d_kv(lc_, pr_c).start()

            RT = tile_of(TS, 128)

            def attn_tile(i, _):
                g = lax.div(i, TS // RT)
                r = lax.rem(i, TS // RT)
                rows = pl.ds(pl.multiple_of(r * RT, RT), RT)
                cols = pl.ds(pl.multiple_of(g * hd, hd), hd)
                q = QS[rows, cols]
                scores = lax.dot_general(q, KV[pr_c, 0], (((1,), (1,)), ((), ())), preferred_element_type=F32) * scale
                qpos = hi * TS + r * RT + lax.broadcasted_iota(jnp.int32, (RT, T), 0)
                kpos = lax.broadcasted_iota(jnp.int32, (RT, T), 1)
                scores = jnp.where(qpos >= kpos, scores, -1e30)
                e = jnp.exp(scores - jnp.max(scores, axis=-1, keepdims=True))
                p = (e / jnp.sum(e, axis=-1, keepdims=True)).astype(BF16)
                OS[rows, cols] = jnp.dot(p, KV[pr_c, 1], preferred_element_type=F32).astype(BF16)
                return 0

            lax.fori_loop(0, G * (TS // RT), attn_tile, 0)

        UT = tile_of(F, 256)

        @pl.when(mlp_c)
        def _():
            @pl.when(sc == 0)
            def _():
                for w in wm_copies(lc_):
                    w.wait()

            def gate_up(i, _):
                cols = pl.ds(pl.multiple_of(i * UT, UT), UT)
                gate = jnp.dot(H[sc], WG[:, cols], preferred_element_type=F32)
                up = jnp.dot(H[sc], WU[:, cols], preferred_element_type=F32)
                US[:, cols] = (gate * (1.0 / (1.0 + jnp.exp(-gate))) * up).astype(BF16)
                return 0

            lax.fori_loop(0, F // UT, gate_up, 0)

        @pl.when(live_n)
        def _():
            for d in range(2):
                d_a(par_n, d).wait_recv()
                Y = Lf if d else R
                PB[par_n, d, Y, c] = PB[par_n, d, Y, c] + AR[par_n, d]
                d_c(par_n, d).start()

        NT = tile_of(DH, 512)

        def put(h, t, val):
            PB[par_c, h, :, :, :, pl.ds(pl.multiple_of(t * NT, NT), NT)] = (
                val[0:TS].astype(BF16).reshape(CHIPS, CORES, BR, NT))

        @pl.when(attn_c)
        def _():
            for h in range(2):
                def out_tile(t, _):
                    cols = pl.ds(pl.multiple_of(h * DH + t * NT, NT), NT)
                    put(h, t, jnp.dot(OS[...], WO[:, cols], preferred_element_type=F32))
                    return 0

                lax.fori_loop(0, DH // NT, out_tile, 0)
                d_pr(par_c, h).start()

        @pl.when(mlp_c)
        def _():
            for h in range(2):
                def down_tile(t, _):
                    cols = pl.ds(pl.multiple_of(h * DH + t * NT, NT), NT)
                    val = jnp.dot(US[...], WD[:, cols], preferred_element_type=F32)
                    put(h, t, val)
                    DP[:, cols] = val[TS:TS + 8]
                    return 0

                lax.fori_loop(0, DH // NT, down_tile, 0)
                d_pr(par_c, h).start()

        @pl.when(live_1)
        def _():
            s = lax.rem(m1, STREAMS)
            d_g(s, par_1, 0, 0).wait_recv()
            d_r(s, par_1, 0).start()
            d_g(s, par_1, 1, 1).wait_recv()
            d_r(s, par_1, 1).start()

        @pl.when(jnp.logical_and(live_c, r8 == 4))
        def _():
            for pr in range(2):
                d_kv(lc_, pr).wait_send()
            for pr in range(2):
                d_kv(lc_, pr).wait_recv()
            rows = lax.broadcasted_iota(jnp.int32, (DEC, hd), 0)
            outs = []
            for pr in range(2):
                for kv in range(2):
                    new = QS[TS:TS + DEC, (G + kv) * hd:(G + kv + 1) * hd].astype(F32)
                    new = jnp.sum(jnp.where(rows == pr, new, 0.0), axis=0, keepdims=True)
                    KVR[lc_, pr, kv, T:T + DEC, :] = jnp.where(rows == 0, new, 0.0).astype(BF16)
                q = jnp.concatenate([QS[TS:TS + DEC, g * hd:(g + 1) * hd] for g in range(G)], axis=0)
                scores = lax.dot_general(q, KVR[lc_, pr, 0], (((1,), (1,)), ((), ())), preferred_element_type=F32) * scale
                kpos = lax.broadcasted_iota(jnp.int32, (G * DEC, T + PAD), 1)
                scores = jnp.where(kpos <= T, scores, -1e30)
                e = jnp.exp(scores - jnp.max(scores, axis=-1, keepdims=True))
                p = (e / jnp.sum(e, axis=-1, keepdims=True)).astype(BF16)
                outs.append(jnp.dot(p, KVR[lc_, pr, 1], preferred_element_type=F32))
            picked = []
            for g in range(G):
                rest = jnp.where(rows == 1, outs[1][g * DEC:(g + 1) * DEC], 0.0)
                picked.append(jnp.where(rows == 0, outs[0][g * DEC:(g + 1) * DEC], rest).astype(BF16))
            od = jnp.concatenate(picked, axis=1)

            for t in range(D // NT):
                part = jnp.dot(od, WO[:, t * NT:(t + 1) * NT], preferred_element_type=F32)
                DP[:, t * NT:(t + 1) * NT] = part[0:8]
            decode_send()
            for pr in range(2):
                lc(KVR.at[lc_, pr, :, pl.ds(0, T + DEC)], (cb if pr else ca).at[lc_], s_ko.at[pr]).start()

            @pl.when(lax.div(mc, 8) + 1 < L)
            def _():
                for w in wa_copies(lax.div(mc, 8) + 1):
                    w.start()

        @pl.when(jnp.logical_and(live_c, r8 == 7))
        def _():
            decode_send()

            @pl.when(lax.div(mc, 8) + 1 < L)
            def _():
                for w in wm_copies(lax.div(mc, 8) + 1):
                    w.start()

        return 0

    lax.fori_loop(0, NS + 4, slot, 0)

    lc(DY, fin, s_fin).start()
    lc(DY, fin, s_fin).wait()
    for pr in range(2):
        lc(KVR.at[:, pr, :, pl.ds(0, T + DEC)], cb if pr else ca, s_ko.at[pr]).wait()
    for s in range(STREAMS):
        lc(H.at[s, pl.ds(0, TS)], (oa if s < 2 else ob).at[pl.ds((s % 2) * TS, TS)], s_out.at[s]).wait()


def device_specs():
    row_axes = ('pairs', 'ho')
    in_specs = (P('pairs', None, None), P('pairs', None, None), P(row_axes, None), P(row_axes, None),
                P(None, None, 'tp', None, None), P(None, 'tp', None, None, None), P(None, None, 'tp'),
                P(None, None, 'tp'), P(None, 'tp', None), P(None, None), P(None, None))
    out_specs = (P(row_axes, None, None), P(row_axes, None, None), P(row_axes, None), P(row_axes, None),
                 P(row_axes, None, None, None, 'tp', None), P(row_axes, None, None, None, 'tp', None))
    return in_specs, out_specs


def solution(mesh):
    n_ho, n_tp = mesh.shape['ho'], mesh.shape['tp']
    in_specs, out_specs = device_specs()

    def per_device(prompt_a, prompt_b, first_a, first_b, w_qkv, w_out, w_gate, w_up, w_down, norm_attn, norm_mlp):
        L, D = w_qkv.shape[0], w_qkv.shape[1]
        G, hd = w_out.shape[2], w_out.shape[3]
        F = w_gate.shape[2]
        T = prompt_a.shape[1]
        TS, DH = T // 2, D // 2
        BR = TS // n_tp
        wq = jnp.transpose(w_qkv[:, :, 0], (0, 2, 1, 3))
        wo = w_out.reshape(L, G * hd, D)
        y0 = jnp.concatenate([first_a, first_b, jnp.zeros((6, D), first_a.dtype)], axis=0).astype(F32)
        any_spec = pl.BlockSpec(memory_space=pl.ANY)
        vmem_spec = pl.BlockSpec(memory_space=pltpu.VMEM)
        dma = pltpu.SemaphoreType.DMA
        flops = 2 * L * 2 * T * D * (wq.shape[1] * hd + G * hd + 3 * F)
        outs = pl.pallas_call(
            functools.partial(body, (n_ho, n_tp, L, T, D, G, hd, F)),
            name='serve',
            out_shape=(
                jax.ShapeDtypeStruct((T, D), BF16), jax.ShapeDtypeStruct((T, D), BF16),
                jax.ShapeDtypeStruct((8, D), F32),
                jax.ShapeDtypeStruct((L, 2, T + DEC, hd), BF16), jax.ShapeDtypeStruct((L, 2, T + DEC, hd), BF16)),
            in_specs=[any_spec, any_spec, vmem_spec] + [any_spec] * 5 + [vmem_spec, vmem_spec],
            out_specs=(any_spec,) * 5,
            scratch_shapes=[
                pltpu.VMEM((STREAMS, TS + DEC, D), BF16),
                pltpu.VMEM((2, 2, CHIPS, CORES, BR, DH), BF16),
                pltpu.VMEM((2, 2, CHIPS, BR, DH), BF16),
                pltpu.VMEM((2, 2, BR, DH), BF16),
                pltpu.VMEM((2, 2, 2, BR, DH), BF16),
                pltpu.VMEM((STREAMS, BR, D), BF16),
                pltpu.VMEM((TS + DEC, (G + 2) * hd), BF16),
                pltpu.VMEM((2, 2, T, hd), BF16),
                pltpu.VMEM((TS, G * hd), BF16),
                pltpu.VMEM((TS + DEC, F), BF16),
                pltpu.VMEM((L, 2, 2, T + PAD, hd), BF16),
                pltpu.VMEM((D, (G + 2) * hd), BF16),
                pltpu.VMEM((G * hd, D), BF16),
                pltpu.VMEM((D, F), BF16),
                pltpu.VMEM((D, F), BF16),
                pltpu.VMEM((F, D), BF16),
                pltpu.VMEM((8, D), F32),
                pltpu.VMEM((8, D), F32),
                pltpu.VMEM((n_tp, 8, hd), F32),
                pltpu.VMEM((n_tp, 8, hd), F32),
                pltpu.VMEM((n_tp, 8, hd), F32),
                dma((2, 2)), dma((2, 2)),
                dma((2, 2)), dma((2, 2)),
                dma((2, 2)), dma((2, 2)),
                dma((2, 2)), dma((2, 2)),
                dma((2, 2, 2)), dma((2, 2, 2)),
                dma((2, 2)), dma((2, 2)),
                dma((STREAMS,)), dma((STREAMS,)),
                dma((2,)), dma((L, 2)),
                dma((G + 3,)), dma((3,)), dma((STREAMS,)), dma((STREAMS,)), dma((2,)),
                dma, dma, dma, dma, dma,
            ],
            compiler_params=pltpu.CompilerParams(
                collective_id=0, has_side_effects=True, vmem_limit_bytes=60 * 1024 * 1024),
            cost_estimate=pl.CostEstimate(flops=flops, bytes_accessed=2 * L * D * (5 * hd + G * hd + 3 * F), transcendentals=0),
        )(prompt_a, prompt_b, y0, wq, wo, w_gate, w_up, w_down, norm_attn, norm_mlp)
        out_a, out_b, fin, cache_a, cache_b = outs

        def cache(rows):
            return rows[:, :, :T + 1, None, :][None]

        return (out_a[None], out_b[None], fin[0:1], fin[1:2], cache(cache_a), cache(cache_b))

    return jax.shard_map(per_device, mesh=mesh, in_specs=in_specs, out_specs=out_specs, check_vma=False)
```

```python
import functools

import jax
import jax.numpy as jnp
from jax import lax
from jax.experimental import pallas as pl
from jax.experimental.pallas import tpu as pltpu
from jax.sharding import PartitionSpec as P

MESH = pl.DeviceIdType.MESH
F32 = jnp.float32
BF16 = jnp.bfloat16
CORES = 2
CHIPS = 4
STREAMS = 4
DEC = 16
PAD = 128


def tile_of(size, most):
    tile = most
    while size % tile:
        tile //= 2
    return tile


def body(cfg, pa, pb, fa, fb, wq, wo, wg, wu, wd, g1, g2, oa, ob, fin_a, fin_b, ca, cb,
         H, PB, PR, AR, BC, XR, QS, KV, OS, US, KVR, WQ, WO, WG, WU, WD, DY, DP, EX, Z32, ZB,
         s_prs, s_prr, s_as, s_ar, s_bs, s_br, s_cs, s_cr, s_gs, s_gr, s_rs, s_rr, s_ds, s_dr,
         s_kvs, s_kvr, s_wa, s_wm, s_in, s_out, s_ko, s_es, s_er):
    n_ho, n_tp, L, T, D, G, hd, F = cfg
    TS = T // 2
    NB = n_tp
    BR = TS // NB
    DH = D // 2
    NS = 8 * L
    NT4 = EX.shape[1]
    scale = hd ** -0.5
    j = lax.axis_index('ho')
    tp = lax.axis_index('tp')
    X = lax.div(tp, CORES)
    c = lax.rem(tp, CORES)
    R = lax.rem(X + 1, CHIPS)
    O = lax.rem(X + 2, CHIPS)
    Lf = lax.rem(X + 3, CHIPS)
    to_right = {'tp': R * CORES + c}
    to_left = {'tp': Lf * CORES + c}
    to_partner = {'tp': X * CORES + (1 - c)}
    ho_right = lax.rem(j + 1, n_ho)
    ho_left = lax.rem(j + n_ho - 1, n_ho)

    def rc(src, dst, ss, rs, dev):
        return pltpu.make_async_remote_copy(src_ref=src, dst_ref=dst, send_sem=ss, recv_sem=rs,
                                            device_id=dev, device_id_type=MESH)

    def lc(src, dst, sem):
        return pltpu.make_async_copy(src, dst, sem)

    def own_rows(Y):
        return pl.ds(pl.multiple_of((Y * CORES + c) * BR, BR), BR)

    def d_pr(par, h):
        return rc(PB.at[par, h, :, 1 - c], PR.at[par, h], s_prs.at[par, h], s_prr.at[par, h], to_partner)

    def d_a(par, d):
        return rc(PB.at[par, d, O, c], AR.at[par, d], s_as.at[par, d], s_ar.at[par, d], to_left if d else to_right)

    def d_b(par, d):
        return rc(PB.at[par, 1 - d, Lf if d else R, c], BC.at[par, d, 1 - d], s_bs.at[par, d], s_br.at[par, d],
                  to_left if d else to_right)

    def d_c(par, d):
        return rc(PB.at[par, d, Lf if d else R, c], BC.at[par, d, d], s_cs.at[par, d], s_cr.at[par, d],
                  to_left if d else to_right)

    def h_part(s, Y, half):
        return H.at[s, own_rows(Y), pl.ds(half * DH, DH)]

    def d_g(s, par, d, half):
        return rc(h_part(s, X, half), h_part(s, X, half), s_gs.at[par, d, half], s_gr.at[par, d, half],
                  to_left if d else to_right)

    def d_r(s, par, d):
        Y = R if d else Lf
        return rc(h_part(s, Y, d), h_part(s, Y, d), s_rs.at[par, d], s_rr.at[par, d], to_left if d else to_right)

    def d_d(s, Y):
        return rc(H.at[s, own_rows(Y)], H.at[s, own_rows(Y)], s_ds.at[s], s_dr.at[s], to_partner)

    def d_d_all(s):
        return rc(H.at[s, pl.ds(0, CHIPS * BR)], H.at[s, pl.ds(0, CHIPS * BR)], s_ds.at[s], s_dr.at[s], to_partner)

    def d_kv(l, pr):
        return rc(KV.at[pr], KVR.at[l, pr, :, pl.ds(0, T)], s_kvs.at[pr], s_kvr.at[l, pr], {'ho': ho_right})

    first_pair = {'tp': (X + 1 - 2 * lax.rem(X, 2)) * CORES + c}
    second_pair = {'tp': (CHIPS - 1 - X) * CORES + c}
    E_OUT, E_IN0, E_A, E_IN1, E_B, E_IN2, E_C, E_IN3 = range(8)

    def d_e(step):
        src, dst, dev = ((E_OUT, E_IN0, to_partner), (E_A, E_IN1, first_pair), (E_B, E_IN2, second_pair),
                         (E_C, E_IN3, to_partner))[step]
        return rc(EX.at[src], EX.at[dst], s_es.at[step], s_er.at[step], dev)

    def cache_copy(l, pr):
        return lc(ZB.at[pr, pl.ds(0, T + 1)], (cb if pr else ca).at[pl.ds(l * (T + 1), T + 1)], s_ko.at[pr])

    def wa_copies(l):
        out = [lc(wq.at[l, i], WQ.at[:, pl.ds(i * hd, hd)], s_wa.at[i]) for i in range(G + 2)]
        return out + [lc(wo.at[l], WO, s_wa.at[G + 2])]

    def wm_copies(l):
        return [lc(wg.at[l], WG, s_wm.at[0]), lc(wu.at[l], WU, s_wm.at[1]), lc(wd.at[l], WD, s_wm.at[2])]

    def prompt_copy(s):
        src = pa if s < 2 else pb
        return lc(src.at[j, pl.ds((s % 2) * TS, TS)], H.at[s, pl.ds(0, TS)], s_in.at[s])

    barrier = pltpu.get_barrier_semaphore()
    for k in range(1, n_tp):
        pl.semaphore_signal(barrier, inc=1, device_id={'tp': lax.rem(tp + k, n_tp)}, device_id_type=MESH)
    for k in (ho_right, ho_left):
        pl.semaphore_signal(barrier, inc=1, device_id={'ho': k}, device_id_type=MESH)

    prompt_copy(0).start()
    for w in wa_copies(0):
        w.start()
    KV[...] = jnp.zeros(KV.shape, BF16)
    for s in range(STREAMS):
        H[s, TS:TS + DEC, :] = jnp.zeros((DEC, D), BF16)

    def zero_kvr(l, _):
        for pr in range(2):
            for kv in range(2):
                KVR[l, pr, kv, T:T + PAD, :] = jnp.zeros((PAD, hd), BF16)
        return 0

    lax.fori_loop(0, L, zero_kvr, 0)

    def normed(xf, gain):
        ms = jnp.mean(xf * xf, axis=-1, keepdims=True)
        return xf * lax.rsqrt(ms + 1e-5) * gain

    def decode_norm(gain):
        h = normed(DY[...], gain)
        H[STREAMS - 1, TS:TS + DEC, :] = jnp.concatenate([h, jnp.zeros_like(h)], axis=0).astype(BF16)

    DY[...] = jnp.zeros(DY.shape, F32)
    DY[0:1, :] = fa[...].astype(F32)
    DY[1:2, :] = fb[...].astype(F32)
    decode_norm(g1[0:1, :])
    pl.semaphore_wait(barrier, n_tp - 1 + 2)

    def slot(it, _):
        n = it - 1
        m1, m2, m3, mc = n - 1, n - 2, n - 3, n + 1
        live_n = jnp.logical_and(n >= 0, n < NS)
        live_1 = jnp.logical_and(m1 >= 0, m1 < NS)
        live_2 = jnp.logical_and(m2 >= 0, m2 < NS)
        live_3 = jnp.logical_and(m3 >= 0, m3 < NS)
        live_c = mc < NS
        par_n = lax.rem(n + 8, 2)
        par_1 = lax.rem(m1 + 8, 2)

        @pl.when(live_n)
        def _():
            par = par_n
            for h in range(2):
                d_pr(par, h).wait_recv()

            def add(h, Y):
                PB[par, h, Y, c] = PB[par, h, Y, c] + PR[par, h, Y]

            add(0, O)
            add(1, O)
            add(1, R)
            add(0, Lf)
            for d in range(2):
                d_a(par, d).start()
            for d in range(2):
                d_b(par, d).start()
            add(0, R)
            add(1, Lf)
            add(0, X)
            add(1, X)

        @pl.when(live_1)
        def _():
            par = par_1
            s = lax.rem(m1, STREAMS)
            l = lax.div(m1, 8)
            is_attn = lax.rem(lax.div(m1, 4), 2) == 0
            last = m1 >= NS - STREAMS
            for d in range(2):
                d_b(par, d).wait_recv()
            for d in range(2):
                d_c(par, d).wait_recv()
            x_new = []
            ms = jnp.zeros((BR, 1), F32)
            for h in range(2):
                total = PB[par, h, X, c].astype(F32) + (BC[par, 0, h].astype(F32) + BC[par, 1, h].astype(F32))
                x = XR[s, :, h * DH:(h + 1) * DH].astype(F32) + total.astype(BF16).astype(F32)
                x = x.astype(BF16)
                XR[s, :, h * DH:(h + 1) * DH] = x
                x = x.astype(F32)
                ms = ms + jnp.sum(x * x, axis=-1, keepdims=True)
                x_new.append(x)
            inv = lax.rsqrt(ms * (1.0 / D) + 1e-5)
            nl = jnp.minimum(l + 1, L - 1)
            for h in range(2):
                cols = slice(h * DH, (h + 1) * DH)
                gain = jnp.where(is_attn, g2[pl.ds(l, 1), cols], g1[pl.ds(nl, 1), cols])
                hn = x_new[h] * inv * gain
                H[s, own_rows(X), cols] = jnp.where(last, x_new[h], hn).astype(BF16)
            for half in range(2):
                for d in range(2):
                    d_g(s, par, d, half if d == 0 else 1 - half).start()
            d_d(s, X).start()

        @pl.when(live_1)
        def _():
            for h in range(2):
                d_pr(par_1, h).wait_send()
            for d in range(2):
                d_a(par_1, d).wait_send()
                d_b(par_1, d).wait_send()
                d_c(par_1, d).wait_send()

        @pl.when(live_2)
        def _():
            par = lax.rem(m2, 2)
            s = lax.rem(m2, STREAMS)
            d_g(s, par, 0, 1).wait_recv()
            d_d(s, Lf).start()
            d_g(s, par, 1, 0).wait_recv()
            d_d(s, R).start()
            for d in range(2):
                d_r(s, par, d).wait_recv()
            d_d(s, O).start()
            for d in range(2):
                for half in range(2):
                    d_g(s, par, d, half).wait_send()
                d_r(s, par, d).wait_send()

        @pl.when(live_3)
        def _():
            s = lax.rem(m3, STREAMS)
            d_d_all(s).wait_recv()
            d_d_all(s).wait_send()

        for s in range(STREAMS):
            @pl.when(m3 == NS - STREAMS + s)
            def _():
                lc(H.at[s, pl.ds(0, TS)], (oa if s < 2 else ob).at[pl.ds((s % 2) * TS, TS)], s_out.at[s]).start()

        r8 = lax.rem(mc, 8)
        rows8 = lax.broadcasted_iota(jnp.int32, (8, hd), 0)

        def half_cols(half, k):
            return pl.ds(pl.multiple_of(half * DH + k * hd, hd), hd)

        def decode_send():
            for slot_, half in ((E_OUT, 1 - c), (E_A, c)):
                for t in range(NT4):
                    acc = DP[:, half_cols(half, 4 * t)]
                    for q in range(1, 4):
                        acc = acc + pltpu.roll(DP[:, half_cols(half, 4 * t + q)], 2 * q, axis=0)
                    EX[slot_, t] = acc
            d_e(0).start()

        @pl.when(jnp.logical_or(r8 == 5, jnp.logical_and(r8 == 0, mc > 0)))
        def _():
            d_e(0).wait_recv()
            d_e(0).wait_send()
            EX[E_A] = EX[E_A] + EX[E_IN0]
            d_e(1).start()

        @pl.when(jnp.logical_or(r8 == 6, jnp.logical_and(r8 == 1, mc > 8)))
        def _():
            d_e(2).wait_recv()
            d_e(2).wait_send()
            EX[E_C] = EX[E_B] + EX[E_IN2]
            d_e(3).start()

        @pl.when(jnp.logical_or(r8 == 7, jnp.logical_and(r8 == 2, mc > 8)))
        def _():
            d_e(3).wait_recv()
            d_e(3).wait_send()
            for slot_, half in ((E_C, c), (E_IN3, 1 - c)):
                for t in range(NT4):
                    block = EX[slot_, t]
                    for q in range(4):
                        part = block if q == 0 else pltpu.roll(block, 8 - 2 * q, axis=0)
                        cols = half_cols(half, 4 * t + q)
                        DY[:, cols] = DY[:, cols] + jnp.where(rows8 < 2, part, 0.0)
            lq = lax.div(mc, 8)

            @pl.when(r8 == 7)
            def _():
                decode_norm(g2[pl.ds(lq, 1), :])

            @pl.when(jnp.logical_and(r8 == 2, mc < NS))
            def _():
                decode_norm(g1[pl.ds(jnp.minimum(lq, L - 1), 1), :])

        par_c = lax.rem(mc, 2)
        sc = lax.rem(mc, STREAMS)
        lc_ = jnp.minimum(lax.div(mc, 8), L - 1)
        attn_c = jnp.logical_and(live_c, r8 < 4)
        mlp_c = jnp.logical_and(live_c, r8 >= 4)
        hi = lax.rem(sc, 2)
        pr_c = lax.div(sc, 2)

        for s in range(STREAMS):
            @pl.when(mc == s)
            def _():
                prompt_copy(s).wait()

                def first_rows(i, _):
                    rows = pl.ds(pl.multiple_of(i * BR, BR), BR)
                    hn = normed(H[s, rows, :].astype(F32), g1[0:1, :])
                    H[s, rows, :] = hn.astype(BF16)
                    return 0

                XR[s] = H[s, own_rows(X), :]
                lax.fori_loop(0, NB, first_rows, 0)

        @pl.when(attn_c)
        def _():
            @pl.when(sc == 0)
            def _():
                for w in wa_copies(lc_):
                    w.wait()

                @pl.when(mc == 0)
                def _():
                    for s in range(1, STREAMS):
                        prompt_copy(s).start()
                    for w in wm_copies(0):
                        w.start()

            c0 = 0
            while c0 < (G + 2) * hd:
                c1 = min(c0 + 2 * hd, (G + 2) * hd)
                QS[:, c0:c1] = jnp.dot(H[sc], WQ[:, c0:c1], preferred_element_type=F32).astype(BF16)
                c0 = c1
            rows = pl.ds(pl.multiple_of(hi * TS, TS), TS)
            for kv in range(2):
                KV[pr_c, kv, rows, :] = QS[0:TS, (G + kv) * hd:(G + kv + 1) * hd]

            @pl.when(hi == 1)
            def _():
                d_kv(lc_, pr_c).start()

            RT = tile_of(TS, 128)

            def attn_tile(i, _):
                g = lax.div(i, TS // RT)
                r = lax.rem(i, TS // RT)
                rows = pl.ds(pl.multiple_of(r * RT, RT), RT)
                cols = pl.ds(pl.multiple_of(g * hd, hd), hd)
                q = QS[rows, cols]
                scores = lax.dot_general(q, KV[pr_c, 0], (((1,), (1,)), ((), ())), preferred_element_type=F32) * scale
                qpos = hi * TS + r * RT + lax.broadcasted_iota(jnp.int32, (RT, T), 0)
                kpos = lax.broadcasted_iota(jnp.int32, (RT, T), 1)
                scores = jnp.where(qpos >= kpos, scores, -1e30)
                e = jnp.exp(scores - jnp.max(scores, axis=-1, keepdims=True))
                p = (e / jnp.sum(e, axis=-1, keepdims=True)).astype(BF16)
                OS[rows, cols] = jnp.dot(p, KV[pr_c, 1], preferred_element_type=F32).astype(BF16)
                return 0

            lax.fori_loop(0, G * (TS // RT), attn_tile, 0)

        UT = tile_of(F, 256)

        @pl.when(mlp_c)
        def _():
            @pl.when(sc == 0)
            def _():
                for w in wm_copies(lc_):
                    w.wait()

            def gate_up(i, _):
                cols = pl.ds(pl.multiple_of(i * UT, UT), UT)
                gate = jnp.dot(H[sc], WG[:, cols], preferred_element_type=F32)
                up = jnp.dot(H[sc], WU[:, cols], preferred_element_type=F32)
                US[:, cols] = (gate * (1.0 / (1.0 + jnp.exp(-gate))) * up).astype(BF16)
                return 0

            lax.fori_loop(0, F // UT, gate_up, 0)

        @pl.when(live_n)
        def _():
            for d in range(2):
                d_a(par_n, d).wait_recv()
                Y = Lf if d else R
                PB[par_n, d, Y, c] = PB[par_n, d, Y, c] + AR[par_n, d]
                d_c(par_n, d).start()

        NT = tile_of(DH, 512)

        def put(h, t, val):
            PB[par_c, h, :, :, :, pl.ds(pl.multiple_of(t * NT, NT), NT)] = (
                val[0:TS].astype(BF16).reshape(CHIPS, CORES, BR, NT))

        @pl.when(attn_c)
        def _():
            for h in range(2):
                def out_tile(t, _):
                    cols = pl.ds(pl.multiple_of(h * DH + t * NT, NT), NT)
                    put(h, t, jnp.dot(OS[...], WO[:, cols], preferred_element_type=F32))
                    return 0

                lax.fori_loop(0, DH // NT, out_tile, 0)
                d_pr(par_c, h).start()

        @pl.when(mlp_c)
        def _():
            for h in range(2):
                def down_tile(t, _):
                    cols = pl.ds(pl.multiple_of(h * DH + t * NT, NT), NT)
                    val = jnp.dot(US[...], WD[:, cols], preferred_element_type=F32)
                    put(h, t, val)
                    DP[:, cols] = val[TS:TS + 8]
                    return 0

                lax.fori_loop(0, DH // NT, down_tile, 0)
                d_pr(par_c, h).start()

        @pl.when(live_1)
        def _():
            s = lax.rem(m1, STREAMS)
            d_g(s, par_1, 0, 0).wait_recv()
            d_r(s, par_1, 0).start()
            d_g(s, par_1, 1, 1).wait_recv()
            d_r(s, par_1, 1).start()

        @pl.when(jnp.logical_or(r8 == 5, jnp.logical_and(r8 == 0, mc > 0)))
        def _():
            d_e(1).wait_recv()
            d_e(1).wait_send()
            EX[E_B] = EX[E_A] + EX[E_IN1]
            d_e(2).start()

        @pl.when(jnp.logical_and(live_c, r8 == 4))
        def _():
            for pr in range(2):
                d_kv(lc_, pr).wait_send()
            for pr in range(2):
                d_kv(lc_, pr).wait_recv()
            rows = lax.broadcasted_iota(jnp.int32, (DEC, hd), 0)
            outs = []
            for pr in range(2):
                @pl.when(lc_ > 0)
                def _():
                    cache_copy(lc_ - 1, pr).wait()

                both = jnp.zeros((DEC, hd), F32)
                for kv in range(2):
                    new = QS[TS:TS + DEC, (G + kv) * hd:(G + kv + 1) * hd].astype(F32)
                    new = jnp.sum(jnp.where(rows == pr, new, 0.0), axis=0, keepdims=True)
                    KVR[lc_, pr, kv, T:T + DEC, :] = jnp.where(rows == 0, new, 0.0).astype(BF16)
                    both = jnp.where(rows == kv, new, both)
                    Z32[pl.ds(kv, T, stride=2), :] = KVR[lc_, pr, kv, 0:T, :].astype(F32)
                ZB[pr, 0:T] = Z32[...].astype(BF16).reshape(T, 2, hd)
                ZB[pr, T:T + DEC // 2] = both.astype(BF16).reshape(DEC // 2, 2, hd)
                cache_copy(lc_, pr).start()
                q = jnp.concatenate([QS[TS:TS + DEC, g * hd:(g + 1) * hd] for g in range(G)], axis=0)
                scores = lax.dot_general(q, KVR[lc_, pr, 0], (((1,), (1,)), ((), ())), preferred_element_type=F32) * scale
                kpos = lax.broadcasted_iota(jnp.int32, (G * DEC, T + PAD), 1)
                scores = jnp.where(kpos <= T, scores, -1e30)
                e = jnp.exp(scores - jnp.max(scores, axis=-1, keepdims=True))
                p = (e / jnp.sum(e, axis=-1, keepdims=True)).astype(BF16)
                outs.append(jnp.dot(p, KVR[lc_, pr, 1], preferred_element_type=F32))
            picked = []
            for g in range(G):
                rest = jnp.where(rows == 1, outs[1][g * DEC:(g + 1) * DEC], 0.0)
                picked.append(jnp.where(rows == 0, outs[0][g * DEC:(g + 1) * DEC], rest).astype(BF16))
            od = jnp.concatenate(picked, axis=1)

            for t in range(D // NT):
                part = jnp.dot(od, WO[:, t * NT:(t + 1) * NT], preferred_element_type=F32)
                DP[:, t * NT:(t + 1) * NT] = part[0:8]
            decode_send()

            @pl.when(lax.div(mc, 8) + 1 < L)
            def _():
                for w in wa_copies(lax.div(mc, 8) + 1):
                    w.start()

        @pl.when(jnp.logical_and(live_c, r8 == 7))
        def _():
            decode_send()

            @pl.when(lax.div(mc, 8) + 1 < L)
            def _():
                for w in wm_copies(lax.div(mc, 8) + 1):
                    w.start()

        return 0

    lax.fori_loop(0, NS + 4, slot, 0)

    fin_a[...] = DY[0:1, :]
    fin_b[...] = DY[1:2, :]
    for pr in range(2):
        cache_copy(L - 1, pr).wait()
    for s in range(STREAMS):
        lc(H.at[s, pl.ds(0, TS)], (oa if s < 2 else ob).at[pl.ds((s % 2) * TS, TS)], s_out.at[s]).wait()


def device_specs():
    row_axes = ('pairs', 'ho')
    in_specs = (P('pairs', None, None), P('pairs', None, None), P(row_axes, None), P(row_axes, None),
                P(None, None, 'tp', None, None), P(None, 'tp', None, None, None), P(None, None, 'tp'),
                P(None, None, 'tp'), P(None, 'tp', None), P(None, None), P(None, None))
    out_specs = (P(row_axes, None, None), P(row_axes, None, None), P(row_axes, None), P(row_axes, None),
                 P(row_axes, None, None, None, 'tp', None), P(row_axes, None, None, None, 'tp', None))
    return in_specs, out_specs


def solution(mesh):
    n_ho, n_tp = mesh.shape['ho'], mesh.shape['tp']
    in_specs, out_specs = device_specs()

    def per_device(prompt_a, prompt_b, first_a, first_b, w_qkv, w_out, w_gate, w_up, w_down, norm_attn, norm_mlp):
        L, D = w_qkv.shape[0], w_qkv.shape[1]
        G, hd = w_out.shape[2], w_out.shape[3]
        F = w_gate.shape[2]
        T = prompt_a.shape[1]
        TS, DH = T // 2, D // 2
        BR = TS // n_tp
        wq = jnp.transpose(w_qkv[:, :, 0], (0, 2, 1, 3))
        wo = w_out.reshape(L, G * hd, D)
        any_spec = pl.BlockSpec(memory_space=pl.ANY)
        vmem_spec = pl.BlockSpec(memory_space=pltpu.VMEM)
        dma = pltpu.SemaphoreType.DMA
        flops = 2 * L * 2 * T * D * (wq.shape[1] * hd + G * hd + 3 * F)
        outs = pl.pallas_call(
            functools.partial(body, (n_ho, n_tp, L, T, D, G, hd, F)),
            name='serve',
            out_shape=(
                jax.ShapeDtypeStruct((T, D), BF16), jax.ShapeDtypeStruct((T, D), BF16),
                jax.ShapeDtypeStruct((1, D), F32), jax.ShapeDtypeStruct((1, D), F32),
                jax.ShapeDtypeStruct((L * (T + 1), 2, hd), BF16), jax.ShapeDtypeStruct((L * (T + 1), 2, hd), BF16)),
            in_specs=[any_spec] * 2 + [vmem_spec] * 2 + [any_spec] * 5 + [vmem_spec] * 2,
            out_specs=(any_spec, any_spec, vmem_spec, vmem_spec, any_spec, any_spec),
            scratch_shapes=[
                pltpu.VMEM((STREAMS, TS + DEC, D), BF16),
                pltpu.VMEM((2, 2, CHIPS, CORES, BR, DH), BF16),
                pltpu.VMEM((2, 2, CHIPS, BR, DH), BF16),
                pltpu.VMEM((2, 2, BR, DH), BF16),
                pltpu.VMEM((2, 2, 2, BR, DH), BF16),
                pltpu.VMEM((STREAMS, BR, D), BF16),
                pltpu.VMEM((TS + DEC, (G + 2) * hd), BF16),
                pltpu.VMEM((2, 2, T, hd), BF16),
                pltpu.VMEM((TS, G * hd), BF16),
                pltpu.VMEM((TS + DEC, F), BF16),
                pltpu.VMEM((L, 2, 2, T + PAD, hd), BF16),
                pltpu.VMEM((D, (G + 2) * hd), BF16),
                pltpu.VMEM((G * hd, D), BF16),
                pltpu.VMEM((D, F), BF16),
                pltpu.VMEM((D, F), BF16),
                pltpu.VMEM((F, D), BF16),
                pltpu.VMEM((8, D), F32),
                pltpu.VMEM((8, D), F32),
                pltpu.VMEM((8, DH // (4 * hd), 8, hd), F32),
                pltpu.VMEM((2 * T, hd), F32),
                pltpu.VMEM((2, T + 8, 2, hd), BF16),
                dma((2, 2)), dma((2, 2)),
                dma((2, 2)), dma((2, 2)),
                dma((2, 2)), dma((2, 2)),
                dma((2, 2)), dma((2, 2)),
                dma((2, 2, 2)), dma((2, 2, 2)),
                dma((2, 2)), dma((2, 2)),
                dma((STREAMS,)), dma((STREAMS,)),
                dma((2,)), dma((L, 2)),
                dma((G + 3,)), dma((3,)), dma((STREAMS,)), dma((STREAMS,)), dma((2,)),
                dma((4,)), dma((4,)),
            ],
            compiler_params=pltpu.CompilerParams(
                collective_id=0, has_side_effects=True, vmem_limit_bytes=44 * 1024 * 1024),
            cost_estimate=pl.CostEstimate(flops=flops, bytes_accessed=2 * L * D * (5 * hd + G * hd + 3 * F), transcendentals=0),
        )(prompt_a, prompt_b, first_a, first_b, wq, wo, w_gate, w_up, w_down, norm_attn, norm_mlp)
        out_a, out_b, fin_a, fin_b, cache_a, cache_b = outs

        def cache(rows):
            return jnp.transpose(rows.reshape(L, T + 1, 2, hd), (0, 2, 1, 3))[None, :, :, :, None, :]

        return (out_a[None], out_b[None], fin_a, fin_b, cache(cache_a), cache(cache_b))

    return jax.shard_map(per_device, mesh=mesh, in_specs=in_specs, out_specs=out_specs, check_vma=False)
```

```python
import functools

import jax
import jax.numpy as jnp
from jax import lax
from jax.experimental import pallas as pl
from jax.experimental.pallas import tpu as pltpu
from jax.sharding import PartitionSpec as P

MESH = pl.DeviceIdType.MESH
F32 = jnp.float32
BF16 = jnp.bfloat16
CORES = 2
CHIPS = 4
STREAMS = 4
DEC = 16
PAD = 128


def tile_of(size, most):
    tile = most
    while size % tile:
        tile //= 2
    return tile


def body(cfg, pa, pb, fa, fb, wq, wo, wg, wu, wd, g1h, g2h, oa, ob, fin_a, fin_b, ca, cb, fq, fo,
         H, PB, PR, AR, BC, XR, QS, KV, OS, US, KVR, WQ, WO, WQF, WOF, WG, WU, WD, g1, g2, FT, DY, DP, EX, Z32, ZB,
         s_prs, s_prr, s_as, s_ar, s_bs, s_br, s_cs, s_cr, s_gs, s_gr, s_rs, s_rr, s_ds, s_dr,
         s_kvs, s_kvr, s_wa, s_wf, s_wm, s_in, s_out, s_ko, s_es, s_er, s_sm,
         s_xs, s_xr, s_us, s_ur, s_ls, s_lr, s_ys, s_yr, s_sync):
    n_ho, n_tp, L, T, D, G, hd, F = cfg
    TS = T // 2
    HS = TS // 2
    BR = TS // n_tp
    DH = D // 2
    NS = 8 * L
    NT4 = EX.shape[1]
    DQ = D // n_ho
    OQ = G * hd // n_ho
    OC = OQ // 3
    scale = hd ** -0.5
    j = lax.axis_index('ho')
    tp = lax.axis_index('tp')
    X = lax.div(tp, CORES)
    c = lax.rem(tp, CORES)
    Q = CHIPS - 1 - X
    V = X + 1 - 2 * lax.rem(X, 2)
    O = CHIPS - 1 - V
    near = (Q, V)

    def pos(Y):
        return 2 * lax.rem(lax.div(Y + 1, 2), 2) + lax.div(Y, 2)

    pX, pQ, pV, pO = pos(X), pos(Q), pos(V), pos(O)
    pN = (pQ, pV)
    hp = lax.div(pX, 2)
    to_near = ({'tp': Q * CORES + c}, {'tp': V * CORES + c})
    to_partner = {'tp': X * CORES + (1 - c)}
    up = lax.rem(j + 1, n_ho)
    down = lax.rem(j + n_ho - 1, n_ho)

    def rc(src, dst, ss, rs, dev):
        return pltpu.make_async_remote_copy(src_ref=src, dst_ref=dst, send_sem=ss, recv_sem=rs,
                                            device_id=dev, device_id_type=MESH)

    def lc(src, dst, sem):
        return pltpu.make_async_copy(src, dst, sem)

    def rows_of(p):
        return pl.ds(pl.multiple_of((p * CORES + c) * BR, BR), BR)

    def d_pr(par, h):
        return rc(PB.at[par, h, :, 1 - c], PR.at[par, h], s_prs.at[par, h], s_prr.at[par, h], to_partner)

    def d_pr_home(par, h):
        return rc(PB.at[par, h, pl.ds(hp * 2, 2), 1 - c], PR.at[par, h, pl.ds(hp * 2, 2)],
                  s_prs.at[par, h], s_prr.at[par, h], to_partner)

    def d_a(par, e, heavy=False):
        return rc(PB.at[par, e, pO, c], AR.at[par, e], s_as.at[par, e], s_ar.at[par, e], to_near[0 if heavy else e])

    def d_b(par, s, e):
        return rc(PB.at[par, e, pN[e], c], BC.at[s, e, e], s_bs.at[s, e], s_br.at[s, e], to_near[e])

    def d_c(par, s, e):
        return rc(PB.at[par, 1 - e, pN[e], c], BC.at[s, e, 1 - e], s_cs.at[s, e], s_cr.at[s, e], to_near[e])

    def h_part(s, p, half):
        return H.at[s, rows_of(p), pl.ds(half * DH, DH)]

    def d_g(s, par, e, half):
        return rc(h_part(s, pX, half), h_part(s, pX, half), s_gs.at[par, e, half], s_gr.at[par, e, half], to_near[e])

    def d_r(s, par, e):
        return rc(h_part(s, pN[e], e), h_part(s, pN[e], e), s_rs.at[par, e], s_rr.at[par, e], to_near[1 - e])

    def d_d(s, p):
        return rc(H.at[s, rows_of(p)], H.at[s, rows_of(p)], s_ds.at[s], s_dr.at[s], to_partner)

    def d_d_all(s, blocks):
        return rc(H.at[s, pl.ds(0, blocks * BR)], H.at[s, pl.ds(0, blocks * BR)], s_ds.at[s], s_dr.at[s], to_partner)

    def quarter(s):
        return pl.ds(pl.multiple_of(s * HS, HS), HS)

    def d_kv(l, f, pr, s, dev):
        return rc(KV.at[f, :, quarter(s)], KVR.at[l, pr, :, quarter(s)], s_kvs.at[f], s_kvr.at[l, pr], dev)

    def d_kv_all(l, f, pr):
        return rc(KV.at[f], KVR.at[l, pr, :, pl.ds(0, T)], s_kvs.at[f], s_kvr.at[l, pr], to_partner)

    E_OUT, E_IN0, E_A, E_IN1, E_B, E_IN2, E_C, E_IN3 = range(8)

    def d_e(step):
        src, dst, dev = ((E_OUT, E_IN0, to_partner), (E_A, E_IN1, to_near[1]), (E_B, E_IN2, to_near[0]),
                         (E_C, E_IN3, to_partner))[step]
        return rc(EX.at[src], EX.at[dst], s_es.at[step], s_er.at[step], dev)

    def cache_copy(l, pr):
        return lc(ZB.at[pr, pl.ds(0, T + 1)], (cb if pr else ca).at[pl.ds(l * (T + 1), T + 1)], s_ko.at[pr])

    def piece(refs, l, k, wide, r):
        if wide:
            return refs[0].at[l, k, pl.ds(pl.multiple_of(r * DQ, DQ), DQ), :]
        return refs[1].at[l, pl.ds(pl.multiple_of(r * OQ + (k - (G + 2)) * OC, OC), OC), :]

    def d_x(l, k, wide):
        return rc(piece((wq, wo), l, k, wide, j), piece((fq, fo), l - 1, k, wide, j), s_xs.at[k], s_xr.at[k], to_near[1])

    def d_up(l, k, wide, r):
        ref = piece((fq, fo), l - 1, k, wide, r)
        return rc(ref, ref, s_us.at[k], s_ur.at[k], {'ho': up})

    def d_down(l, k, wide, r):
        ref = piece((fq, fo), l - 1, k, wide, r)
        return rc(ref, ref, s_ls.at[k], s_lr.at[k], {'ho': down})

    def d_on(l, k, wide, r, dev):
        ref = piece((fq, fo), l - 1, k, wide, r)
        return rc(ref, ref, s_ys.at[k], s_yr.at[k], dev)

    def wa_copies(l):
        out = [lc(wq.at[l, i], WQ.at[:, pl.ds(i * hd, hd)], s_wa.at[i]) for i in range(G + 2)]
        return out + [lc(wo.at[l], WO, s_wa.at[G + 2])]

    def wf_copies(l):
        out = [lc(fq.at[l - 1, i], WQF.at[:, pl.ds(i * hd, hd)], s_wf.at[i]) for i in range(G + 2)]
        return out + [lc(fo.at[l - 1], WOF, s_wf.at[G + 2])]

    def wm_copies(l):
        return [lc(wg.at[l], WG, s_wm.at[0]), lc(wu.at[l], WU, s_wm.at[1]), lc(wd.at[l], WD, s_wm.at[2])]

    def prompt_copies(s):
        return [lc(p.at[j, pl.ds(s * HS, HS)], H.at[s, pl.ds(i * HS, HS)], s_in.at[s, i]) for i, p in enumerate((pa, pb))]

    def out_copies(s):
        return [lc(H.at[s, pl.ds(i * HS, HS)], o.at[pl.ds(s * HS, HS)], s_out.at[s, i]) for i, o in enumerate((oa, ob))]

    small = [lc(g1h, g1, s_sm.at[0]), lc(g2h, g2, s_sm.at[1]), lc(fa, FT.at[0], s_sm.at[2]), lc(fb, FT.at[1], s_sm.at[3])]

    barrier = pltpu.get_barrier_semaphore()
    met = [to_partner, to_near[0], to_near[1], {'ho': up}, {'ho': down},
           {'ho': up, 'tp': V * CORES + c}, {'ho': down, 'tp': V * CORES + c}]
    for dev in met:
        pl.semaphore_signal(barrier, inc=1, device_id=dev, device_id_type=MESH)

    for w in prompt_copies(0) + small + wa_copies(0):
        w.start()
    KV[...] = jnp.zeros(KV.shape, BF16)
    for s in range(STREAMS):
        H[s, TS:TS + DEC, :] = jnp.zeros((DEC, D), BF16)

    def zero_kvr(l, _):
        for pr in range(2):
            for kv in range(2):
                KVR[l, pr, kv, T:T + PAD, :] = jnp.zeros((PAD, hd), BF16)
        return 0

    lax.fori_loop(0, L, zero_kvr, 0)

    def normed(xf, gain):
        ms = jnp.mean(xf * xf, axis=-1, keepdims=True)
        return xf * lax.rsqrt(ms + 1e-5) * gain

    def decode_norm(gain):
        h = normed(DY[...], gain)
        H[STREAMS - 1, TS:TS + DEC, :] = jnp.concatenate([h, jnp.zeros_like(h)], axis=0).astype(BF16)

    for w in small:
        w.wait()
    DY[...] = jnp.zeros(DY.shape, F32)
    DY[0:1, :] = FT[0].astype(F32)
    DY[1:2, :] = FT[1].astype(F32)
    decode_norm(g1[0:1, :])
    pl.semaphore_wait(barrier, len(met))

    def slot(it, _):
        n = it - 1
        m1, m2, m3, mc = n - 1, n - 2, n - 3, n + 1

        def state(m):
            live = jnp.logical_and(m >= 0, m < NS)
            r = lax.rem(m + 16, 8)
            full_rs = jnp.logical_or(m < 8, r >= 4)
            full_ag = jnp.logical_or(r < 4, m >= NS - STREAMS)
            return live, full_rs, full_ag

        def when(*conds):
            out = conds[0]
            for x in conds[1:]:
                out = jnp.logical_and(out, x)
            return pl.when(out)

        live_n, frs_n, _ = state(n)
        live_1, frs_1, fag_1 = state(m1)
        live_2, _, fag_2 = state(m2)
        live_3, _, fag_3 = state(m3)
        live_c, frs_c, _ = state(mc)
        heavy = jnp.logical_and(n >= 1, n < STREAMS)
        par_n, par_1 = lax.rem(n + 8, 2), lax.rem(m1 + 8, 2)
        s_n, s_1, s_2, s_3 = (lax.rem(m + 8, STREAMS) for m in (n, m1, m2, m3))

        def add(h, p):
            PB[par_n, h, p, c] = PB[par_n, h, p, c] + PR[par_n, h, p]

        @when(live_n, frs_n)
        def _():
            for h in range(2):
                d_pr(par_n, h).wait_recv()
            for e in range(2):
                add(e, pO)

            @when(jnp.logical_not(heavy))
            def _():
                for e in range(2):
                    d_a(par_n, e).start()
                for e in range(2):
                    add(e, pN[e])
                for e in range(2):
                    d_b(par_n, s_n, e).start()
                for e in range(2):
                    add(1 - e, pN[e])

            @when(heavy)
            def _():
                for e in range(2):
                    d_a(par_n, e, True).start()
                for e in range(2):
                    add(e, pQ)
                d_b(par_n, s_n, 0).start()
                d_c(par_n, s_n, 0).start()
                for e in range(2):
                    add(e, pV)

            for e in range(2):
                add(e, pX)

        @when(live_n, jnp.logical_not(frs_n))
        def _():
            for h in range(2):
                d_pr_home(par_n, h).wait_recv()
            for h in range(2):
                add(h, pQ)
            d_b(par_n, s_n, 0).start()
            d_c(par_n, s_n, 0).start()
            for h in range(2):
                add(h, pX)

        def pieces(t, fn):
            r = lax.rem(t + 8, 8)

            @when(t == -1)
            def _():
                for k in range(3):
                    fn(1, k, True)

            @when(t >= 0, r == 0, lax.div(t, 8) + 1 < L)
            def _():
                for k in (3, 4):
                    fn(lax.div(t, 8) + 1, k, True)

            @when(t >= 0, r >= 1, r <= 3, lax.div(t, 8) + 1 < L)
            def _():
                fn(lax.div(t, 8) + 1, 4 + r, False)

            @when(t >= 0, r >= 5, lax.div(t, 8) + 2 < L)
            def _():
                fn(lax.div(t, 8) + 2, r - 5, True)

        pieces(n, lambda l, k, wide: d_x(l, k, wide).start())

        @when(n >= 0)
        def _():
            for e in range(2):
                pl.semaphore_wait(s_sync.at[e], 1)

        @when(live_1)
        def _():
            l = lax.div(m1, 8)
            is_attn = lax.rem(lax.div(m1, 4), 2) == 0
            last = m1 >= NS - STREAMS
            d_b(par_1, s_1, 0).wait_recv()
            d_c(par_1, s_1, 0).wait_recv()

            @when(frs_1)
            def _():
                d_b(par_1, s_1, 1).wait_recv()
                d_c(par_1, s_1, 1).wait_recv()

            x_new = []
            ms = jnp.zeros((BR, 1), F32)
            for h in range(2):
                second = jnp.where(frs_1, BC[s_1, 1, h].astype(F32), 0.0)
                total = PB[par_1, h, pX, c].astype(F32) + (BC[s_1, 0, h].astype(F32) + second)
                cols = slice(h * DH, (h + 1) * DH)
                x = XR[s_1, :, cols].astype(F32) + total.astype(BF16).astype(F32)
                x = x.astype(BF16)
                XR[s_1, :, cols] = x
                x = x.astype(F32)
                ms = ms + jnp.sum(x * x, axis=-1, keepdims=True)
                x_new.append(x)
            inv = lax.rsqrt(ms * (1.0 / D) + 1e-5)
            nl = jnp.minimum(l + 1, L - 1)
            for h in range(2):
                cols = slice(h * DH, (h + 1) * DH)
                gain = jnp.where(is_attn, g2[pl.ds(l, 1), cols], g1[pl.ds(nl, 1), cols])
                hn = x_new[h] * inv * gain
                H[s_1, rows_of(pX), cols] = jnp.where(last, x_new[h], hn).astype(BF16)

            d_g(s_1, par_1, 0, 0).start()

            @when(fag_1)
            def _():
                d_g(s_1, par_1, 1, 1).start()

            d_g(s_1, par_1, 0, 1).start()

            @when(fag_1)
            def _():
                d_g(s_1, par_1, 1, 0).start()

            d_d(s_1, pX).start()

        @when(live_1)
        def _():
            d_b(par_1, s_1, 0).wait_send()
            d_c(par_1, s_1, 0).wait_send()

            @when(frs_1)
            def _():
                for h in range(2):
                    d_pr(par_1, h).wait_send()
                for e in range(2):
                    d_a(par_1, e).wait_send()
                d_b(par_1, s_1, 1).wait_send()
                d_c(par_1, s_1, 1).wait_send()

            @when(jnp.logical_not(frs_1))
            def _():
                for h in range(2):
                    d_pr_home(par_1, h).wait_send()

        @when(live_2)
        def _():
            par = lax.rem(m2, 2)
            d_g(s_2, par, 0, 1).wait_recv()

            @when(jnp.logical_not(fag_2))
            def _():
                d_g(s_2, par, 0, 0).wait_recv()

            d_d(s_2, pQ).start()

            @when(fag_2)
            def _():
                d_g(s_2, par, 1, 0).wait_recv()
                d_d(s_2, pV).start()
                for e in range(2):
                    d_r(s_2, par, e).wait_recv()
                d_d(s_2, pO).start()
                for half in range(2):
                    d_g(s_2, par, 1, half).wait_send()
                for e in range(2):
                    d_r(s_2, par, e).wait_send()

            for half in range(2):
                d_g(s_2, par, 0, half).wait_send()

        for full, blocks in ((True, CHIPS), (False, CHIPS // 2)):
            @when(live_3, fag_3 if full else jnp.logical_not(fag_3))
            def _():
                d_d_all(s_3, blocks).wait_recv()
                d_d_all(s_3, blocks).wait_send()

        for s in range(STREAMS):
            @when(m3 == NS - STREAMS + s)
            def _():
                for w in out_copies(s):
                    w.start()

        r8 = lax.rem(mc, 8)
        rows8 = lax.broadcasted_iota(jnp.int32, (8, hd), 0)

        def half_cols(half, k):
            return pl.ds(pl.multiple_of(half * DH + k * hd, hd), hd)

        def decode_send():
            for slot_, half in ((E_OUT, 1 - c), (E_A, c)):
                for t in range(NT4):
                    acc = DP[:, half_cols(half, 4 * t)]
                    for q in range(1, 4):
                        acc = acc + pltpu.roll(DP[:, half_cols(half, 4 * t + q)], 2 * q, axis=0)
                    EX[slot_, t] = acc
            d_e(0).start()

        @when(jnp.logical_or(r8 == 5, jnp.logical_and(r8 == 0, mc > 0)))
        def _():
            d_e(0).wait_recv()
            d_e(0).wait_send()
            EX[E_A] = EX[E_A] + EX[E_IN0]
            d_e(1).start()

        @when(jnp.logical_or(r8 == 6, jnp.logical_and(r8 == 1, mc > 8)))
        def _():
            d_e(2).wait_recv()
            d_e(2).wait_send()
            EX[E_C] = EX[E_B] + EX[E_IN2]
            d_e(3).start()

        @when(jnp.logical_or(r8 == 7, jnp.logical_and(r8 == 2, mc > 8)))
        def _():
            d_e(3).wait_recv()
            d_e(3).wait_send()
            for slot_, half in ((E_C, c), (E_IN3, 1 - c)):
                for t in range(NT4):
                    block = EX[slot_, t]
                    for q in range(4):
                        part = block if q == 0 else pltpu.roll(block, 8 - 2 * q, axis=0)
                        cols = half_cols(half, 4 * t + q)
                        DY[:, cols] = DY[:, cols] + jnp.where(rows8 < 2, part, 0.0)
            lq = lax.div(mc, 8)

            @when(r8 == 7)
            def _():
                decode_norm(g2[pl.ds(lq, 1), :])

            @when(r8 == 2, mc < NS)
            def _():
                decode_norm(g1[pl.ds(jnp.minimum(lq, L - 1), 1), :])

        par_c = lax.rem(mc, 2)
        sc = lax.rem(mc, STREAMS)
        lq_c = jnp.minimum(lax.div(mc, 8), L - 1)
        attn_c = jnp.logical_and(live_c, r8 < 4)
        mlp_c = jnp.logical_and(live_c, r8 >= 4)

        for s in range(STREAMS):
            @when(mc == s)
            def _():
                for w in prompt_copies(s):
                    w.wait()

                def first_rows(i, _):
                    rows = pl.ds(pl.multiple_of(i * BR, BR), BR)
                    hn = normed(H[s, rows, :].astype(F32), g1[0:1, :])
                    H[s, rows, :] = hn.astype(BF16)
                    return 0

                XR[s] = H[s, rows_of(pX), :]
                lax.fori_loop(0, n_tp, first_rows, 0)

        NQKV = (G + 2) * hd

        def qkv_tiles(fn):
            c0 = 0
            while c0 < NQKV:
                c1 = min(c0 + 2 * hd, NQKV)
                fn(c0, c1)
                c0 = c1

        @when(attn_c)
        def _():
            @when(sc == 0)
            def _():
                for w in wa_copies(lq_c):
                    w.wait()

                @when(mc == 0)
                def _():
                    for s in range(1, STREAMS):
                        for w in prompt_copies(s):
                            w.start()
                    for w in wm_copies(0):
                        w.start()

                @when(mc > 0)
                def _():
                    for w in wf_copies(lq_c):
                        w.wait()

            @when(mc < 8)
            def _():
                def go(c0, c1):
                    QS[:, c0:c1] = jnp.dot(H[sc], WQ[:, c0:c1], preferred_element_type=F32).astype(BF16)

                qkv_tiles(go)

            @when(mc >= 8)
            def _():
                home = pl.ds(pl.multiple_of(hp * HS, HS), HS)

                def go(c0, c1):
                    for f, w in enumerate((WQ, WQF)):
                        QS[f * HS:(f + 1) * HS, c0:c1] = jnp.dot(
                            H[sc, home, :], w[:, c0:c1], preferred_element_type=F32).astype(BF16)

                qkv_tiles(go)

                @when(sc == STREAMS - 1)
                def _():
                    def dec(c0, c1):
                        QS[TS:TS + DEC, c0:c1] = jnp.dot(
                            H[STREAMS - 1, TS:TS + DEC, :], WQ[:, c0:c1], preferred_element_type=F32).astype(BF16)

                    qkv_tiles(dec)

            for f in range(2):
                for kv in range(2):
                    KV[f, kv, quarter(sc), :] = QS[f * HS:(f + 1) * HS, (G + kv) * hd:(G + kv + 1) * hd]

            @when(mc < 8)
            def _():
                for f in range(2):
                    d_kv(lq_c, f, f, sc, {'ho': up}).start()

            @when(mc >= 8)
            def _():
                d_kv(lq_c, 0, hp, sc, {'ho': up}).start()
                d_kv(lq_c, 1, hp, sc, {'ho': up, 'tp': V * CORES + c}).start()

            RT = tile_of(HS, 128)

            def attn_tile(i, _):
                g = lax.div(i, TS // RT)
                r = lax.rem(i, TS // RT)
                f = lax.div(r, HS // RT)
                rows = pl.ds(pl.multiple_of(r * RT, RT), RT)
                cols = pl.ds(pl.multiple_of(g * hd, hd), hd)
                q = QS[rows, cols]
                scores = lax.dot_general(q, KV[f, 0], (((1,), (1,)), ((), ())), preferred_element_type=F32) * scale
                qpos = sc * HS + lax.rem(r, HS // RT) * RT + lax.broadcasted_iota(jnp.int32, (RT, T), 0)
                kpos = lax.broadcasted_iota(jnp.int32, (RT, T), 1)
                scores = jnp.where(qpos >= kpos, scores, -1e30)
                e = jnp.exp(scores - jnp.max(scores, axis=-1, keepdims=True))
                p = (e / jnp.sum(e, axis=-1, keepdims=True)).astype(BF16)
                OS[rows, cols] = jnp.dot(p, KV[f, 1], preferred_element_type=F32).astype(BF16)
                return 0

            lax.fori_loop(0, G * (TS // RT), attn_tile, 0)

        UT = tile_of(F, 256)

        @when(mlp_c)
        def _():
            @when(sc == 0)
            def _():
                for w in wm_copies(lq_c):
                    w.wait()

            def gate_up(i, _):
                cols = pl.ds(pl.multiple_of(i * UT, UT), UT)
                gate = jnp.dot(H[sc], WG[:, cols], preferred_element_type=F32)
                up_ = jnp.dot(H[sc], WU[:, cols], preferred_element_type=F32)
                US[:, cols] = (gate * (1.0 / (1.0 + jnp.exp(-gate))) * up_).astype(BF16)
                return 0

            lax.fori_loop(0, F // UT, gate_up, 0)

        @when(live_n, frs_n, jnp.logical_not(heavy))
        def _():
            for e in range(2):
                d_a(par_n, e).wait_recv()
                PB[par_n, e, pN[1 - e], c] = PB[par_n, e, pN[1 - e], c] + AR[par_n, e]
            for e in range(2):
                d_c(par_n, s_n, 1 - e).start()

        @when(heavy)
        def _():
            for e in range(2):
                d_a(par_n, e, True).wait_recv()
                PB[par_n, e, pV, c] = PB[par_n, e, pV, c] + AR[par_n, e]
            d_c(par_n, s_n, 1).start()
            d_b(par_n, s_n, 1).start()

        NT = tile_of(DH, 512)

        def at_cols(t):
            return pl.ds(pl.multiple_of(t * NT, NT), NT)

        @when(attn_c, mc < 8)
        def _():
            for h in range(2):
                def out_tile(t, _):
                    cols = pl.ds(pl.multiple_of(h * DH + t * NT, NT), NT)
                    val = jnp.dot(OS[...], WO[:, cols], preferred_element_type=F32)
                    PB[par_c, h, :, :, :, at_cols(t)] = val.astype(BF16).reshape(CHIPS, CORES, BR, NT)
                    return 0

                lax.fori_loop(0, DH // NT, out_tile, 0)
                d_pr(par_c, h).start()

        @when(attn_c, mc >= 8)
        def _():
            for h in range(2):
                def out_tile(t, _):
                    cols = pl.ds(pl.multiple_of(h * DH + t * NT, NT), NT)
                    val = jnp.dot(OS[0:HS, :], WO[:, cols], preferred_element_type=F32)
                    val = val + jnp.dot(OS[HS:TS, :], WOF[:, cols], preferred_element_type=F32)
                    PB[par_c, h, pl.ds(hp * 2, 2), :, :, at_cols(t)] = val.astype(BF16).reshape(2, CORES, BR, NT)
                    return 0

                lax.fori_loop(0, DH // NT, out_tile, 0)
                d_pr_home(par_c, h).start()

        @when(mlp_c)
        def _():
            for h in range(2):
                def down_tile(t, _):
                    cols = pl.ds(pl.multiple_of(h * DH + t * NT, NT), NT)
                    val = jnp.dot(US[...], WD[:, cols], preferred_element_type=F32)
                    PB[par_c, h, :, :, :, at_cols(t)] = val[0:TS].astype(BF16).reshape(CHIPS, CORES, BR, NT)
                    DP[:, cols] = val[TS:TS + 8]
                    return 0

                lax.fori_loop(0, DH // NT, down_tile, 0)
                d_pr(par_c, h).start()

        @when(n < NS + 2)
        def _():
            for e in range(2):
                pl.semaphore_signal(s_sync.at[e], inc=1, device_id=to_near[e], device_id_type=MESH)

        @when(live_1, fag_1)
        def _():
            for e in range(2):
                d_g(s_1, par_1, e, e).wait_recv()
                d_r(s_1, par_1, e).start()

        @when(jnp.logical_or(r8 == 5, jnp.logical_and(r8 == 0, mc > 0)))
        def _():
            d_e(1).wait_recv()
            d_e(1).wait_send()
            EX[E_B] = EX[E_A] + EX[E_IN1]
            d_e(2).start()

        @when(live_c, r8 == 4)
        def _():
            for pr in range(2):
                d_kv_all(lq_c, pr, pr).wait_send()
            for pr in range(2):
                d_kv_all(lq_c, pr, pr).wait_recv()
            rows = lax.broadcasted_iota(jnp.int32, (DEC, hd), 0)
            outs = []
            for pr in range(2):
                @when(lq_c > 0)
                def _():
                    cache_copy(lq_c - 1, pr).wait()

                both = jnp.zeros((DEC, hd), F32)
                for kv in range(2):
                    new = QS[TS:TS + DEC, (G + kv) * hd:(G + kv + 1) * hd].astype(F32)
                    new = jnp.sum(jnp.where(rows == pr, new, 0.0), axis=0, keepdims=True)
                    KVR[lq_c, pr, kv, T:T + DEC, :] = jnp.where(rows == 0, new, 0.0).astype(BF16)
                    both = jnp.where(rows == kv, new, both)
                    Z32[pl.ds(kv, T, stride=2), :] = KVR[lq_c, pr, kv, 0:T, :].astype(F32)
                ZB[pr, 0:T] = Z32[...].astype(BF16).reshape(T, 2, hd)
                ZB[pr, T:T + DEC // 2] = both.astype(BF16).reshape(DEC // 2, 2, hd)
                cache_copy(lq_c, pr).start()
                q = jnp.concatenate([QS[TS:TS + DEC, g * hd:(g + 1) * hd] for g in range(G)], axis=0)
                scores = lax.dot_general(q, KVR[lq_c, pr, 0], (((1,), (1,)), ((), ())), preferred_element_type=F32) * scale
                kpos = lax.broadcasted_iota(jnp.int32, (G * DEC, T + PAD), 1)
                scores = jnp.where(kpos <= T, scores, -1e30)
                e = jnp.exp(scores - jnp.max(scores, axis=-1, keepdims=True))
                p = (e / jnp.sum(e, axis=-1, keepdims=True)).astype(BF16)
                outs.append(jnp.dot(p, KVR[lq_c, pr, 1], preferred_element_type=F32))
            picked = []
            for g in range(G):
                rest = jnp.where(rows == 1, outs[1][g * DEC:(g + 1) * DEC], 0.0)
                picked.append(jnp.where(rows == 0, outs[0][g * DEC:(g + 1) * DEC], rest).astype(BF16))
            od = jnp.concatenate(picked, axis=1)

            for t in range(D // NT):
                part = jnp.dot(od, WO[:, t * NT:(t + 1) * NT], preferred_element_type=F32)
                DP[:, t * NT:(t + 1) * NT] = part[0:8]
            decode_send()

            @when(lax.div(mc, 8) + 1 < L)
            def _():
                for w in wa_copies(lax.div(mc, 8) + 1):
                    w.start()

        @when(live_c, r8 == 7)
        def _():
            decode_send()

            @when(lax.div(mc, 8) + 1 < L)
            def _():
                for w in wm_copies(lax.div(mc, 8) + 1):
                    w.start()

        def by_parity(k, even, odd):
            if isinstance(k, int):
                (odd if k % 2 else even)()
            else:
                when(lax.rem(k, 2) == 0)(even)
                when(lax.rem(k, 2) == 1)(odd)

        def arrived(l, k, wide):
            opposite = lax.rem(j + 2, n_ho)
            d_on(l, k, wide, opposite, {'ho': up}).wait_recv()
            d_on(l, k, wide, opposite, {'ho': up}).wait_send()

        def pass_on(l, k, wide):
            d_up(l, k, wide, j).wait_recv()
            d_down(l, k, wide, j).wait_recv()
            by_parity(k, lambda: d_on(l, k, wide, down, {'ho': up}).start(),
                      lambda: d_on(l, k, wide, up, {'ho': down}).start())
            d_up(l, k, wide, j).wait_send()
            d_down(l, k, wide, j).wait_send()

        def spread(l, k, wide):
            d_x(l, k, wide).wait_recv()
            d_up(l, k, wide, j).start()
            d_down(l, k, wide, j).start()
            d_x(l, k, wide).wait_send()

        pieces(n - 3, arrived)
        pieces(n - 2, pass_on)
        pieces(n - 1, spread)

        @when(mc >= 7, r8 == 7, lax.div(mc, 8) + 1 < L)
        def _():
            for w in wf_copies(lax.div(mc, 8) + 1):
                w.start()

        return 0

    lax.fori_loop(0, NS + 4, slot, 0)

    fin_a[...] = DY[0:1, :]
    fin_b[...] = DY[1:2, :]
    for pr in range(2):
        cache_copy(L - 1, pr).wait()
    for s in range(STREAMS):
        for w in out_copies(s):
            w.wait()


def device_specs():
    row_axes = ('pairs', 'ho')
    in_specs = (P('pairs', None, None), P('pairs', None, None), P(row_axes, None), P(row_axes, None),
                P(None, None, 'tp', None, None), P(None, 'tp', None, None, None), P(None, None, 'tp'),
                P(None, None, 'tp'), P(None, 'tp', None), P(None, None), P(None, None))
    out_specs = (P(row_axes, None, None), P(row_axes, None, None), P(row_axes, None), P(row_axes, None),
                 P(row_axes, None, None, None, 'tp', None), P(row_axes, None, None, None, 'tp', None))
    return in_specs, out_specs


def solution(mesh):
    n_ho, n_tp = mesh.shape['ho'], mesh.shape['tp']
    in_specs, out_specs = device_specs()

    def per_device(prompt_a, prompt_b, first_a, first_b, w_qkv, w_out, w_gate, w_up, w_down, norm_attn, norm_mlp):
        L, D = w_qkv.shape[0], w_qkv.shape[1]
        G, hd = w_out.shape[2], w_out.shape[3]
        F = w_gate.shape[2]
        T = prompt_a.shape[1]
        TS, DH = T // 2, D // 2
        BR = TS // n_tp
        wq = jnp.transpose(w_qkv[:, :, 0], (0, 2, 1, 3))
        wo = w_out.reshape(L, G * hd, D)
        any_spec = pl.BlockSpec(memory_space=pl.ANY)
        hbm_spec = pl.BlockSpec(memory_space=pltpu.HBM)
        vmem_spec = pl.BlockSpec(memory_space=pltpu.VMEM)
        dma = pltpu.SemaphoreType.DMA
        flops = 2 * L * 2 * T * D * (wq.shape[1] * hd + G * hd + 3 * F)
        outs = pl.pallas_call(
            functools.partial(body, (n_ho, n_tp, L, T, D, G, hd, F)),
            name='serve',
            out_shape=(
                jax.ShapeDtypeStruct((T, D), BF16), jax.ShapeDtypeStruct((T, D), BF16),
                jax.ShapeDtypeStruct((1, D), F32), jax.ShapeDtypeStruct((1, D), F32),
                jax.ShapeDtypeStruct((L * (T + 1), 2, hd), BF16), jax.ShapeDtypeStruct((L * (T + 1), 2, hd), BF16),
                jax.ShapeDtypeStruct((L - 1, G + 2, D, hd), BF16), jax.ShapeDtypeStruct((L - 1, G * hd, D), BF16)),
            in_specs=[hbm_spec] * 11,
            out_specs=(any_spec, any_spec, vmem_spec, vmem_spec, any_spec, any_spec, hbm_spec, hbm_spec),
            scratch_shapes=[
                pltpu.VMEM((STREAMS, TS + DEC, D), BF16),
                pltpu.VMEM((2, 2, CHIPS, CORES, BR, DH), BF16),
                pltpu.VMEM((2, 2, CHIPS, BR, DH), BF16),
                pltpu.VMEM((2, 2, BR, DH), BF16),
                pltpu.VMEM((STREAMS, 2, 2, BR, DH), BF16),
                pltpu.VMEM((STREAMS, BR, D), BF16),
                pltpu.VMEM((TS + DEC, (G + 2) * hd), BF16),
                pltpu.VMEM((2, 2, T, hd), BF16),
                pltpu.VMEM((TS, G * hd), BF16),
                pltpu.VMEM((TS + DEC, F), BF16),
                pltpu.VMEM((L, 2, 2, T + PAD, hd), BF16),
                pltpu.VMEM((D, (G + 2) * hd), BF16),
                pltpu.VMEM((G * hd, D), BF16),
                pltpu.VMEM((D, (G + 2) * hd), BF16),
                pltpu.VMEM((G * hd, D), BF16),
                pltpu.VMEM((D, F), BF16),
                pltpu.VMEM((D, F), BF16),
                pltpu.VMEM((F, D), BF16),
                pltpu.VMEM((L, D), F32),
                pltpu.VMEM((L, D), F32),
                pltpu.VMEM((2, 1, D), BF16),
                pltpu.VMEM((8, D), F32),
                pltpu.VMEM((8, D), F32),
                pltpu.VMEM((8, DH // (4 * hd), 8, hd), F32),
                pltpu.VMEM((2 * T, hd), F32),
                pltpu.VMEM((2, T + 8, 2, hd), BF16),
                dma((2, 2)), dma((2, 2)),
                dma((2, 2)), dma((2, 2)),
                dma((STREAMS, 2)), dma((STREAMS, 2)),
                dma((STREAMS, 2)), dma((STREAMS, 2)),
                dma((2, 2, 2)), dma((2, 2, 2)),
                dma((2, 2)), dma((2, 2)),
                dma((STREAMS,)), dma((STREAMS,)),
                dma((2,)), dma((L, 2)),
                dma((G + 3,)), dma((G + 3,)), dma((3,)),
                dma((STREAMS, 2)), dma((STREAMS, 2)), dma((2,)),
                dma((4,)), dma((4,)), dma((4,)),
                dma((8,)), dma((8,)), dma((8,)), dma((8,)), dma((8,)), dma((8,)), dma((8,)), dma((8,)),
                pltpu.SemaphoreType.REGULAR((2,)),
            ],
            compiler_params=pltpu.CompilerParams(
                collective_id=0, has_side_effects=True, vmem_limit_bytes=54 * 1024 * 1024),
            cost_estimate=pl.CostEstimate(flops=flops, bytes_accessed=2 * L * D * (5 * hd + G * hd + 3 * F), transcendentals=0),
        )(prompt_a, prompt_b, first_a, first_b, wq, wo, w_gate, w_up, w_down, norm_attn, norm_mlp)
        out_a, out_b, fin_a, fin_b, cache_a, cache_b = outs[:6]

        def cache(rows):
            return jnp.transpose(rows.reshape(L, T + 1, 2, hd), (0, 2, 1, 3))[None, :, :, :, None, :]

        return (out_a[None], out_b[None], fin_a, fin_b, cache(cache_a), cache(cache_b))

    return jax.shard_map(per_device, mesh=mesh, in_specs=in_specs, out_specs=out_specs, check_vma=False)
```

```python
import functools

import jax
import jax.numpy as jnp
from jax import lax
from jax.experimental import pallas as pl
from jax.experimental.pallas import tpu as pltpu
from jax.sharding import PartitionSpec as P

MESH = pl.DeviceIdType.MESH
F32 = jnp.float32
BF16 = jnp.bfloat16
CORES = 2
CHIPS = 4
BOTH = range(2)
STREAMS = 4
DEC = 16
PAD = 128


def tile_of(size, most):
    tile = most
    while size % tile:
        tile //= 2
    return tile


def body(cfg, pa, pb, fa, fb, wq, wo, wg, wu, wd, g1h, g2h, oa, ob, fin_a, fin_b, ca, cb,
         H, PB, PR, AR, BC, XR, QS, KV, OS, US, KVR, WQ, WO, WQF, WOF, XSQ, XSO, WG, WU, WD, g1, g2, FT, DY, DP, EX, Z32, ZB,
         s_prs, s_prr, s_as, s_ar, s_bs, s_br, s_cs, s_cr, s_gs, s_gr, s_rs, s_rr, s_ds, s_dr,
         s_kvs, s_kvr, s_wa, s_ps, s_wm, s_in, s_out, s_ko, s_es, s_er, s_sm,
         s_xs, s_xr, s_us, s_ur, s_ls, s_lr, s_ys, s_yr, s_sync):
    n_ho, n_tp, L, T, D, G, hd, F = cfg
    TS = T // 2
    HS = TS // 2
    BR = TS // n_tp
    DH = D // 2
    NS = 8 * L
    NT4 = EX.shape[1]
    DQ = D // n_ho
    OQ = G * hd // n_ho
    OC = OQ // 3
    scale = hd ** -0.5
    j = lax.axis_index('ho')
    tp = lax.axis_index('tp')
    X = lax.div(tp, CORES)
    c = lax.rem(tp, CORES)
    Q = CHIPS - 1 - X
    V = X + 1 - 2 * lax.rem(X, 2)
    O = CHIPS - 1 - V
    near = (Q, V)

    def pos(Y):
        return 2 * lax.rem(lax.div(Y + 1, 2), 2) + lax.div(Y, 2)

    pX, pQ, pV, pO = pos(X), pos(Q), pos(V), pos(O)
    pN = (pQ, pV)
    hp = lax.div(pX, 2)
    to_near = ({'tp': Q * CORES + c}, {'tp': V * CORES + c})
    to_partner = {'tp': X * CORES + (1 - c)}
    up = lax.rem(j + 1, n_ho)
    down = lax.rem(j + n_ho - 1, n_ho)

    def rc(src, dst, ss, rs, dev):
        return pltpu.make_async_remote_copy(src_ref=src, dst_ref=dst, send_sem=ss, recv_sem=rs,
                                            device_id=dev, device_id_type=MESH)

    def lc(src, dst, sem):
        return pltpu.make_async_copy(src, dst, sem)

    def rows_of(p):
        return pl.ds(pl.multiple_of((p * CORES + c) * BR, BR), BR)

    def d_pr(par, h):
        return rc(PB.at[par, h, :, 1 - c], PR.at[par, h], s_prs.at[par, h], s_prr.at[par, h], to_partner)

    def d_pr_home(par, h):
        return rc(PB.at[par, h, pl.ds(hp * 2, 2), 1 - c], PR.at[par, h, pl.ds(hp * 2, 2)],
                  s_prs.at[par, h], s_prr.at[par, h], to_partner)

    def d_a(par, e, heavy=False):
        return rc(PB.at[par, e, pO, c], AR.at[par, e], s_as.at[par, e], s_ar.at[par, e], to_near[0 if heavy else e])

    def d_b(par, s, e):
        return rc(PB.at[par, e, pN[e], c], BC.at[s, e, e], s_bs.at[s, e], s_br.at[s, e], to_near[e])

    def d_c(par, s, e):
        return rc(PB.at[par, 1 - e, pN[e], c], BC.at[s, e, 1 - e], s_cs.at[s, e], s_cr.at[s, e], to_near[e])

    def h_part(s, p, half):
        return H.at[s, rows_of(p), pl.ds(half * DH, DH)]

    def d_g(s, par, e, half):
        return rc(h_part(s, pX, half), h_part(s, pX, half), s_gs.at[par, e, half], s_gr.at[par, e, half], to_near[e])

    def d_r(s, par, e):
        return rc(h_part(s, pN[e], e), h_part(s, pN[e], e), s_rs.at[par, e], s_rr.at[par, e], to_near[1 - e])

    def d_d(s, p):
        return rc(H.at[s, rows_of(p)], H.at[s, rows_of(p)], s_ds.at[s], s_dr.at[s], to_partner)

    def d_d_all(s, blocks):
        return rc(H.at[s, pl.ds(0, blocks * BR)], H.at[s, pl.ds(0, blocks * BR)], s_ds.at[s], s_dr.at[s], to_partner)

    def quarter(s):
        return pl.ds(pl.multiple_of(s * HS, HS), HS)

    def d_kv(l, f, pr, s, dev):
        return rc(KV.at[f, :, quarter(s)], KVR.at[l, pr, :, quarter(s)], s_kvs.at[f], s_kvr.at[l, pr], dev)

    def d_kv_all(l, f, pr):
        return rc(KV.at[f], KVR.at[l, pr, :, pl.ds(0, T)], s_kvs.at[f], s_kvr.at[l, pr], to_partner)

    E_OUT, E_IN0, E_A, E_IN1, E_B, E_IN2, E_C, E_IN3 = range(8)

    def d_e(step):
        src, dst, dev = ((E_OUT, E_IN0, to_partner), (E_A, E_IN1, to_near[1]), (E_B, E_IN2, to_near[0]),
                         (E_C, E_IN3, to_partner))[step]
        return rc(EX.at[src], EX.at[dst], s_es.at[step], s_er.at[step], dev)

    def cache_copy(l, pr):
        return lc(ZB.at[pr, pl.ds(0, T + 1)], (cb if pr else ca).at[pl.ds(l * (T + 1), T + 1)], s_ko.at[pr])

    def piece(l, k, wide, r):
        par = lax.rem(l, 2)
        if wide:
            return WQF.at[par, pl.ds(pl.multiple_of(r * DQ, DQ), DQ), pl.ds(pl.multiple_of(k * hd, hd), hd)]
        return WOF.at[par, pl.ds(pl.multiple_of(r * OQ + (k - (G + 2)) * OC, OC), OC), :]

    def fetched(k, wide):
        return XSQ.at[k] if wide else XSO.at[k - (G + 2)]

    def d_fetch(l, k, wide):
        if wide:
            src = wq.at[l, k, pl.ds(pl.multiple_of(j * DQ, DQ), DQ), :]
        else:
            src = wo.at[l, pl.ds(pl.multiple_of(j * OQ + (k - (G + 2)) * OC, OC), OC), :]
        return lc(src, fetched(k, wide), s_ps.at[k])

    def d_x(l, k, wide):
        return rc(fetched(k, wide), piece(l, k, wide, j), s_xs.at[k], s_xr.at[k], to_near[1])

    def d_up(l, k, wide, r):
        return rc(piece(l, k, wide, r), piece(l, k, wide, r), s_us.at[k], s_ur.at[k], {'ho': up})

    def d_down(l, k, wide, r):
        return rc(piece(l, k, wide, r), piece(l, k, wide, r), s_ls.at[k], s_lr.at[k], {'ho': down})

    def d_on(l, k, wide, r, dev):
        return rc(piece(l, k, wide, r), piece(l, k, wide, r), s_ys.at[k], s_yr.at[k], dev)

    def wa_copies(l):
        out = [lc(wq.at[l, i], WQ.at[:, pl.ds(i * hd, hd)], s_wa.at[i]) for i in range(G + 2)]
        return out + [lc(wo.at[l], WO, s_wa.at[G + 2])]

    def wm_copies(l):
        return [lc(src.at[l], dst, s_wm.at[i]) for i, (src, dst) in enumerate(((wg, WG), (wu, WU), (wd, WD)))]

    def prompt_copies(s):
        return [lc(p.at[j, pl.ds(s * HS, HS)], H.at[s, pl.ds(i * HS, HS)], s_in.at[s, i]) for i, p in enumerate((pa, pb))]

    def out_copies(s):
        return [lc(H.at[s, pl.ds(i * HS, HS)], o.at[pl.ds(s * HS, HS)], s_out.at[s, i]) for i, o in enumerate((oa, ob))]

    small = [lc(src, dst, s_sm.at[i])
             for i, (src, dst) in enumerate(((g1h, g1), (g2h, g2), (fa, FT.at[0]), (fb, FT.at[1])))]

    barrier = pltpu.get_barrier_semaphore()
    met = [to_partner, to_near[0], to_near[1], {'ho': up}, {'ho': down},
           {'ho': up, 'tp': V * CORES + c}, {'ho': down, 'tp': V * CORES + c}]
    for dev in met:
        pl.semaphore_signal(barrier, inc=1, device_id=dev, device_id_type=MESH)

    for w in prompt_copies(0) + small + [d_fetch(1, k, True) for k in range(3)] + wa_copies(0):
        w.start()
    KV[...] = jnp.zeros(KV.shape, BF16)
    for s in range(STREAMS):
        H[s, TS:TS + DEC, :] = jnp.zeros((DEC, D), BF16)

    def zero_kvr(l, _):
        for pr in BOTH:
            for kv in BOTH:
                KVR[l, pr, kv, T:T + PAD, :] = jnp.zeros((PAD, hd), BF16)
        return 0

    lax.fori_loop(0, L, zero_kvr, 0)

    def normed(xf, gain):
        ms = jnp.mean(xf * xf, axis=-1, keepdims=True)
        return xf * lax.rsqrt(ms + 1e-5) * gain

    def decode_norm(gain):
        h = normed(DY[...], gain)
        H[STREAMS - 1, TS:TS + DEC, :] = jnp.concatenate([h, jnp.zeros_like(h)], axis=0).astype(BF16)

    for w in small:
        w.wait()
    DY[...] = jnp.zeros(DY.shape, F32)
    for i in BOTH:
        DY[i:i + 1, :] = FT[i].astype(F32)
    decode_norm(g1[0:1, :])
    pl.semaphore_wait(barrier, len(met))

    def slot(it, _):
        n = it - 1
        m1, m2, m3, mc = n - 1, n - 2, n - 3, n + 1

        def state(m):
            live = jnp.logical_and(m >= 0, m < NS)
            r = lax.rem(m + 16, 8)
            full_rs = jnp.logical_or(m < 8, r >= 4)
            full_ag = jnp.logical_or(r < 4, m >= NS - STREAMS)
            return live, full_rs, full_ag

        def when(*conds):
            out = conds[0]
            for x in conds[1:]:
                out = jnp.logical_and(out, x)
            return pl.when(out)

        live_n, frs_n, _ = state(n)
        live_1, frs_1, fag_1 = state(m1)
        live_2, _, fag_2 = state(m2)
        live_3, _, fag_3 = state(m3)
        live_c, frs_c, _ = state(mc)
        heavy = jnp.logical_and(n >= 1, n < STREAMS)
        par_n, par_1 = lax.rem(n + 8, 2), lax.rem(m1 + 8, 2)
        s_n, s_1, s_2, s_3 = (lax.rem(m + 8, STREAMS) for m in (n, m1, m2, m3))

        def add(h, p):
            PB[par_n, h, p, c] = PB[par_n, h, p, c] + PR[par_n, h, p]

        @when(live_n, frs_n)
        def _():
            for h in BOTH:
                d_pr(par_n, h).wait_recv()
            for e in BOTH:
                add(e, pO)

            @when(jnp.logical_not(heavy))
            def _():
                for e in BOTH:
                    d_a(par_n, e).start()
                for e in BOTH:
                    add(e, pN[e])
                for e in BOTH:
                    d_b(par_n, s_n, e).start()
                for e in BOTH:
                    add(1 - e, pN[e])

            @when(heavy)
            def _():
                for e in BOTH:
                    d_a(par_n, e, True).start()
                for e in BOTH:
                    add(e, pQ)
                d_b(par_n, s_n, 0).start()
                d_c(par_n, s_n, 0).start()
                for e in BOTH:
                    add(e, pV)

            for e in BOTH:
                add(e, pX)

        @when(live_n, jnp.logical_not(frs_n))
        def _():
            for h in BOTH:
                d_pr_home(par_n, h).wait_recv()
            for h in BOTH:
                add(h, pQ)
            d_b(par_n, s_n, 0).start()
            d_c(par_n, s_n, 0).start()
            for h in BOTH:
                add(h, pX)

        def pieces(t, fn):
            r = lax.rem(t + 8, 8)

            @when(t == -1)
            def _():
                for k in range(3):
                    fn(1, k, True)

            @when(t >= 0, r == 0, lax.div(t, 8) + 1 < L)
            def _():
                for k in (3, 4):
                    fn(lax.div(t, 8) + 1, k, True)

            @when(t >= 0, r >= 1, r <= 3, lax.div(t, 8) + 1 < L)
            def _():
                fn(lax.div(t, 8) + 1, 4 + r, False)

            @when(t >= 0, r >= 5, lax.div(t, 8) + 2 < L)
            def _():
                fn(lax.div(t, 8) + 2, r - 5, True)

        def by_parity(k, even, odd):
            if isinstance(k, int):
                (odd if k % 2 else even)()
            else:
                when(lax.rem(k, 2) == 0)(even)
                when(lax.rem(k, 2) == 1)(odd)

        def arrived(l, k, wide):
            opposite = lax.rem(j + 2, n_ho)
            d_on(l, k, wide, opposite, {'ho': up}).wait_recv()
            d_on(l, k, wide, opposite, {'ho': up}).wait_send()

        def pass_on(l, k, wide):
            d_up(l, k, wide, j).wait_recv()
            d_down(l, k, wide, j).wait_recv()
            by_parity(k, lambda: d_on(l, k, wide, down, {'ho': up}).start(),
                      lambda: d_on(l, k, wide, up, {'ho': down}).start())
            d_up(l, k, wide, j).wait_send()
            d_down(l, k, wide, j).wait_send()

        def spread(l, k, wide):
            d_x(l, k, wide).wait_recv()
            d_up(l, k, wide, j).start()
            d_down(l, k, wide, j).start()
            d_x(l, k, wide).wait_send()

        def send_over(l, k, wide):
            d_fetch(l, k, wide).wait()
            d_x(l, k, wide).start()

        pieces(n, send_over)

        @when(n >= 0)
        def _():
            for e in BOTH:
                pl.semaphore_wait(s_sync.at[e], 1)

        @when(live_1)
        def _():
            l = lax.div(m1, 8)
            is_attn = lax.rem(lax.div(m1, 4), 2) == 0
            last = m1 >= NS - STREAMS
            d_b(par_1, s_1, 0).wait_recv()
            d_c(par_1, s_1, 0).wait_recv()

            @when(frs_1)
            def _():
                d_b(par_1, s_1, 1).wait_recv()
                d_c(par_1, s_1, 1).wait_recv()

            x_new = []
            ms = jnp.zeros((BR, 1), F32)
            for h in BOTH:
                second = jnp.where(frs_1, BC[s_1, 1, h].astype(F32), 0.0)
                total = PB[par_1, h, pX, c].astype(F32) + (BC[s_1, 0, h].astype(F32) + second)
                cols = slice(h * DH, (h + 1) * DH)
                x = XR[s_1, :, cols].astype(F32) + total.astype(BF16).astype(F32)
                x = x.astype(BF16)
                XR[s_1, :, cols] = x
                x = x.astype(F32)
                ms = ms + jnp.sum(x * x, axis=-1, keepdims=True)
                x_new.append(x)
            inv = lax.rsqrt(ms * (1.0 / D) + 1e-5)
            nl = jnp.minimum(l + 1, L - 1)
            for h in BOTH:
                cols = slice(h * DH, (h + 1) * DH)
                gain = jnp.where(is_attn, g2[pl.ds(l, 1), cols], g1[pl.ds(nl, 1), cols])
                hn = x_new[h] * inv * gain
                H[s_1, rows_of(pX), cols] = jnp.where(last, x_new[h], hn).astype(BF16)

            d_g(s_1, par_1, 0, 0).start()

            @when(fag_1)
            def _():
                d_g(s_1, par_1, 1, 1).start()

            d_g(s_1, par_1, 0, 1).start()

            @when(fag_1)
            def _():
                d_g(s_1, par_1, 1, 0).start()

            d_d(s_1, pX).start()

        @when(live_1)
        def _():
            d_b(par_1, s_1, 0).wait_send()
            d_c(par_1, s_1, 0).wait_send()

            @when(frs_1)
            def _():
                for h in BOTH:
                    d_pr(par_1, h).wait_send()
                for e in BOTH:
                    d_a(par_1, e).wait_send()
                d_b(par_1, s_1, 1).wait_send()
                d_c(par_1, s_1, 1).wait_send()

            @when(jnp.logical_not(frs_1))
            def _():
                for h in BOTH:
                    d_pr_home(par_1, h).wait_send()

        @when(live_2)
        def _():
            par = lax.rem(m2, 2)
            d_g(s_2, par, 0, 1).wait_recv()

            @when(jnp.logical_not(fag_2))
            def _():
                d_g(s_2, par, 0, 0).wait_recv()

            d_d(s_2, pQ).start()

            @when(fag_2)
            def _():
                d_g(s_2, par, 1, 0).wait_recv()
                d_d(s_2, pV).start()
                for e in BOTH:
                    d_r(s_2, par, e).wait_recv()
                d_d(s_2, pO).start()
                for half in BOTH:
                    d_g(s_2, par, 1, half).wait_send()
                for e in BOTH:
                    d_r(s_2, par, e).wait_send()

            for half in BOTH:
                d_g(s_2, par, 0, half).wait_send()

        for full, blocks in ((True, CHIPS), (False, CHIPS // 2)):
            @when(live_3, fag_3 if full else jnp.logical_not(fag_3))
            def _():
                d_d_all(s_3, blocks).wait_recv()
                d_d_all(s_3, blocks).wait_send()

        for s in range(STREAMS):
            @when(m3 == NS - STREAMS + s)
            def _():
                for w in out_copies(s):
                    w.start()

        pieces(n - 4, arrived)
        pieces(n - 1, spread)

        r8 = lax.rem(mc, 8)
        rows8 = lax.broadcasted_iota(jnp.int32, (8, hd), 0)

        def half_cols(half, k):
            return pl.ds(pl.multiple_of(half * DH + k * hd, hd), hd)

        def decode_send():
            for slot_, half in ((E_OUT, 1 - c), (E_A, c)):
                for t in range(NT4):
                    acc = DP[:, half_cols(half, 4 * t)]
                    for q in range(1, 4):
                        acc = acc + pltpu.roll(DP[:, half_cols(half, 4 * t + q)], 2 * q, axis=0)
                    EX[slot_, t] = acc
            d_e(0).start()

        @when(jnp.logical_or(r8 == 5, jnp.logical_and(r8 == 0, mc > 0)))
        def _():
            d_e(0).wait_recv()
            d_e(0).wait_send()
            EX[E_A] = EX[E_A] + EX[E_IN0]
            d_e(1).start()

        @when(jnp.logical_or(r8 == 6, jnp.logical_and(r8 == 1, mc > 8)))
        def _():
            d_e(2).wait_recv()
            d_e(2).wait_send()
            EX[E_C] = EX[E_B] + EX[E_IN2]
            d_e(3).start()

        @when(jnp.logical_or(r8 == 7, jnp.logical_and(r8 == 2, mc > 8)))
        def _():
            d_e(3).wait_recv()
            d_e(3).wait_send()
            for slot_, half in ((E_C, c), (E_IN3, 1 - c)):
                for t in range(NT4):
                    block = EX[slot_, t]
                    for q in range(4):
                        part = block if q == 0 else pltpu.roll(block, 8 - 2 * q, axis=0)
                        cols = half_cols(half, 4 * t + q)
                        DY[:, cols] = DY[:, cols] + jnp.where(rows8 < 2, part, 0.0)
            lq = lax.div(mc, 8)

            @when(r8 == 7)
            def _():
                decode_norm(g2[pl.ds(lq, 1), :])

            @when(r8 == 2, mc < NS)
            def _():
                decode_norm(g1[pl.ds(jnp.minimum(lq, L - 1), 1), :])

        par_c = lax.rem(mc, 2)
        sc = lax.rem(mc, STREAMS)
        lq_c = jnp.minimum(lax.div(mc, 8), L - 1)
        attn_c = jnp.logical_and(live_c, r8 < 4)
        mlp_c = jnp.logical_and(live_c, r8 >= 4)

        for s in range(STREAMS):
            @when(mc == s)
            def _():
                for w in prompt_copies(s):
                    w.wait()

                def first_rows(i, _):
                    rows = pl.ds(pl.multiple_of(i * BR, BR), BR)
                    hn = normed(H[s, rows, :].astype(F32), g1[0:1, :])
                    H[s, rows, :] = hn.astype(BF16)
                    return 0

                XR[s] = H[s, rows_of(pX), :]
                lax.fori_loop(0, n_tp, first_rows, 0)

        NQKV = (G + 2) * hd

        def qkv_tiles(fn):
            c0 = 0
            while c0 < NQKV:
                c1 = min(c0 + 2 * hd, NQKV)
                fn(c0, c1)
                c0 = c1

        @when(attn_c)
        def _():
            @when(sc == 0)
            def _():
                for w in wa_copies(lq_c):
                    w.wait()

                @when(mc == 0)
                def _():
                    for s in range(1, STREAMS):
                        for w in prompt_copies(s):
                            w.start()
                    for w in wm_copies(0):
                        w.start()

            @when(mc < 8)
            def _():
                def go(c0, c1):
                    QS[:, c0:c1] = jnp.dot(H[sc], WQ[:, c0:c1], preferred_element_type=F32).astype(BF16)

                qkv_tiles(go)

            @when(mc >= 8)
            def _():
                home = pl.ds(pl.multiple_of(hp * HS, HS), HS)
                lpar = lax.rem(lq_c, 2)

                def go(c0, c1):
                    for f, w in enumerate((WQ, WQF.at[lpar])):
                        QS[f * HS:(f + 1) * HS, c0:c1] = jnp.dot(
                            H[sc, home, :], w[:, c0:c1], preferred_element_type=F32).astype(BF16)

                qkv_tiles(go)

                @when(sc == STREAMS - 1)
                def _():
                    def dec(c0, c1):
                        QS[TS:TS + DEC, c0:c1] = jnp.dot(
                            H[STREAMS - 1, TS:TS + DEC, :], WQ[:, c0:c1], preferred_element_type=F32).astype(BF16)

                    qkv_tiles(dec)

            for f in BOTH:
                for kv in BOTH:
                    KV[f, kv, quarter(sc), :] = QS[f * HS:(f + 1) * HS, (G + kv) * hd:(G + kv + 1) * hd]

            @when(mc < 8)
            def _():
                for f in BOTH:
                    d_kv(lq_c, f, f, sc, {'ho': up}).start()

            @when(mc >= 8)
            def _():
                d_kv(lq_c, 0, hp, sc, {'ho': up}).start()
                d_kv(lq_c, 1, hp, sc, {'ho': up, 'tp': V * CORES + c}).start()

            RT = tile_of(HS, 128)

            def attn_tile(i, _):
                g = lax.div(i, TS // RT)
                r = lax.rem(i, TS // RT)
                f = lax.div(r, HS // RT)
                rows = pl.ds(pl.multiple_of(r * RT, RT), RT)
                cols = pl.ds(pl.multiple_of(g * hd, hd), hd)
                q = QS[rows, cols]
                scores = lax.dot_general(q, KV[f, 0], (((1,), (1,)), ((), ())), preferred_element_type=F32) * scale
                qpos = sc * HS + lax.rem(r, HS // RT) * RT + lax.broadcasted_iota(jnp.int32, (RT, T), 0)
                kpos = lax.broadcasted_iota(jnp.int32, (RT, T), 1)
                scores = jnp.where(qpos >= kpos, scores, -1e30)
                e = jnp.exp(scores - jnp.max(scores, axis=-1, keepdims=True))
                p = (e / jnp.sum(e, axis=-1, keepdims=True)).astype(BF16)
                OS[rows, cols] = jnp.dot(p, KV[f, 1], preferred_element_type=F32).astype(BF16)
                return 0

            lax.fori_loop(0, G * (TS // RT), attn_tile, 0)

        UT = tile_of(F, 256)

        @when(mlp_c)
        def _():
            @when(sc == 0)
            def _():
                for w in wm_copies(lq_c):
                    w.wait()

            def gate_up(i, _):
                cols = pl.ds(pl.multiple_of(i * UT, UT), UT)
                gate = jnp.dot(H[sc], WG[:, cols], preferred_element_type=F32)
                up_ = jnp.dot(H[sc], WU[:, cols], preferred_element_type=F32)
                US[:, cols] = (gate * (1.0 / (1.0 + jnp.exp(-gate))) * up_).astype(BF16)
                return 0

            lax.fori_loop(0, F // UT, gate_up, 0)

        @when(live_n, frs_n, jnp.logical_not(heavy))
        def _():
            for e in BOTH:
                d_a(par_n, e).wait_recv()
                PB[par_n, e, pN[1 - e], c] = PB[par_n, e, pN[1 - e], c] + AR[par_n, e]
            for e in BOTH:
                d_c(par_n, s_n, 1 - e).start()

        @when(heavy)
        def _():
            for e in BOTH:
                d_a(par_n, e, True).wait_recv()
                PB[par_n, e, pV, c] = PB[par_n, e, pV, c] + AR[par_n, e]
            d_c(par_n, s_n, 1).start()
            d_b(par_n, s_n, 1).start()

        NT = tile_of(DH, 512)

        def at_cols(t):
            return pl.ds(pl.multiple_of(t * NT, NT), NT)

        @when(attn_c, mc < 8)
        def _():
            for h in BOTH:
                def out_tile(t, _):
                    cols = pl.ds(pl.multiple_of(h * DH + t * NT, NT), NT)
                    val = jnp.dot(OS[...], WO[:, cols], preferred_element_type=F32)
                    PB[par_c, h, :, :, :, at_cols(t)] = val.astype(BF16).reshape(CHIPS, CORES, BR, NT)
                    return 0

                lax.fori_loop(0, DH // NT, out_tile, 0)
                d_pr(par_c, h).start()

        @when(attn_c, mc >= 8)
        def _():
            for h in BOTH:
                def out_tile(t, _):
                    cols = pl.ds(pl.multiple_of(h * DH + t * NT, NT), NT)
                    val = jnp.dot(OS[0:HS, :], WO[:, cols], preferred_element_type=F32)
                    val = val + jnp.dot(OS[HS:TS, :], WOF[lax.rem(lq_c, 2), :, cols], preferred_element_type=F32)
                    PB[par_c, h, pl.ds(hp * 2, 2), :, :, at_cols(t)] = val.astype(BF16).reshape(2, CORES, BR, NT)
                    return 0

                lax.fori_loop(0, DH // NT, out_tile, 0)
                d_pr_home(par_c, h).start()

        @when(mlp_c)
        def _():
            for h in BOTH:
                def down_tile(t, _):
                    cols = pl.ds(pl.multiple_of(h * DH + t * NT, NT), NT)
                    val = jnp.dot(US[...], WD[:, cols], preferred_element_type=F32)
                    PB[par_c, h, :, :, :, at_cols(t)] = val[0:TS].astype(BF16).reshape(CHIPS, CORES, BR, NT)
                    DP[:, cols] = val[TS:TS + 8]
                    return 0

                lax.fori_loop(0, DH // NT, down_tile, 0)
                d_pr(par_c, h).start()

        @when(n < NS + 2)
        def _():
            for e in BOTH:
                pl.semaphore_signal(s_sync.at[e], inc=1, device_id=to_near[e], device_id_type=MESH)

        @when(live_1, fag_1)
        def _():
            for e in BOTH:
                d_g(s_1, par_1, e, e).wait_recv()
                d_r(s_1, par_1, e).start()

        @when(jnp.logical_or(r8 == 5, jnp.logical_and(r8 == 0, mc > 0)))
        def _():
            d_e(1).wait_recv()
            d_e(1).wait_send()
            EX[E_B] = EX[E_A] + EX[E_IN1]
            d_e(2).start()

        @when(live_c, r8 == 4)
        def _():
            for pr in BOTH:
                d_kv_all(lq_c, pr, pr).wait_send()
            for pr in BOTH:
                d_kv_all(lq_c, pr, pr).wait_recv()
            rows = lax.broadcasted_iota(jnp.int32, (DEC, hd), 0)
            outs = []
            for pr in BOTH:
                @when(lq_c > 0)
                def _():
                    cache_copy(lq_c - 1, pr).wait()

                both = jnp.zeros((DEC, hd), F32)
                for kv in BOTH:
                    new = QS[TS:TS + DEC, (G + kv) * hd:(G + kv + 1) * hd].astype(F32)
                    new = jnp.sum(jnp.where(rows == pr, new, 0.0), axis=0, keepdims=True)
                    KVR[lq_c, pr, kv, T:T + DEC, :] = jnp.where(rows == 0, new, 0.0).astype(BF16)
                    both = jnp.where(rows == kv, new, both)
                    Z32[pl.ds(kv, T, stride=2), :] = KVR[lq_c, pr, kv, 0:T, :].astype(F32)
                ZB[pr, 0:T] = Z32[...].astype(BF16).reshape(T, 2, hd)
                ZB[pr, T:T + DEC // 2] = both.astype(BF16).reshape(DEC // 2, 2, hd)
                cache_copy(lq_c, pr).start()
                q = jnp.concatenate([QS[TS:TS + DEC, g * hd:(g + 1) * hd] for g in range(G)], axis=0)
                scores = lax.dot_general(q, KVR[lq_c, pr, 0], (((1,), (1,)), ((), ())), preferred_element_type=F32) * scale
                kpos = lax.broadcasted_iota(jnp.int32, (G * DEC, T + PAD), 1)
                scores = jnp.where(kpos <= T, scores, -1e30)
                e = jnp.exp(scores - jnp.max(scores, axis=-1, keepdims=True))
                p = (e / jnp.sum(e, axis=-1, keepdims=True)).astype(BF16)
                outs.append(jnp.dot(p, KVR[lq_c, pr, 1], preferred_element_type=F32))
            picked = []
            for g in range(G):
                rest = jnp.where(rows == 1, outs[1][g * DEC:(g + 1) * DEC], 0.0)
                picked.append(jnp.where(rows == 0, outs[0][g * DEC:(g + 1) * DEC], rest).astype(BF16))
            od = jnp.concatenate(picked, axis=1)

            for t in range(D // NT):
                part = jnp.dot(od, WO[:, t * NT:(t + 1) * NT], preferred_element_type=F32)
                DP[:, t * NT:(t + 1) * NT] = part[0:8]
            decode_send()

            @when(lax.div(mc, 8) + 1 < L)
            def _():
                for w in wa_copies(lax.div(mc, 8) + 1):
                    w.start()

        @when(live_c, r8 == 7)
        def _():
            decode_send()

            @when(lax.div(mc, 8) + 1 < L)
            def _():
                for w in wm_copies(lax.div(mc, 8) + 1):
                    w.start()

        pieces(n - 2, pass_on)

        @when(n >= 0)
        def _():
            pieces(n + 1, lambda l, k, wide: d_fetch(l, k, wide).start())

        @when(n == -1)
        def _():
            for k in (3, 4):
                d_fetch(1, k, True).start()

        return 0

    lax.fori_loop(0, NS + 4, slot, 0)

    for i, ref in enumerate((fin_a, fin_b)):
        ref[...] = DY[i:i + 1, :]
    for pr in BOTH:
        cache_copy(L - 1, pr).wait()
    for s in range(STREAMS):
        for w in out_copies(s):
            w.wait()


def device_specs():
    row, whole, last = P(('pairs', 'ho')), P(), P(None, None, 'tp')
    in_specs = (P('pairs'), P('pairs'), row, row, last, P(None, 'tp'), last, last, P(None, 'tp'), whole, whole)
    cache = P(('pairs', 'ho'), None, None, None, 'tp')
    out_specs = (row, row, row, row, cache, cache)
    return in_specs, out_specs


def solution(mesh):
    n_ho, n_tp = mesh.shape['ho'], mesh.shape['tp']
    in_specs, out_specs = device_specs()

    def per_device(prompt_a, prompt_b, first_a, first_b, w_qkv, w_out, w_gate, w_up, w_down, norm_attn, norm_mlp):
        L, D = w_qkv.shape[0], w_qkv.shape[1]
        G, hd = w_out.shape[2], w_out.shape[3]
        F = w_gate.shape[2]
        T = prompt_a.shape[1]
        TS, DH = T // 2, D // 2
        BR = TS // n_tp
        wq = jnp.swapaxes(w_qkv[:, :, 0], 1, 2)
        wo = w_out.reshape(L, G * hd, D)
        any_spec = pl.BlockSpec(memory_space=pl.ANY)
        hbm_spec = pl.BlockSpec(memory_space=pltpu.HBM)
        vmem_spec = pl.BlockSpec(memory_space=pltpu.VMEM)
        dma = pltpu.SemaphoreType.DMA
        two, four, eight = (2, 2), (STREAMS,), (8,)
        by_stream = four + two[:1]
        flops = 2 * L * 2 * T * D * (wq.shape[1] * hd + G * hd + 3 * F)
        outs = pl.pallas_call(
            functools.partial(body, (n_ho, n_tp, L, T, D, G, hd, F)),
            name='serve',
            out_shape=(
                jax.ShapeDtypeStruct((T + DEC, D), BF16), jax.ShapeDtypeStruct((T + DEC, D), BF16),
                jax.ShapeDtypeStruct((1, D), F32), jax.ShapeDtypeStruct((1, D), F32),
                jax.ShapeDtypeStruct((L * (T + 1), 2, hd), BF16), jax.ShapeDtypeStruct((L * (T + 1), 2, hd), BF16)),
            in_specs=[hbm_spec] * 11,
            out_specs=(any_spec, any_spec, vmem_spec, vmem_spec, any_spec, any_spec),
            scratch_shapes=[
                pltpu.VMEM((STREAMS, TS + DEC, D), BF16),
                pltpu.VMEM((2, 2, CHIPS, CORES, BR, DH), BF16),
                pltpu.VMEM((2, 2, CHIPS, BR, DH), BF16),
                pltpu.VMEM((2, 2, BR, DH), BF16),
                pltpu.VMEM((STREAMS, 2, 2, BR, DH), BF16),
                pltpu.VMEM((STREAMS, BR, D), BF16),
                pltpu.VMEM((TS + DEC, (G + 2) * hd), BF16),
                pltpu.VMEM((2, 2, T, hd), BF16),
                pltpu.VMEM((TS, G * hd), BF16),
                pltpu.VMEM((TS + DEC, F), BF16),
                pltpu.VMEM((L, 2, 2, T + PAD, hd), BF16),
                pltpu.VMEM((D, (G + 2) * hd), BF16),
                pltpu.VMEM((G * hd, D), BF16),
                pltpu.VMEM((2, D, (G + 2) * hd), BF16),
                pltpu.VMEM((2, G * hd, D), BF16),
                pltpu.VMEM((G + 2, D // n_ho, hd), BF16),
                pltpu.VMEM((3, G * hd // n_ho // 3, D), BF16),
                pltpu.VMEM((D, F), BF16),
                pltpu.VMEM((D, F), BF16),
                pltpu.VMEM((F, D), BF16),
                pltpu.VMEM((L, D), F32),
                pltpu.VMEM((L, D), F32),
                pltpu.VMEM((2, 1, D), BF16),
                pltpu.VMEM((8, D), F32),
                pltpu.VMEM((8, D), F32),
                pltpu.VMEM((8, DH // (4 * hd), 8, hd), F32),
                pltpu.VMEM((2 * T, hd), F32),
                pltpu.VMEM((2, T + 8, 2, hd), BF16),
                *map(dma, (two, two, two, two)),
                *map(dma, (by_stream, by_stream, by_stream, by_stream)),
                *map(dma, (two + two[:1], two + two[:1], two, two)),
                *map(dma, (four, four)),
                *map(dma, (two[:1], (L,) + two[:1])),
                *map(dma, ((G + 3,), eight, (3,))),
                *map(dma, (by_stream, by_stream, two[:1])),
                *map(dma, (four, four, four)),
                *map(dma, (eight,) * 8),
                pltpu.SemaphoreType.REGULAR((2,)),
            ],
            compiler_params=pltpu.CompilerParams(
                collective_id=0, has_side_effects=True, vmem_limit_bytes=60 << 20),
            cost_estimate=pl.CostEstimate(flops=flops, bytes_accessed=flops // T, transcendentals=0),
        )(prompt_a, prompt_b, first_a, first_b, wq, wo, w_gate, w_up, w_down, norm_attn, norm_mlp)
        out_a, out_b, fin_a, fin_b, cache_a, cache_b = outs

        def cache(rows):
            return jnp.swapaxes(rows.reshape(L, T + 1, 2, hd), 1, 2)[None, :, :, :, None]

        return (out_a[None, :T], out_b[None, :T], fin_a, fin_b, cache(cache_a), cache(cache_b))

    return jax.shard_map(per_device, mesh=mesh, in_specs=in_specs, out_specs=out_specs, check_vma=False)
```

```python
import functools

import jax
import jax.numpy as jnp
from jax import lax
from jax.experimental import pallas as pl
from jax.experimental.pallas import tpu as pltpu
from jax.sharding import PartitionSpec as P

MESH = pl.DeviceIdType.MESH
F32 = jnp.float32
BF16 = jnp.bfloat16
CORES = 2
CHIPS = 4
BOTH = range(2)
STREAMS = 4
DEC = 16
PAD = 128


def tile_of(size, most):
    tile = most
    while size % tile:
        tile //= 2
    return tile


def body(cfg, pa, pb, fa, fb, wq, wo, wg, wu, wd, g1h, g2h, oa, ob, fin_a, fin_b, ca, cb,
         H, PB, PR, AR, BC, XR, QS, KV, OS, US, KVR, WQ, WO, WQF, WOF, XSQ, XSO, WG, WU, WD, g1, g2, FT, DY, DP, EX, Z32, ZB,
         s_prs, s_prr, s_as, s_ar, s_bs, s_br, s_cs, s_cr, s_gs, s_gr, s_rs, s_rr, s_ds, s_dr,
         s_kvs, s_kvr, s_wa, s_ps, s_wm, s_in, s_out, s_ko, s_es, s_er, s_sm,
         s_xs, s_xr, s_us, s_ur, s_ls, s_lr, s_ys, s_yr, s_sync):
    n_ho, n_tp, L, T, D, G, hd, F = cfg
    TS = T // 2
    HS = TS // 2
    BR = TS // n_tp
    DH = D // 2
    NS = 8 * L
    NT4 = EX.shape[1]
    DQ = D // n_ho
    OQ = G * hd // n_ho
    OC = OQ // 3
    scale = hd ** -0.5
    j = lax.axis_index('ho')
    tp = lax.axis_index('tp')
    X = lax.div(tp, CORES)
    c = lax.rem(tp, CORES)
    Q = CHIPS - 1 - X
    V = X + 1 - 2 * lax.rem(X, 2)
    O = CHIPS - 1 - V
    near = (Q, V)

    def pos(Y):
        return 2 * lax.rem(lax.div(Y + 1, 2), 2) + lax.div(Y, 2)

    pX, pQ, pV, pO = pos(X), pos(Q), pos(V), pos(O)
    pN = (pQ, pV)
    hp = lax.div(pX, 2)
    to_near = ({'tp': Q * CORES + c}, {'tp': V * CORES + c})
    to_partner = {'tp': X * CORES + (1 - c)}
    up = lax.rem(j + 1, n_ho)
    down = lax.rem(j + n_ho - 1, n_ho)

    def rc(src, dst, ss, rs, dev):
        return pltpu.make_async_remote_copy(src_ref=src, dst_ref=dst, send_sem=ss, recv_sem=rs,
                                            device_id=dev, device_id_type=MESH)

    def lc(src, dst, sem):
        return pltpu.make_async_copy(src, dst, sem)

    def rows_of(p):
        return pl.ds(pl.multiple_of((p * CORES + c) * BR, BR), BR)

    def d_pr(par, h):
        return rc(PB.at[par, h, :, 1 - c], PR.at[par, h], s_prs.at[par, h], s_prr.at[par, h], to_partner)

    def d_pr_home(par, h):
        return rc(PB.at[par, h, pl.ds(hp * 2, 2), 1 - c], PR.at[par, h, pl.ds(hp * 2, 2)],
                  s_prs.at[par, h], s_prr.at[par, h], to_partner)

    def d_a(par, e, heavy=False):
        return rc(PB.at[par, e, pO, c], AR.at[par, e], s_as.at[par, e], s_ar.at[par, e], to_near[0 if heavy else e])

    def d_b(par, s, e):
        return rc(PB.at[par, e, pN[e], c], BC.at[s, e, e], s_bs.at[s, e], s_br.at[s, e], to_near[e])

    def d_c(par, s, e):
        return rc(PB.at[par, 1 - e, pN[e], c], BC.at[s, e, 1 - e], s_cs.at[s, e], s_cr.at[s, e], to_near[e])

    def h_part(s, p, half):
        return H.at[s, rows_of(p), pl.ds(half * DH, DH)]

    def d_g(s, e, half):
        return rc(h_part(s, pX, half), h_part(s, pX, half), s_gs.at[s, e, half], s_gr.at[s, e, half], to_near[e])

    def d_r(s, e):
        return rc(h_part(s, pN[e], e), h_part(s, pN[e], e), s_rs.at[s, e], s_rr.at[s, e], to_near[1 - e])

    def d_d(s, p):
        return rc(H.at[s, rows_of(p)], H.at[s, rows_of(p)], s_ds.at[s], s_dr.at[s], to_partner)

    def d_d_all(s, blocks):
        return rc(H.at[s, pl.ds(0, blocks * BR)], H.at[s, pl.ds(0, blocks * BR)], s_ds.at[s], s_dr.at[s], to_partner)

    def quarter(s):
        return pl.ds(pl.multiple_of(s * HS, HS), HS)

    def d_kv(l, f, pr, s, dev):
        return rc(KV.at[f, :, quarter(s)], KVR.at[l, pr, :, quarter(s)], s_kvs.at[f], s_kvr.at[l, pr], dev)

    def d_kv_all(l, f, pr):
        return rc(KV.at[f], KVR.at[l, pr, :, pl.ds(0, T)], s_kvs.at[f], s_kvr.at[l, pr], to_partner)

    E_OUT, E_IN0, E_A, E_IN1, E_B, E_IN2, E_C, E_IN3 = range(8)

    def d_e(step):
        src, dst, dev = ((E_OUT, E_IN0, to_partner), (E_A, E_IN1, to_near[1]), (E_B, E_IN2, to_near[0]),
                         (E_C, E_IN3, to_partner))[step]
        return rc(EX.at[src], EX.at[dst], s_es.at[step], s_er.at[step], dev)

    def cache_copy(l, pr):
        return lc(ZB.at[pr, pl.ds(0, T + 1)], (cb if pr else ca).at[pl.ds(l * (T + 1), T + 1)], s_ko.at[pr])

    def piece(l, k, wide, r):
        par = lax.rem(l, 2)
        if wide:
            return WQF.at[par, k, pl.ds(pl.multiple_of(r * DQ, DQ), DQ), :]
        return WOF.at[par, pl.ds(pl.multiple_of(r * OQ + (k - (G + 2)) * OC, OC), OC), :]

    def fetched(k, wide):
        return XSQ.at[k] if wide else XSO.at[k - (G + 2)]

    def d_fetch(l, k, wide):
        if wide:
            src = wq.at[l, k, pl.ds(pl.multiple_of(j * DQ, DQ), DQ), :]
        else:
            src = wo.at[l, pl.ds(pl.multiple_of(j * OQ + (k - (G + 2)) * OC, OC), OC), :]
        return lc(src, fetched(k, wide), s_ps.at[k])

    def d_x(l, k, wide):
        return rc(fetched(k, wide), piece(l, k, wide, j), s_xs.at[k], s_xr.at[k], to_near[1])

    def d_up(l, k, wide, r):
        return rc(piece(l, k, wide, r), piece(l, k, wide, r), s_us.at[k], s_ur.at[k], {'ho': up})

    def d_down(l, k, wide, r):
        return rc(piece(l, k, wide, r), piece(l, k, wide, r), s_ls.at[k], s_lr.at[k], {'ho': down})

    def d_on(l, k, wide, r, dev):
        return rc(piece(l, k, wide, r), piece(l, k, wide, r), s_ys.at[k], s_yr.at[k], dev)

    def wa_copies(l):
        out = [lc(wq.at[l, i], WQ.at[:, pl.ds(i * hd, hd)], s_wa.at[i]) for i in range(G + 2)]
        return out + [lc(wo.at[l], WO, s_wa.at[G + 2])]

    def wm_copies(l):
        return [lc(src.at[l], dst, s_wm.at[i]) for i, (src, dst) in enumerate(((wg, WG), (wu, WU), (wd, WD)))]

    def prompt_copies(s):
        return [lc(p.at[j, pl.ds(s * HS, HS)], H.at[s, pl.ds(i * HS, HS)], s_in.at[s, i]) for i, p in enumerate((pa, pb))]

    def out_copies(s):
        return [lc(H.at[s, pl.ds(i * HS, HS)], o.at[pl.ds(s * HS, HS)], s_out.at[s, i]) for i, o in enumerate((oa, ob))]

    small = [lc(src, dst, s_sm.at[i])
             for i, (src, dst) in enumerate(((g1h, g1), (g2h, g2), (fa, FT.at[0]), (fb, FT.at[1])))]

    barrier = pltpu.get_barrier_semaphore()
    met = [to_partner, to_near[0], to_near[1], {'ho': up}, {'ho': down},
           {'ho': up, 'tp': V * CORES + c}, {'ho': down, 'tp': V * CORES + c}]
    for dev in met:
        pl.semaphore_signal(barrier, inc=1, device_id=dev, device_id_type=MESH)

    for w in prompt_copies(0) + small + [d_fetch(1, k, True) for k in range(3)] + wa_copies(0):
        w.start()

    def normed(xf, gain):
        ms = jnp.mean(xf * xf, axis=-1, keepdims=True)
        return xf * lax.rsqrt(ms + 1e-5) * gain

    def decode_norm(gain):
        h = normed(DY[...], gain)
        H[STREAMS - 1, TS:TS + DEC, :] = jnp.concatenate([h, jnp.zeros_like(h)], axis=0).astype(BF16)

    for w in small:
        w.wait()
    DY[...] = jnp.zeros(DY.shape, F32)
    for i in BOTH:
        DY[i:i + 1, :] = FT[i].astype(F32)
    decode_norm(g1[0:1, :])
    pl.semaphore_wait(barrier, len(met))

    def slot(it, _):
        n = it - 1
        m1, m2, m3, mc = n - 1, n - 2, n - 3, n + 1

        def state(m):
            live = jnp.logical_and(m >= 0, m < NS)
            r = lax.rem(m + 16, 8)
            full_rs = jnp.logical_or(m < 8, r >= 4)
            full_ag = jnp.logical_or(r < 4, m >= NS - STREAMS)
            return live, full_rs, full_ag

        def when(*conds):
            out = conds[0]
            for x in conds[1:]:
                out = jnp.logical_and(out, x)
            return pl.when(out)

        live_n, frs_n, _ = state(n)
        live_1, frs_1, fag_1 = state(m1)
        live_2, _, fag_2 = state(m2)
        live_3, _, fag_3 = state(m3)
        live_c, frs_c, _ = state(mc)
        heavy = jnp.logical_and(n >= 0, n < STREAMS)
        par_n, par_1 = lax.rem(n + 8, 2), lax.rem(m1 + 8, 2)
        s_n, s_1, s_2, s_3 = (lax.rem(m + 8, STREAMS) for m in (n, m1, m2, m3))

        def pieces(t, fn, first=0):
            r = lax.rem(t + 8, 8)

            @when(t == first)
            def _():
                for k in range(3):
                    fn(1, k, True)

            @when(t >= 0, r == 0, lax.div(t, 8) + 1 < L)
            def _():
                for k in (3, 4):
                    fn(lax.div(t, 8) + 1, k, True)

            @when(t >= 0, r >= 1, r <= 3, lax.div(t, 8) + 1 < L)
            def _():
                fn(lax.div(t, 8) + 1, 4 + r, False)

            @when(t >= 0, r >= 5, lax.div(t, 8) + 2 < L)
            def _():
                fn(lax.div(t, 8) + 2, r - 5, True)

        def by_parity(k, even, odd):
            if isinstance(k, int):
                (odd if k % 2 else even)()
            else:
                when(lax.rem(k, 2) == 0)(even)
                when(lax.rem(k, 2) == 1)(odd)

        def arrived(l, k, wide):
            opposite = lax.rem(j + 2, n_ho)
            d_on(l, k, wide, opposite, {'ho': up}).wait_recv()
            d_on(l, k, wide, opposite, {'ho': up}).wait_send()

        def pass_on(l, k, wide):
            d_up(l, k, wide, j).wait_recv()
            d_down(l, k, wide, j).wait_recv()
            by_parity(k, lambda: d_on(l, k, wide, down, {'ho': up}).start(),
                      lambda: d_on(l, k, wide, up, {'ho': down}).start())
            d_up(l, k, wide, j).wait_send()
            d_down(l, k, wide, j).wait_send()

        def spread(l, k, wide):
            d_x(l, k, wide).wait_recv()
            d_up(l, k, wide, j).start()
            d_down(l, k, wide, j).start()
            d_x(l, k, wide).wait_send()

        def send_over(l, k, wide):
            d_fetch(l, k, wide).wait()
            d_x(l, k, wide).start()

        pieces(n, send_over, -1)
        pieces(n + 1, lambda l, k, wide: d_fetch(l, k, wide).start(), -1)

        def add(h, p):
            PB[par_n, h, p, c] = PB[par_n, h, p, c] + PR[par_n, h, p]

        @when(live_n, frs_n)
        def _():
            for h in BOTH:
                d_pr(par_n, h).wait_recv()
            for e in BOTH:
                add(e, pO)

            @when(jnp.logical_not(heavy))
            def _():
                for e in BOTH:
                    d_a(par_n, e).start()
                for e in BOTH:
                    add(e, pN[e])
                for e in BOTH:
                    d_b(par_n, s_n, e).start()
                for e in BOTH:
                    add(1 - e, pN[e])

            @when(heavy)
            def _():
                for e in BOTH:
                    d_a(par_n, e, True).start()
                for e in BOTH:
                    add(e, pQ)
                d_b(par_n, s_n, 0).start()
                d_c(par_n, s_n, 0).start()
                for e in BOTH:
                    add(e, pV)

            for e in BOTH:
                add(e, pX)

        @when(live_n, jnp.logical_not(frs_n))
        def _():
            for h in BOTH:
                d_pr_home(par_n, h).wait_recv()
            for h in BOTH:
                add(h, pQ)
            d_b(par_n, s_n, 0).start()
            d_c(par_n, s_n, 0).start()
            for h in BOTH:
                add(h, pX)

        @when(live_1)
        def _():
            l = lax.div(m1, 8)
            is_attn = lax.rem(lax.div(m1, 4), 2) == 0
            last = m1 >= NS - STREAMS
            d_b(par_1, s_1, 0).wait_recv()
            d_c(par_1, s_1, 0).wait_recv()

            @when(frs_1)
            def _():
                d_b(par_1, s_1, 1).wait_recv()
                d_c(par_1, s_1, 1).wait_recv()

            x_new = []
            ms = jnp.zeros((BR, 1), F32)
            for h in BOTH:
                second = jnp.where(frs_1, BC[s_1, 1, h].astype(F32), 0.0)
                total = PB[par_1, h, pX, c].astype(F32) + (BC[s_1, 0, h].astype(F32) + second)
                cols = slice(h * DH, (h + 1) * DH)
                x = XR[s_1, :, cols].astype(F32) + total.astype(BF16).astype(F32)
                x = x.astype(BF16)
                XR[s_1, :, cols] = x
                x = x.astype(F32)
                ms = ms + jnp.sum(x * x, axis=-1, keepdims=True)
                x_new.append(x)
            inv = lax.rsqrt(ms * (1.0 / D) + 1e-5)
            nl = jnp.minimum(l + 1, L - 1)
            for h in BOTH:
                cols = slice(h * DH, (h + 1) * DH)
                gain = jnp.where(is_attn, g2[pl.ds(l, 1), cols], g1[pl.ds(nl, 1), cols])
                hn = x_new[h] * inv * gain
                H[s_1, rows_of(pX), cols] = jnp.where(last, x_new[h], hn).astype(BF16)

            d_g(s_1, 0, 0).start()

            @when(fag_1)
            def _():
                d_g(s_1, 1, 1).start()

            d_g(s_1, 0, 1).start()

            @when(fag_1)
            def _():
                d_g(s_1, 1, 0).start()

            d_d(s_1, pX).start()

        @when(live_1)
        def _():
            d_b(par_1, s_1, 0).wait_send()
            d_c(par_1, s_1, 0).wait_send()

            @when(frs_1)
            def _():
                for h in BOTH:
                    d_pr(par_1, h).wait_send()
                for e in BOTH:
                    d_a(par_1, e).wait_send()
                d_b(par_1, s_1, 1).wait_send()
                d_c(par_1, s_1, 1).wait_send()

            @when(jnp.logical_not(frs_1))
            def _():
                for h in BOTH:
                    d_pr_home(par_1, h).wait_send()

        for full, blocks in ((True, CHIPS), (False, CHIPS // 2)):
            @when(live_3, fag_3 if full else jnp.logical_not(fag_3))
            def _():
                d_d_all(s_3, blocks).wait_recv()
                d_d_all(s_3, blocks).wait_send()

        for s in range(STREAMS):
            @when(m3 == NS - STREAMS + s)
            def _():
                for w in out_copies(s):
                    w.start()

        pieces(n - 4, arrived)
        pieces(n - 1, spread)

        @when(n == 0)
        def _():
            def zero(l, _):
                for pr in BOTH:
                    for kv in BOTH:
                        KVR[l, pr, kv, T:T + PAD, :] = jnp.zeros((PAD, hd), BF16)
                return 0

            lax.fori_loop(0, L, zero, 0)

        r8 = lax.rem(mc, 8)
        rows8 = lax.broadcasted_iota(jnp.int32, (8, hd), 0)

        def half_cols(half, k):
            return pl.ds(pl.multiple_of(half * DH + k * hd, hd), hd)

        def decode_send():
            for slot_, half in ((E_OUT, 1 - c), (E_A, c)):
                for t in range(NT4):
                    acc = DP[:, half_cols(half, 4 * t)]
                    for q in range(1, 4):
                        acc = acc + pltpu.roll(DP[:, half_cols(half, 4 * t + q)], 2 * q, axis=0)
                    EX[slot_, t] = acc
            d_e(0).start()

        @when(jnp.logical_or(r8 == 5, jnp.logical_and(r8 == 0, mc > 0)))
        def _():
            d_e(0).wait_recv()
            d_e(0).wait_send()
            EX[E_A] = EX[E_A] + EX[E_IN0]
            d_e(1).start()

        @when(jnp.logical_or(r8 == 6, jnp.logical_and(r8 == 1, mc > 8)))
        def _():
            d_e(1).wait_recv()
            d_e(1).wait_send()
            EX[E_B] = EX[E_A] + EX[E_IN1]
            d_e(2).start()

        @when(jnp.logical_or(r8 == 7, jnp.logical_and(r8 == 2, mc > 8)))
        def _():
            d_e(3).wait_recv()
            d_e(3).wait_send()
            for slot_, half in ((E_C, c), (E_IN3, 1 - c)):
                for t in range(NT4):
                    block = EX[slot_, t]
                    for q in range(4):
                        part = block if q == 0 else pltpu.roll(block, 8 - 2 * q, axis=0)
                        cols = half_cols(half, 4 * t + q)
                        DY[:, cols] = DY[:, cols] + jnp.where(rows8 < 2, part, 0.0)
            lq = lax.div(mc, 8)

            @when(r8 == 7)
            def _():
                decode_norm(g2[pl.ds(lq, 1), :])

            @when(r8 == 2, mc < NS)
            def _():
                decode_norm(g1[pl.ds(jnp.minimum(lq, L - 1), 1), :])

        par_c = lax.rem(mc, 2)
        sc = lax.rem(mc, STREAMS)
        lq_c = jnp.minimum(lax.div(mc, 8), L - 1)
        attn_c = jnp.logical_and(live_c, r8 < 4)
        mlp_c = jnp.logical_and(live_c, r8 >= 4)

        for s in range(STREAMS):
            @when(mc == s)
            def _():
                for w in prompt_copies(s):
                    w.wait()

                def first_rows(i, _):
                    rows = pl.ds(pl.multiple_of(i * BR, BR), BR)
                    hn = normed(H[s, rows, :].astype(F32), g1[0:1, :])
                    H[s, rows, :] = hn.astype(BF16)
                    return 0

                XR[s] = H[s, rows_of(pX), :]
                lax.fori_loop(0, n_tp, first_rows, 0)

        NQKV = (G + 2) * hd

        def qkv_tiles(fn):
            c0 = 0
            while c0 < NQKV:
                c1 = min(c0 + 2 * hd, NQKV)
                fn(c0, c1)
                c0 = c1

        @when(attn_c)
        def _():
            @when(sc == 0)
            def _():
                for w in wa_copies(lq_c):
                    w.wait()

                @when(mc == 0)
                def _():
                    for s in range(1, STREAMS):
                        for w in prompt_copies(s):
                            w.start()
                    for w in wm_copies(0):
                        w.start()

            @when(mc < 8)
            def _():
                def go(c0, c1):
                    QS[:, c0:c1] = jnp.dot(H[sc], WQ[:, c0:c1], preferred_element_type=F32).astype(BF16)

                qkv_tiles(go)

            @when(mc >= 8)
            def _():
                home = pl.ds(pl.multiple_of(hp * HS, HS), HS)
                lpar = lax.rem(lq_c, 2)

                def go(c0, c1):
                    other = jnp.concatenate([WQF[lpar, i] for i in range(c0 // hd, c1 // hd)], axis=1)
                    for f, w in enumerate((WQ[:, c0:c1], other)):
                        QS[f * HS:(f + 1) * HS, c0:c1] = jnp.dot(
                            H[sc, home, :], w, preferred_element_type=F32).astype(BF16)

                qkv_tiles(go)

                @when(sc == STREAMS - 1)
                def _():
                    def dec(c0, c1):
                        QS[TS:TS + DEC, c0:c1] = jnp.dot(
                            H[STREAMS - 1, TS:TS + DEC, :], WQ[:, c0:c1], preferred_element_type=F32).astype(BF16)

                    qkv_tiles(dec)

            for f in BOTH:
                for kv in BOTH:
                    KV[f, kv, quarter(sc), :] = QS[f * HS:(f + 1) * HS, (G + kv) * hd:(G + kv + 1) * hd]

            @when(mc < 8)
            def _():
                for f in BOTH:
                    d_kv(lq_c, f, f, sc, {'ho': up}).start()

            @when(mc >= 8)
            def _():
                d_kv(lq_c, 0, hp, sc, {'ho': up}).start()
                d_kv(lq_c, 1, hp, sc, {'ho': up, 'tp': V * CORES + c}).start()

            for s in range(STREAMS):
                @when(sc == s)
                def _():
                    keys = (s + 1) * HS

                    def attn_tile(i, _):
                        g = lax.div(i, CORES)
                        f = lax.rem(i, CORES)
                        rows = pl.ds(pl.multiple_of(f * HS, HS), HS)
                        cols = pl.ds(pl.multiple_of(g * hd, hd), hd)
                        scores = lax.dot_general(QS[rows, cols], KV[f, 0, 0:keys, :], (((1,), (1,)), ((), ())),
                                                 preferred_element_type=F32) * scale
                        qpos = s * HS + lax.broadcasted_iota(jnp.int32, (HS, keys), 0)
                        kpos = lax.broadcasted_iota(jnp.int32, (HS, keys), 1)
                        scores = jnp.where(qpos >= kpos, scores, -1e30)
                        e = jnp.exp(scores - jnp.max(scores, axis=-1, keepdims=True))
                        p = (e / jnp.sum(e, axis=-1, keepdims=True)).astype(BF16)
                        OS[rows, cols] = jnp.dot(p, KV[f, 1, 0:keys, :], preferred_element_type=F32).astype(BF16)
                        return 0

                    lax.fori_loop(0, CORES * G, attn_tile, 0)

        UT = tile_of(F, 256)

        @when(mlp_c)
        def _():
            @when(sc == 0)
            def _():
                for w in wm_copies(lq_c):
                    w.wait()

            def gate_up(i, _):
                cols = pl.ds(pl.multiple_of(i * UT, UT), UT)
                gate = jnp.dot(H[sc], WG[:, cols], preferred_element_type=F32)
                up_ = jnp.dot(H[sc], WU[:, cols], preferred_element_type=F32)
                US[:, cols] = (gate * (1.0 / (1.0 + jnp.exp(-gate))) * up_).astype(BF16)
                return 0

            lax.fori_loop(0, F // UT, gate_up, 0)

        @when(live_n, frs_n, jnp.logical_not(heavy))
        def _():
            for e in BOTH:
                d_a(par_n, e).wait_recv()
                PB[par_n, e, pN[1 - e], c] = PB[par_n, e, pN[1 - e], c] + AR[par_n, e]
            for e in BOTH:
                d_c(par_n, s_n, 1 - e).start()

        @when(heavy)
        def _():
            for e in BOTH:
                d_a(par_n, e, True).wait_recv()
                PB[par_n, e, pV, c] = PB[par_n, e, pV, c] + AR[par_n, e]
            d_c(par_n, s_n, 1).start()
            d_b(par_n, s_n, 1).start()

        @when(live_2)
        def _():
            d_g(s_2, 0, 1).wait_recv()

            @when(jnp.logical_not(fag_2))
            def _():
                d_g(s_2, 0, 0).wait_recv()

            d_d(s_2, pQ).start()

            @when(fag_2)
            def _():
                d_g(s_2, 1, 0).wait_recv()
                d_d(s_2, pV).start()
                for e in BOTH:
                    d_r(s_2, e).wait_recv()
                d_d(s_2, pO).start()
                for half in BOTH:
                    d_g(s_2, 1, half).wait_send()
                for e in BOTH:
                    d_r(s_2, e).wait_send()

            for half in BOTH:
                d_g(s_2, 0, half).wait_send()

        NT = tile_of(DH, 512)

        def at_cols(t):
            return pl.ds(pl.multiple_of(t * NT, NT), NT)

        @when(attn_c, mc < 8)
        def _():
            for h in BOTH:
                def out_tile(t, _):
                    cols = pl.ds(pl.multiple_of(h * DH + t * NT, NT), NT)
                    val = jnp.dot(OS[...], WO[:, cols], preferred_element_type=F32)
                    PB[par_c, h, :, :, :, at_cols(t)] = val.astype(BF16).reshape(CHIPS, CORES, BR, NT)
                    return 0

                lax.fori_loop(0, DH // NT, out_tile, 0)
                d_pr(par_c, h).start()

        @when(attn_c, mc >= 8)
        def _():
            for h in BOTH:
                def out_tile(t, _):
                    cols = pl.ds(pl.multiple_of(h * DH + t * NT, NT), NT)
                    val = jnp.dot(OS[0:HS, :], WO[:, cols], preferred_element_type=F32)
                    val = val + jnp.dot(OS[HS:TS, :], WOF[lax.rem(lq_c, 2), :, cols], preferred_element_type=F32)
                    PB[par_c, h, pl.ds(hp * 2, 2), :, :, at_cols(t)] = val.astype(BF16).reshape(2, CORES, BR, NT)
                    return 0

                lax.fori_loop(0, DH // NT, out_tile, 0)
                d_pr_home(par_c, h).start()

        @when(mlp_c)
        def _():
            for h in BOTH:
                def down_tile(t, _):
                    cols = pl.ds(pl.multiple_of(h * DH + t * NT, NT), NT)
                    val = jnp.dot(US[...], WD[:, cols], preferred_element_type=F32)
                    PB[par_c, h, :, :, :, at_cols(t)] = val[0:TS].astype(BF16).reshape(CHIPS, CORES, BR, NT)
                    DP[:, cols] = val[TS:TS + 8]
                    return 0

                lax.fori_loop(0, DH // NT, down_tile, 0)
                d_pr(par_c, h).start()

        @when(n < NS + 2)
        def _():
            for e in BOTH:
                pl.semaphore_signal(s_sync.at[e], inc=1, device_id=to_near[e], device_id_type=MESH)

        @when(live_1, fag_1)
        def _():
            for e in BOTH:
                d_g(s_1, e, e).wait_recv()
                d_r(s_1, e).start()

        @when(jnp.logical_or(r8 == 6, jnp.logical_and(r8 == 1, mc > 8)))
        def _():
            d_e(2).wait_recv()
            d_e(2).wait_send()
            EX[E_C] = EX[E_B] + EX[E_IN2]
            d_e(3).start()

        @when(live_c, r8 == 4)
        def _():
            for pr in BOTH:
                d_kv_all(lq_c, pr, pr).wait_send()
            for pr in BOTH:
                d_kv_all(lq_c, pr, pr).wait_recv()
            rows = lax.broadcasted_iota(jnp.int32, (DEC, hd), 0)
            outs = []
            for pr in BOTH:
                @when(lq_c > 0)
                def _():
                    cache_copy(lq_c - 1, pr).wait()

                both = jnp.zeros((DEC, hd), F32)
                for kv in BOTH:
                    new = QS[TS:TS + DEC, (G + kv) * hd:(G + kv + 1) * hd].astype(F32)
                    new = jnp.sum(jnp.where(rows == pr, new, 0.0), axis=0, keepdims=True)
                    KVR[lq_c, pr, kv, T:T + DEC, :] = jnp.where(rows == 0, new, 0.0).astype(BF16)
                    both = jnp.where(rows == kv, new, both)
                    Z32[pl.ds(kv, T, stride=2), :] = KVR[lq_c, pr, kv, 0:T, :].astype(F32)
                ZB[pr, 0:T] = Z32[...].astype(BF16).reshape(T, 2, hd)
                ZB[pr, T:T + DEC // 2] = both.astype(BF16).reshape(DEC // 2, 2, hd)
                cache_copy(lq_c, pr).start()
                q = jnp.concatenate([QS[TS:TS + DEC, g * hd:(g + 1) * hd] for g in range(G)], axis=0)
                scores = lax.dot_general(q, KVR[lq_c, pr, 0], (((1,), (1,)), ((), ())), preferred_element_type=F32) * scale
                kpos = lax.broadcasted_iota(jnp.int32, (G * DEC, T + PAD), 1)
                scores = jnp.where(kpos <= T, scores, -1e30)
                e = jnp.exp(scores - jnp.max(scores, axis=-1, keepdims=True))
                p = (e / jnp.sum(e, axis=-1, keepdims=True)).astype(BF16)
                outs.append(jnp.dot(p, KVR[lq_c, pr, 1], preferred_element_type=F32))
            picked = []
            for g in range(G):
                rest = jnp.where(rows == 1, outs[1][g * DEC:(g + 1) * DEC], 0.0)
                picked.append(jnp.where(rows == 0, outs[0][g * DEC:(g + 1) * DEC], rest).astype(BF16))
            od = jnp.concatenate(picked, axis=1)

            for t in range(D // NT):
                part = jnp.dot(od, WO[:, t * NT:(t + 1) * NT], preferred_element_type=F32)
                DP[:, t * NT:(t + 1) * NT] = part[0:8]
            decode_send()

            @when(lax.div(mc, 8) + 1 < L)
            def _():
                for w in wa_copies(lax.div(mc, 8) + 1):
                    w.start()

        @when(live_c, r8 == 7)
        def _():
            decode_send()

            @when(lax.div(mc, 8) + 1 < L)
            def _():
                for w in wm_copies(lax.div(mc, 8) + 1):
                    w.start()

        pieces(n - 2, pass_on)

        @when(n >= 0)
        def _():
            for e in BOTH:
                pl.semaphore_wait(s_sync.at[e], 1)

        return 0

    lax.fori_loop(0, NS + 4, slot, 0)

    for i, ref in enumerate((fin_a, fin_b)):
        ref[...] = DY[i:i + 1, :]
    for pr in BOTH:
        cache_copy(L - 1, pr).wait()
    for s in range(STREAMS):
        for w in out_copies(s):
            w.wait()


def device_specs():
    row, whole, last = P(('pairs', 'ho')), P(), P(None, None, 'tp')
    in_specs = (P('pairs'), P('pairs'), row, row, last, P(None, 'tp'), last, last, P(None, 'tp'), whole, whole)
    cache = P(('pairs', 'ho'), None, None, None, 'tp')
    out_specs = (row, row, row, row, cache, cache)
    return in_specs, out_specs


def solution(mesh):
    n_ho, n_tp = mesh.shape['ho'], mesh.shape['tp']
    in_specs, out_specs = device_specs()

    def per_device(prompt_a, prompt_b, first_a, first_b, w_qkv, w_out, w_gate, w_up, w_down, norm_attn, norm_mlp):
        L, D = w_qkv.shape[0], w_qkv.shape[1]
        G, hd = w_out.shape[2], w_out.shape[3]
        F = w_gate.shape[2]
        T = prompt_a.shape[1]
        TS, DH = T // 2, D // 2
        BR = TS // n_tp
        wq = jnp.swapaxes(w_qkv[:, :, 0], 1, 2)
        wo = w_out.reshape(L, G * hd, D)
        any_spec = pl.BlockSpec(memory_space=pl.ANY)
        hbm_spec = pl.BlockSpec(memory_space=pltpu.HBM)
        vmem_spec = pl.BlockSpec(memory_space=pltpu.VMEM)
        dma = pltpu.SemaphoreType.DMA
        two, four, eight = (2, 2), (STREAMS,), (8,)
        by_stream = four + two[:1]
        flops = 2 * L * 2 * T * D * (wq.shape[1] * hd + G * hd + 3 * F)
        outs = pl.pallas_call(
            functools.partial(body, (n_ho, n_tp, L, T, D, G, hd, F)),
            name='serve',
            out_shape=(
                jax.ShapeDtypeStruct((T + DEC, D), BF16), jax.ShapeDtypeStruct((T + DEC, D), BF16),
                jax.ShapeDtypeStruct((1, D), F32), jax.ShapeDtypeStruct((1, D), F32),
                jax.ShapeDtypeStruct((L * (T + 1), 2, hd), BF16), jax.ShapeDtypeStruct((L * (T + 1), 2, hd), BF16)),
            in_specs=[hbm_spec] * 11,
            out_specs=(any_spec, any_spec, vmem_spec, vmem_spec, any_spec, any_spec),
            scratch_shapes=[
                pltpu.VMEM((STREAMS, TS + DEC, D), BF16),
                pltpu.VMEM((2, 2, CHIPS, CORES, BR, DH), BF16),
                pltpu.VMEM((2, 2, CHIPS, BR, DH), BF16),
                pltpu.VMEM((2, 2, BR, DH), BF16),
                pltpu.VMEM((STREAMS, 2, 2, BR, DH), BF16),
                pltpu.VMEM((STREAMS, BR, D), BF16),
                pltpu.VMEM((TS + DEC, (G + 2) * hd), BF16),
                pltpu.VMEM((2, 2, T, hd), BF16),
                pltpu.VMEM((TS, G * hd), BF16),
                pltpu.VMEM((TS + DEC, F), BF16),
                pltpu.VMEM((L, 2, 2, T + PAD, hd), BF16),
                pltpu.VMEM((D, (G + 2) * hd), BF16),
                pltpu.VMEM((G * hd, D), BF16),
                pltpu.VMEM((2, G + 2, D, hd), BF16),
                pltpu.VMEM((2, G * hd, D), BF16),
                pltpu.VMEM((G + 2, D // n_ho, hd), BF16),
                pltpu.VMEM((3, G * hd // n_ho // 3, D), BF16),
                pltpu.VMEM((D, F), BF16),
                pltpu.VMEM((D, F), BF16),
                pltpu.VMEM((F, D), BF16),
                pltpu.VMEM((L, D), F32),
                pltpu.VMEM((L, D), F32),
                pltpu.VMEM((2, 1, D), BF16),
                pltpu.VMEM((8, D), F32),
                pltpu.VMEM((8, D), F32),
                pltpu.VMEM((8, DH // (4 * hd), 8, hd), F32),
                pltpu.VMEM((2 * T, hd), F32),
                pltpu.VMEM((2, T + 8, 2, hd), BF16),
                *map(dma, (two, two, two, two)),
                *map(dma, (by_stream, by_stream, by_stream, by_stream)),
                *map(dma, (by_stream + two[:1], by_stream + two[:1], by_stream, by_stream)),
                *map(dma, (four, four)),
                *map(dma, (two[:1], (L,) + two[:1])),
                *map(dma, ((G + 3,), eight, (3,))),
                *map(dma, (by_stream, by_stream, two[:1])),
                *map(dma, (four, four, four)),
                *map(dma, (eight,) * 8),
                pltpu.SemaphoreType.REGULAR((2,)),
            ],
            compiler_params=pltpu.CompilerParams(
                collective_id=0, has_side_effects=True, vmem_limit_bytes=60 << 20),
            cost_estimate=pl.CostEstimate(flops=flops, bytes_accessed=flops // T, transcendentals=0),
        )(prompt_a, prompt_b, first_a, first_b, wq, wo, w_gate, w_up, w_down, norm_attn, norm_mlp)
        out_a, out_b, fin_a, fin_b, cache_a, cache_b = outs

        def cache(rows):
            return jnp.swapaxes(rows.reshape(L, T + 1, 2, hd), 1, 2)[None, :, :, :, None]

        return (out_a[None, :T], out_b[None, :T], fin_a, fin_b, cache(cache_a), cache(cache_b))

    return jax.shard_map(per_device, mesh=mesh, in_specs=in_specs, out_specs=out_specs, check_vma=False)
```

```python
import functools

import jax
import jax.numpy as jnp
from jax import lax
from jax.experimental import pallas as pl
from jax.experimental.pallas import tpu as pltpu
from jax.sharding import PartitionSpec as P

MESH = pl.DeviceIdType.MESH
F32 = jnp.float32
BF16 = jnp.bfloat16
CORES = 2
CHIPS = 4
BOTH = range(2)
STREAMS = 4
DEC = 16
PAD = 128


def tile_of(size, most):
    tile = most
    while size % tile:
        tile //= 2
    return tile


def body(cfg, pa, pb, fa, fb, wq, wo, wg, wu, wd, g1h, g2h, oa, ob, fin_a, fin_b, ca, cb,
         H, PB, PR, AR, BC, XR, QS, KV, OS, US, KVR, WQ, WO, WQF, WOF, XSQ, XSO, WG, WU, WD, g1, g2, FT, DY, DP, EX, Z32, ZB,
         s_prs, s_prr, s_as, s_ar, s_bs, s_br, s_cs, s_cr, s_gs, s_gr, s_rs, s_rr, s_ds, s_dr,
         s_kvs, s_kvr, s_wa, s_ps, s_wm, s_in, s_out, s_ko, s_es, s_er, s_sm,
         s_xs, s_xr, s_us, s_ur, s_ls, s_lr, s_ys, s_yr, s_sync):
    n_ho, n_tp, L, T, D, G, hd, F = cfg
    TS = T // 2
    HS = TS // 2
    BR = TS // n_tp
    DH = D // 2
    NS = 8 * L
    NT4 = EX.shape[1]
    DQ = D // n_ho
    OQ = G * hd // n_ho
    OC = OQ // 3
    scale = hd ** -0.5
    j = lax.axis_index('ho')
    tp = lax.axis_index('tp')
    X = lax.div(tp, CORES)
    c = lax.rem(tp, CORES)
    Q = CHIPS - 1 - X
    V = X + 1 - 2 * lax.rem(X, 2)
    O = CHIPS - 1 - V
    near = (Q, V)

    def pos(Y):
        return 2 * lax.rem(lax.div(Y + 1, 2), 2) + lax.div(Y, 2)

    pX, pQ, pV, pO = pos(X), pos(Q), pos(V), pos(O)
    pN = (pQ, pV)
    hp = lax.div(pX, 2)
    to_near = ({'tp': Q * CORES + c}, {'tp': V * CORES + c})
    to_partner = {'tp': X * CORES + (1 - c)}
    up = lax.rem(j + 1, n_ho)
    down = lax.rem(j + n_ho - 1, n_ho)

    def rc(src, dst, ss, rs, dev):
        return pltpu.make_async_remote_copy(src_ref=src, dst_ref=dst, send_sem=ss, recv_sem=rs,
                                            device_id=dev, device_id_type=MESH)

    def lc(src, dst, sem):
        return pltpu.make_async_copy(src, dst, sem)

    def rows_of(p):
        return pl.ds(pl.multiple_of((p * CORES + c) * BR, BR), BR)

    def d_pr(par, h):
        return rc(PB.at[par, h, :, 1 - c], PR.at[par, h], s_prs.at[par, h], s_prr.at[par, h], to_partner)

    def d_pr_home(par, h):
        return rc(PB.at[par, h, pl.ds(hp * 2, 2), 1 - c], PR.at[par, h, pl.ds(hp * 2, 2)],
                  s_prs.at[par, h], s_prr.at[par, h], to_partner)

    def d_a(par, e, heavy=False):
        return rc(PB.at[par, e, pO, c], AR.at[par, e], s_as.at[par, e], s_ar.at[par, e], to_near[0 if heavy else e])

    def d_b(par, s, e):
        return rc(PB.at[par, e, pN[e], c], BC.at[s, e, e], s_bs.at[s, e], s_br.at[s, e], to_near[e])

    def d_c(par, s, e):
        return rc(PB.at[par, 1 - e, pN[e], c], BC.at[s, e, 1 - e], s_cs.at[s, e], s_cr.at[s, e], to_near[e])

    def h_part(s, p, half):
        return H.at[s, rows_of(p), pl.ds(half * DH, DH)]

    def d_g(s, e, half):
        return rc(h_part(s, pX, half), h_part(s, pX, half), s_gs.at[s, e, half], s_gr.at[s, e, half], to_near[e])

    def d_r(s, e):
        return rc(h_part(s, pN[e], e), h_part(s, pN[e], e), s_rs.at[s, e], s_rr.at[s, e], to_near[1 - e])

    def d_d(s, p):
        return rc(H.at[s, rows_of(p)], H.at[s, rows_of(p)], s_ds.at[s], s_dr.at[s], to_partner)

    def d_d_all(s, blocks):
        return rc(H.at[s, pl.ds(0, blocks * BR)], H.at[s, pl.ds(0, blocks * BR)], s_ds.at[s], s_dr.at[s], to_partner)

    def quarter(s):
        return pl.ds(pl.multiple_of(s * HS, HS), HS)

    def d_kv(l, f, pr, s, dev):
        return rc(KV.at[f, :, quarter(s)], KVR.at[l, pr, :, quarter(s)], s_kvs.at[f], s_kvr.at[l, pr], dev)

    def d_kv_all(l, f, pr):
        return rc(KV.at[f], KVR.at[l, pr, :, pl.ds(0, T)], s_kvs.at[f], s_kvr.at[l, pr], to_partner)

    E_OUT, E_IN0, E_A, E_IN1, E_B, E_IN2, E_C, E_IN3 = range(8)

    def d_e(step):
        src, dst, dev = ((E_OUT, E_IN0, to_partner), (E_A, E_IN1, to_near[1]), (E_B, E_IN2, to_near[0]),
                         (E_C, E_IN3, to_partner))[step]
        return rc(EX.at[src], EX.at[dst], s_es.at[step], s_er.at[step], dev)

    def cache_copy(l, pr):
        return lc(ZB.at[pr, pl.ds(0, T + 1)], (cb if pr else ca).at[pl.ds(l * (T + 1), T + 1)], s_ko.at[pr])

    def piece(l, k, wide, r):
        par = lax.rem(l, 2)
        if wide:
            return WQF.at[par, k, pl.ds(pl.multiple_of(r * DQ, DQ), DQ), :]
        return WOF.at[par, pl.ds(pl.multiple_of(r * OQ + (k - (G + 2)) * OC, OC), OC), :]

    def fetched(k, wide):
        return XSQ.at[k] if wide else XSO.at[k - (G + 2)]

    def d_fetch(l, k, wide):
        if wide:
            src = wq.at[l, k, pl.ds(pl.multiple_of(j * DQ, DQ), DQ), :]
        else:
            src = wo.at[l, pl.ds(pl.multiple_of(j * OQ + (k - (G + 2)) * OC, OC), OC), :]
        return lc(src, fetched(k, wide), s_ps.at[k])

    def d_x(l, k, wide):
        return rc(fetched(k, wide), piece(l, k, wide, j), s_xs.at[k], s_xr.at[k], to_near[1])

    def d_up(l, k, wide, r):
        return rc(piece(l, k, wide, r), piece(l, k, wide, r), s_us.at[k], s_ur.at[k], {'ho': up})

    def d_down(l, k, wide, r):
        return rc(piece(l, k, wide, r), piece(l, k, wide, r), s_ls.at[k], s_lr.at[k], {'ho': down})

    def d_on(l, k, wide, r, dev):
        return rc(piece(l, k, wide, r), piece(l, k, wide, r), s_ys.at[k], s_yr.at[k], dev)

    def wa_copies(l):
        out = [lc(wq.at[l, i], WQ.at[:, pl.ds(i * hd, hd)], s_wa.at[i]) for i in range(G + 2)]
        return out + [lc(wo.at[l], WO, s_wa.at[G + 2])]

    def wm_copies(l):
        return [lc(src.at[l], dst, s_wm.at[i]) for i, (src, dst) in enumerate(((wg, WG), (wu, WU), (wd, WD)))]

    def prompt_copies(s):
        return [lc(p.at[j, pl.ds(s * HS, HS)], H.at[s, pl.ds(i * HS, HS)], s_in.at[s, i]) for i, p in enumerate((pa, pb))]

    def out_copies(s):
        return [lc(H.at[s, pl.ds(i * HS, HS)], o.at[pl.ds(s * HS, HS)], s_out.at[s, i]) for i, o in enumerate((oa, ob))]

    small = [lc(src, dst, s_sm.at[i])
             for i, (src, dst) in enumerate(((g1h, g1), (g2h, g2), (fa, FT.at[0]), (fb, FT.at[1])))]

    barrier = pltpu.get_barrier_semaphore()
    met = [to_partner, to_near[0], to_near[1], {'ho': up}, {'ho': down},
           {'ho': up, 'tp': V * CORES + c}, {'ho': down, 'tp': V * CORES + c}]
    for dev in met:
        pl.semaphore_signal(barrier, inc=1, device_id=dev, device_id_type=MESH)

    for w in prompt_copies(0) + small + [d_fetch(1, k, True) for k in range(3)] + wa_copies(0):
        w.start()

    def normed(xf, gain):
        ms = jnp.mean(xf * xf, axis=-1, keepdims=True)
        return xf * lax.rsqrt(ms + 1e-5) * gain

    def decode_norm(gain):
        h = normed(DY[...], gain)
        H[STREAMS - 1, TS:TS + DEC, :] = jnp.concatenate([h, jnp.zeros_like(h)], axis=0).astype(BF16)

    for w in small:
        w.wait()
    DY[...] = jnp.zeros(DY.shape, F32)
    for i in BOTH:
        DY[i:i + 1, :] = FT[i].astype(F32)
    decode_norm(g1[0:1, :])
    pl.semaphore_wait(barrier, len(met))

    def slot(it, _):
        n = it - 1
        m1, m2, m3, mc = n - 1, n - 2, n - 3, n + 1

        def state(m):
            live = jnp.logical_and(m >= 0, m < NS)
            r = lax.rem(m + 16, 8)
            full_rs = jnp.logical_or(m < 8, r >= 4)
            full_ag = jnp.logical_or(r < 4, m >= NS - STREAMS)
            return live, full_rs, full_ag

        def when(*conds):
            out = conds[0]
            for x in conds[1:]:
                out = jnp.logical_and(out, x)
            return pl.when(out)

        live_n, frs_n, _ = state(n)
        live_1, frs_1, fag_1 = state(m1)
        live_2, _, fag_2 = state(m2)
        live_3, _, fag_3 = state(m3)
        live_c, frs_c, _ = state(mc)
        heavy = jnp.logical_and(n >= 0, n < STREAMS)
        par_n, par_1 = lax.rem(n + 8, 2), lax.rem(m1 + 8, 2)
        s_n, s_1, s_2, s_3 = (lax.rem(m + 8, STREAMS) for m in (n, m1, m2, m3))

        def pieces(t, fn, first=0):
            r = lax.rem(t + 8, 8)

            @when(t == first)
            def _():
                for k in range(3):
                    fn(1, k, True)

            @when(t >= 0, r == 0, lax.div(t, 8) + 1 < L)
            def _():
                for k in (3, 4):
                    fn(lax.div(t, 8) + 1, k, True)

            @when(t >= 0, r >= 1, r <= 3, lax.div(t, 8) + 1 < L)
            def _():
                fn(lax.div(t, 8) + 1, 4 + r, False)

            @when(t >= 0, r >= 5, lax.div(t, 8) + 2 < L)
            def _():
                fn(lax.div(t, 8) + 2, r - 5, True)

        def by_parity(k, even, odd):
            if isinstance(k, int):
                (odd if k % 2 else even)()
            else:
                when(lax.rem(k, 2) == 0)(even)
                when(lax.rem(k, 2) == 1)(odd)

        def arrived(l, k, wide):
            opposite = lax.rem(j + 2, n_ho)
            d_on(l, k, wide, opposite, {'ho': up}).wait_recv()
            d_on(l, k, wide, opposite, {'ho': up}).wait_send()

        def pass_on(l, k, wide):
            d_up(l, k, wide, j).wait_recv()
            d_down(l, k, wide, j).wait_recv()
            by_parity(k, lambda: d_on(l, k, wide, down, {'ho': up}).start(),
                      lambda: d_on(l, k, wide, up, {'ho': down}).start())
            d_up(l, k, wide, j).wait_send()
            d_down(l, k, wide, j).wait_send()

        def spread(l, k, wide):
            d_x(l, k, wide).wait_recv()
            d_up(l, k, wide, j).start()
            d_down(l, k, wide, j).start()
            d_x(l, k, wide).wait_send()

        def send_over(l, k, wide):
            d_fetch(l, k, wide).wait()
            d_x(l, k, wide).start()

        pieces(n, send_over, -1)
        pieces(n + 1, lambda l, k, wide: d_fetch(l, k, wide).start(), -1)

        def add(h, p):
            PB[par_n, h, p, c] = PB[par_n, h, p, c] + PR[par_n, h, p]

        @when(live_n, frs_n)
        def _():
            for h in BOTH:
                d_pr(par_n, h).wait_recv()
            for e in BOTH:
                add(e, pO)

            @when(jnp.logical_not(heavy))
            def _():
                for e in BOTH:
                    d_a(par_n, e).start()
                for e in BOTH:
                    add(e, pN[e])
                for e in BOTH:
                    d_b(par_n, s_n, e).start()
                for e in BOTH:
                    add(1 - e, pN[e])

            @when(heavy)
            def _():
                for e in BOTH:
                    d_a(par_n, e, True).start()
                for e in BOTH:
                    add(e, pQ)
                d_b(par_n, s_n, 0).start()
                d_c(par_n, s_n, 0).start()
                for e in BOTH:
                    add(e, pV)

            for e in BOTH:
                add(e, pX)

        @when(live_n, jnp.logical_not(frs_n))
        def _():
            for h in BOTH:
                d_pr_home(par_n, h).wait_recv()
            for h in BOTH:
                add(h, pQ)
            d_b(par_n, s_n, 0).start()
            d_c(par_n, s_n, 0).start()
            for h in BOTH:
                add(h, pX)

        @when(live_1)
        def _():
            l = lax.div(m1, 8)
            is_attn = lax.rem(lax.div(m1, 4), 2) == 0
            last = m1 >= NS - STREAMS
            d_b(par_1, s_1, 0).wait_recv()
            d_c(par_1, s_1, 0).wait_recv()

            @when(frs_1)
            def _():
                d_b(par_1, s_1, 1).wait_recv()
                d_c(par_1, s_1, 1).wait_recv()

            x_new = []
            ms = jnp.zeros((BR, 1), F32)
            for h in BOTH:
                second = jnp.where(frs_1, BC[s_1, 1, h].astype(F32), 0.0)
                total = PB[par_1, h, pX, c].astype(F32) + (BC[s_1, 0, h].astype(F32) + second)
                cols = slice(h * DH, (h + 1) * DH)
                x = XR[s_1, :, cols].astype(F32) + total.astype(BF16).astype(F32)
                x = x.astype(BF16)
                XR[s_1, :, cols] = x
                x = x.astype(F32)
                ms = ms + jnp.sum(x * x, axis=-1, keepdims=True)
                x_new.append(x)
            inv = lax.rsqrt(ms * (1.0 / D) + 1e-5)
            nl = jnp.minimum(l + 1, L - 1)
            for h in BOTH:
                cols = slice(h * DH, (h + 1) * DH)
                gain = jnp.where(is_attn, g2[pl.ds(l, 1), cols], g1[pl.ds(nl, 1), cols])
                hn = x_new[h] * inv * gain
                H[s_1, rows_of(pX), cols] = jnp.where(last, x_new[h], hn).astype(BF16)

            d_g(s_1, 0, 0).start()

            @when(fag_1)
            def _():
                d_g(s_1, 1, 1).start()

            d_g(s_1, 0, 1).start()

            @when(fag_1)
            def _():
                d_g(s_1, 1, 0).start()

            d_d(s_1, pX).start()

        @when(live_1)
        def _():
            d_b(par_1, s_1, 0).wait_send()
            d_c(par_1, s_1, 0).wait_send()

            @when(frs_1)
            def _():
                for h in BOTH:
                    d_pr(par_1, h).wait_send()
                for e in BOTH:
                    d_a(par_1, e).wait_send()
                d_b(par_1, s_1, 1).wait_send()
                d_c(par_1, s_1, 1).wait_send()

            @when(jnp.logical_not(frs_1))
            def _():
                for h in BOTH:
                    d_pr_home(par_1, h).wait_send()

        for full, blocks in ((True, CHIPS), (False, CHIPS // 2)):
            @when(live_3, fag_3 if full else jnp.logical_not(fag_3))
            def _():
                d_d_all(s_3, blocks).wait_recv()
                d_d_all(s_3, blocks).wait_send()

        for s in range(STREAMS):
            @when(m3 == NS - STREAMS + s)
            def _():
                for w in out_copies(s):
                    w.start()

        pieces(n - 4, arrived)
        pieces(n - 1, spread)

        @when(n == 0)
        def _():
            def zero(l, _):
                for pr in BOTH:
                    for kv in BOTH:
                        KVR[l, pr, kv, T:T + PAD, :] = jnp.zeros((PAD, hd), BF16)
                return 0

            lax.fori_loop(0, L, zero, 0)

        r8 = lax.rem(mc, 8)
        rows8 = lax.broadcasted_iota(jnp.int32, (8, hd), 0)

        def half_cols(half, k):
            return pl.ds(pl.multiple_of(half * DH + k * hd, hd), hd)

        def decode_send():
            for slot_, half in ((E_OUT, 1 - c), (E_A, c)):
                for t in range(NT4):
                    acc = DP[:, half_cols(half, 4 * t)]
                    for q in range(1, 4):
                        acc = acc + pltpu.roll(DP[:, half_cols(half, 4 * t + q)], 2 * q, axis=0)
                    EX[slot_, t] = acc
            d_e(0).start()

        def sum_cores():
            d_e(0).wait_recv()
            d_e(0).wait_send()
            EX[E_A] = EX[E_A] + EX[E_IN0]
            d_e(1).start()

        def sum_pair():
            d_e(1).wait_recv()
            d_e(1).wait_send()
            EX[E_B] = EX[E_A] + EX[E_IN1]
            d_e(2).start()

        def sum_all():
            d_e(2).wait_recv()
            d_e(2).wait_send()
            EX[E_C] = EX[E_B] + EX[E_IN2]
            d_e(3).start()

        def decode_update():
            d_e(3).wait_recv()
            d_e(3).wait_send()
            for slot_, half in ((E_C, c), (E_IN3, 1 - c)):
                for t in range(NT4):
                    block = EX[slot_, t]
                    for q in range(4):
                        part = block if q == 0 else pltpu.roll(block, 8 - 2 * q, axis=0)
                        cols = half_cols(half, 4 * t + q)
                        DY[:, cols] = DY[:, cols] + jnp.where(rows8 < 2, part, 0.0)
            lq = lax.div(mc, 8)

            @when(r8 == 7)
            def _():
                decode_norm(g2[pl.ds(lq, 1), :])

            @when(r8 == 3, mc < NS)
            def _():
                decode_norm(g1[pl.ds(jnp.minimum(lq, L - 1), 1), :])

        when(r8 == 0, mc > 0)(sum_cores)
        when(jnp.logical_or(r8 == 7, jnp.logical_and(r8 == 3, mc > 8)))(decode_update)

        par_c = lax.rem(mc, 2)
        sc = lax.rem(mc, STREAMS)
        lq_c = jnp.minimum(lax.div(mc, 8), L - 1)
        attn_c = jnp.logical_and(live_c, r8 < 4)
        mlp_c = jnp.logical_and(live_c, r8 >= 4)

        for s in range(STREAMS):
            @when(mc == s)
            def _():
                for w in prompt_copies(s):
                    w.wait()

                def first_rows(i, _):
                    rows = pl.ds(pl.multiple_of(i * BR, BR), BR)
                    hn = normed(H[s, rows, :].astype(F32), g1[0:1, :])
                    H[s, rows, :] = hn.astype(BF16)
                    return 0

                XR[s] = H[s, rows_of(pX), :]
                lax.fori_loop(0, n_tp, first_rows, 0)

        NQKV = (G + 2) * hd

        def qkv_tiles(fn):
            c0 = 0
            while c0 < NQKV:
                c1 = min(c0 + 2 * hd, NQKV)
                fn(c0, c1)
                c0 = c1

        @when(attn_c)
        def _():
            @when(sc == 0)
            def _():
                for w in wa_copies(lq_c)[:-1]:
                    w.wait()

                @when(mc == 0)
                def _():
                    for s in range(1, STREAMS):
                        for w in prompt_copies(s):
                            w.start()
                    for w in wm_copies(0):
                        w.start()

            @when(mc < 8)
            def _():
                def go(c0, c1):
                    QS[:, c0:c1] = jnp.dot(H[sc], WQ[:, c0:c1], preferred_element_type=F32).astype(BF16)

                qkv_tiles(go)

            @when(mc >= 8)
            def _():
                home = pl.ds(pl.multiple_of(hp * HS, HS), HS)
                lpar = lax.rem(lq_c, 2)

                def go(c0, c1):
                    other = jnp.concatenate([WQF[lpar, i] for i in range(c0 // hd, c1 // hd)], axis=1)
                    for f, w in enumerate((WQ[:, c0:c1], other)):
                        QS[f * HS:(f + 1) * HS, c0:c1] = jnp.dot(
                            H[sc, home, :], w, preferred_element_type=F32).astype(BF16)

                qkv_tiles(go)

                @when(sc == STREAMS - 1)
                def _():
                    def dec(c0, c1):
                        QS[TS:TS + DEC, c0:c1] = jnp.dot(
                            H[STREAMS - 1, TS:TS + DEC, :], WQ[:, c0:c1], preferred_element_type=F32).astype(BF16)

                    qkv_tiles(dec)

            for f in BOTH:
                for kv in BOTH:
                    KV[f, kv, quarter(sc), :] = QS[f * HS:(f + 1) * HS, (G + kv) * hd:(G + kv + 1) * hd]

            @when(mc < 8)
            def _():
                for f in BOTH:
                    d_kv(lq_c, f, f, sc, {'ho': up}).start()

            @when(mc >= 8)
            def _():
                d_kv(lq_c, 0, hp, sc, {'ho': up}).start()
                d_kv(lq_c, 1, hp, sc, {'ho': up, 'tp': V * CORES + c}).start()

            for s in range(STREAMS):
                @when(sc == s)
                def _():
                    keys = (s + 1) * HS

                    def attn_tile(i, _):
                        g = lax.div(i, CORES)
                        f = lax.rem(i, CORES)
                        rows = pl.ds(pl.multiple_of(f * HS, HS), HS)
                        cols = pl.ds(pl.multiple_of(g * hd, hd), hd)
                        scores = lax.dot_general(QS[rows, cols], KV[f, 0, 0:keys, :], (((1,), (1,)), ((), ())),
                                                 preferred_element_type=F32) * scale
                        qpos = s * HS + lax.broadcasted_iota(jnp.int32, (HS, keys), 0)
                        kpos = lax.broadcasted_iota(jnp.int32, (HS, keys), 1)
                        scores = jnp.where(qpos >= kpos, scores, -1e30)
                        e = jnp.exp(scores - jnp.max(scores, axis=-1, keepdims=True))
                        p = (e / jnp.sum(e, axis=-1, keepdims=True)).astype(BF16)
                        OS[rows, cols] = jnp.dot(p, KV[f, 1, 0:keys, :], preferred_element_type=F32).astype(BF16)
                        return 0

                    lax.fori_loop(0, CORES * G, attn_tile, 0)

        UT, NT = tile_of(F, 256), tile_of(DH, 512)

        @when(mlp_c)
        def _():
            @when(sc == 0)
            def _():
                for w in wm_copies(lq_c):
                    w.wait()

            def gate_up(i, _):
                cols = pl.ds(pl.multiple_of(i * UT, UT), UT)
                gate = jnp.dot(H[sc], WG[:, cols], preferred_element_type=F32)
                up_ = jnp.dot(H[sc], WU[:, cols], preferred_element_type=F32)
                US[:, cols] = (gate * (1.0 / (1.0 + jnp.exp(-gate))) * up_).astype(BF16)
                return 0

            lax.fori_loop(0, F // UT, gate_up, 0)

        @when(live_n, frs_n, jnp.logical_not(heavy))
        def _():
            for e in BOTH:
                d_a(par_n, e).wait_recv()
                PB[par_n, e, pN[1 - e], c] = PB[par_n, e, pN[1 - e], c] + AR[par_n, e]
            for e in BOTH:
                d_c(par_n, s_n, 1 - e).start()

        @when(heavy)
        def _():
            for e in BOTH:
                d_a(par_n, e, True).wait_recv()
                PB[par_n, e, pV, c] = PB[par_n, e, pV, c] + AR[par_n, e]
            d_c(par_n, s_n, 1).start()
            d_b(par_n, s_n, 1).start()

        @when(live_c, r8 == 4)
        def _():
            for pr in BOTH:
                d_kv_all(lq_c, pr, pr).wait_send()
            for pr in BOTH:
                d_kv_all(lq_c, pr, pr).wait_recv()
            rows = lax.broadcasted_iota(jnp.int32, (DEC, hd), 0)
            outs = []
            for pr in BOTH:
                @when(lq_c > 0)
                def _():
                    cache_copy(lq_c - 1, pr).wait()

                both = jnp.zeros((DEC, hd), F32)
                for kv in BOTH:
                    new = QS[TS:TS + DEC, (G + kv) * hd:(G + kv + 1) * hd].astype(F32)
                    new = jnp.sum(jnp.where(rows == pr, new, 0.0), axis=0, keepdims=True)
                    KVR[lq_c, pr, kv, T:T + DEC, :] = jnp.where(rows == 0, new, 0.0).astype(BF16)
                    both = jnp.where(rows == kv, new, both)
                    Z32[pl.ds(kv, T, stride=2), :] = KVR[lq_c, pr, kv, 0:T, :].astype(F32)
                ZB[pr, 0:T] = Z32[...].astype(BF16).reshape(T, 2, hd)
                ZB[pr, T:T + DEC // 2] = both.astype(BF16).reshape(DEC // 2, 2, hd)
                cache_copy(lq_c, pr).start()
                q = jnp.concatenate([QS[TS:TS + DEC, g * hd:(g + 1) * hd] for g in range(G)], axis=0)
                scores = lax.dot_general(q, KVR[lq_c, pr, 0], (((1,), (1,)), ((), ())), preferred_element_type=F32) * scale
                kpos = lax.broadcasted_iota(jnp.int32, (G * DEC, T + PAD), 1)
                scores = jnp.where(kpos <= T, scores, -1e30)
                e = jnp.exp(scores - jnp.max(scores, axis=-1, keepdims=True))
                p = (e / jnp.sum(e, axis=-1, keepdims=True)).astype(BF16)
                outs.append(jnp.dot(p, KVR[lq_c, pr, 1], preferred_element_type=F32))
            picked = []
            for g in range(G):
                rest = jnp.where(rows == 1, outs[1][g * DEC:(g + 1) * DEC], 0.0)
                picked.append(jnp.where(rows == 0, outs[0][g * DEC:(g + 1) * DEC], rest).astype(BF16))
            od = jnp.concatenate(picked, axis=1)

            for t in range(D // NT):
                part = jnp.dot(od, WO[:, t * NT:(t + 1) * NT], preferred_element_type=F32)
                DP[:, t * NT:(t + 1) * NT] = part[0:8]
            decode_send()

            @when(lax.div(mc, 8) + 1 < L)
            def _():
                for w in wa_copies(lax.div(mc, 8) + 1):
                    w.start()

        when(r8 == 1, mc > 8)(sum_pair)
        when(r8 == 2, mc > 8)(sum_all)

        @when(live_2)
        def _():
            d_g(s_2, 0, 1).wait_recv()

            @when(jnp.logical_not(fag_2))
            def _():
                d_g(s_2, 0, 0).wait_recv()

            d_d(s_2, pQ).start()

            @when(fag_2)
            def _():
                d_g(s_2, 1, 0).wait_recv()
                d_d(s_2, pV).start()
                for e in BOTH:
                    d_r(s_2, e).wait_recv()
                d_d(s_2, pO).start()
                for half in BOTH:
                    d_g(s_2, 1, half).wait_send()
                for e in BOTH:
                    d_r(s_2, e).wait_send()

            for half in BOTH:
                d_g(s_2, 0, half).wait_send()


        def at_cols(t):
            return pl.ds(pl.multiple_of(t * NT, NT), NT)

        @when(attn_c, sc == 0)
        def _():
            wa_copies(lq_c)[-1].wait()

        @when(attn_c, mc < 8)
        def _():
            for h in BOTH:
                def out_tile(t, _):
                    cols = pl.ds(pl.multiple_of(h * DH + t * NT, NT), NT)
                    val = jnp.dot(OS[...], WO[:, cols], preferred_element_type=F32)
                    PB[par_c, h, :, :, :, at_cols(t)] = val.astype(BF16).reshape(CHIPS, CORES, BR, NT)
                    return 0

                lax.fori_loop(0, DH // NT, out_tile, 0)
                d_pr(par_c, h).start()

        @when(attn_c, mc >= 8)
        def _():
            for h in BOTH:
                def out_tile(t, _):
                    cols = pl.ds(pl.multiple_of(h * DH + t * NT, NT), NT)
                    val = jnp.dot(OS[0:HS, :], WO[:, cols], preferred_element_type=F32)
                    val = val + jnp.dot(OS[HS:TS, :], WOF[lax.rem(lq_c, 2), :, cols], preferred_element_type=F32)
                    PB[par_c, h, pl.ds(hp * 2, 2), :, :, at_cols(t)] = val.astype(BF16).reshape(2, CORES, BR, NT)
                    return 0

                lax.fori_loop(0, DH // NT, out_tile, 0)
                d_pr_home(par_c, h).start()

        @when(mlp_c)
        def _():
            for h in BOTH:
                def down_tile(t, _):
                    cols = pl.ds(pl.multiple_of(h * DH + t * NT, NT), NT)
                    val = jnp.dot(US[...], WD[:, cols], preferred_element_type=F32)
                    PB[par_c, h, :, :, :, at_cols(t)] = val[0:TS].astype(BF16).reshape(CHIPS, CORES, BR, NT)
                    DP[:, cols] = val[TS:TS + 8]
                    return 0

                lax.fori_loop(0, DH // NT, down_tile, 0)
                d_pr(par_c, h).start()

        @when(n < NS + 2)
        def _():
            for e in BOTH:
                pl.semaphore_signal(s_sync.at[e], inc=1, device_id=to_near[e], device_id_type=MESH)

        @when(live_1, fag_1)
        def _():
            for e in BOTH:
                d_g(s_1, e, e).wait_recv()
                d_r(s_1, e).start()

        when(r8 == 4)(sum_cores)
        when(r8 == 5)(sum_pair)
        when(r8 == 6)(sum_all)

        @when(live_c, r8 == 7)
        def _():
            decode_send()

            @when(lax.div(mc, 8) + 1 < L)
            def _():
                for w in wm_copies(lax.div(mc, 8) + 1):
                    w.start()

        pieces(n - 2, pass_on)

        @when(n >= 0)
        def _():
            for e in BOTH:
                pl.semaphore_wait(s_sync.at[e], 1)

        return 0

    lax.fori_loop(0, NS + 4, slot, 0)

    for i, ref in enumerate((fin_a, fin_b)):
        ref[...] = DY[i:i + 1, :]
    for pr in BOTH:
        cache_copy(L - 1, pr).wait()
    for s in range(STREAMS):
        for w in out_copies(s):
            w.wait()


def device_specs():
    row, whole, last = P(('pairs', 'ho')), P(), P(None, None, 'tp')
    in_specs = (P('pairs'), P('pairs'), row, row, last, P(None, 'tp'), last, last, P(None, 'tp'), whole, whole)
    cache = P(('pairs', 'ho'), None, None, None, 'tp')
    out_specs = (row, row, row, row, cache, cache)
    return in_specs, out_specs


def solution(mesh):
    n_ho, n_tp = mesh.shape['ho'], mesh.shape['tp']
    in_specs, out_specs = device_specs()

    def per_device(prompt_a, prompt_b, first_a, first_b, w_qkv, w_out, w_gate, w_up, w_down, norm_attn, norm_mlp):
        L, D = w_qkv.shape[0], w_qkv.shape[1]
        G, hd = w_out.shape[2], w_out.shape[3]
        F = w_gate.shape[2]
        T = prompt_a.shape[1]
        TS, DH = T // 2, D // 2
        BR = TS // n_tp
        wq = jnp.swapaxes(w_qkv[:, :, 0], 1, 2)
        wo = w_out.reshape(L, G * hd, D)
        any_spec = pl.BlockSpec(memory_space=pl.ANY)
        hbm_spec = pl.BlockSpec(memory_space=pltpu.HBM)
        vmem_spec = pl.BlockSpec(memory_space=pltpu.VMEM)
        dma = pltpu.SemaphoreType.DMA
        two, four, eight = (2, 2), (STREAMS,), (8,)
        by_stream = four + two[:1]
        flops = 2 * L * 2 * T * D * (wq.shape[1] * hd + G * hd + 3 * F)
        outs = pl.pallas_call(
            functools.partial(body, (n_ho, n_tp, L, T, D, G, hd, F)),
            name='serve',
            out_shape=(
                jax.ShapeDtypeStruct((T + DEC, D), BF16), jax.ShapeDtypeStruct((T + DEC, D), BF16),
                jax.ShapeDtypeStruct((1, D), F32), jax.ShapeDtypeStruct((1, D), F32),
                jax.ShapeDtypeStruct((L * (T + 1), 2, hd), BF16), jax.ShapeDtypeStruct((L * (T + 1), 2, hd), BF16)),
            in_specs=[hbm_spec] * 11,
            out_specs=(any_spec, any_spec, vmem_spec, vmem_spec, any_spec, any_spec),
            scratch_shapes=[
                pltpu.VMEM((STREAMS, TS + DEC, D), BF16),
                pltpu.VMEM((2, 2, CHIPS, CORES, BR, DH), BF16),
                pltpu.VMEM((2, 2, CHIPS, BR, DH), BF16),
                pltpu.VMEM((2, 2, BR, DH), BF16),
                pltpu.VMEM((STREAMS, 2, 2, BR, DH), BF16),
                pltpu.VMEM((STREAMS, BR, D), BF16),
                pltpu.VMEM((TS + DEC, (G + 2) * hd), BF16),
                pltpu.VMEM((2, 2, T, hd), BF16),
                pltpu.VMEM((TS, G * hd), BF16),
                pltpu.VMEM((TS + DEC, F), BF16),
                pltpu.VMEM((L, 2, 2, T + PAD, hd), BF16),
                pltpu.VMEM((D, (G + 2) * hd), BF16),
                pltpu.VMEM((G * hd, D), BF16),
                pltpu.VMEM((2, G + 2, D, hd), BF16),
                pltpu.VMEM((2, G * hd, D), BF16),
                pltpu.VMEM((G + 2, D // n_ho, hd), BF16),
                pltpu.VMEM((3, G * hd // n_ho // 3, D), BF16),
                pltpu.VMEM((D, F), BF16),
                pltpu.VMEM((D, F), BF16),
                pltpu.VMEM((F, D), BF16),
                pltpu.VMEM((L, D), F32),
                pltpu.VMEM((L, D), F32),
                pltpu.VMEM((2, 1, D), BF16),
                pltpu.VMEM((8, D), F32),
                pltpu.VMEM((8, D), F32),
                pltpu.VMEM((8, DH // (4 * hd), 8, hd), F32),
                pltpu.VMEM((2 * T, hd), F32),
                pltpu.VMEM((2, T + 8, 2, hd), BF16),
                *map(dma, (two, two, two, two)),
                *map(dma, (by_stream, by_stream, by_stream, by_stream)),
                *map(dma, (by_stream + two[:1], by_stream + two[:1], by_stream, by_stream)),
                *map(dma, (four, four)),
                *map(dma, (two[:1], (L,) + two[:1])),
                *map(dma, ((G + 3,), eight, (3,))),
                *map(dma, (by_stream, by_stream, two[:1])),
                *map(dma, (four, four, four)),
                *map(dma, (eight,) * 8),
                pltpu.SemaphoreType.REGULAR((2,)),
            ],
            compiler_params=pltpu.CompilerParams(
                collective_id=0, has_side_effects=True, vmem_limit_bytes=60 << 20),
            cost_estimate=pl.CostEstimate(flops=flops, bytes_accessed=flops // T, transcendentals=0),
        )(prompt_a, prompt_b, first_a, first_b, wq, wo, w_gate, w_up, w_down, norm_attn, norm_mlp)
        out_a, out_b, fin_a, fin_b, cache_a, cache_b = outs

        def cache(rows):
            return jnp.swapaxes(rows.reshape(L, T + 1, 2, hd), 1, 2)[None, :, :, :, None]

        return (out_a[None, :T], out_b[None, :T], fin_a, fin_b, cache(cache_a), cache(cache_b))

    return jax.shard_map(per_device, mesh=mesh, in_specs=in_specs, out_specs=out_specs, check_vma=False)
```

```python
import functools

import jax
import jax.numpy as jnp
from jax import lax
from jax.experimental import pallas as pl
from jax.experimental.pallas import tpu as pltpu
from jax.sharding import PartitionSpec as P

MESH = pl.DeviceIdType.MESH
F32 = jnp.float32
BF16 = jnp.bfloat16
CORES = 2
CHIPS = 4
BOTH = range(2)
STREAMS = 4
DEC = 16
PAD = 128


def tile_of(size, most):
    tile = most
    while size % tile:
        tile //= 2
    return tile


def body(cfg, pa, pb, fa, fb, wq, wo, wg, wu, wd, g1h, g2h, oa, ob, fin_a, fin_b, ca, cb,
         H, PB, PR, AR, BC, XR, QS, KV, OS, US, KVR, WQ, WO, WQF, WOF, XSQ, XSO, WG, WU, WD, g1, g2, FT, DY, DP, EX, Z32, ZB,
         s_prs, s_prr, s_as, s_ar, s_bs, s_br, s_cs, s_cr, s_gs, s_gr, s_rs, s_rr, s_ds, s_dr,
         s_kvs, s_kvr, s_wa, s_ps, s_wm, s_in, s_out, s_ko, s_es, s_er, s_sm,
         s_xs, s_xr, s_us, s_ur, s_ls, s_lr, s_ys, s_yr, s_sync):
    n_ho, n_tp, L, T, D, G, hd, F = cfg
    TS = T // 2
    HS = TS // 2
    BR = TS // n_tp
    DH = D // 2
    NS = 8 * L
    NT4 = EX.shape[1]
    DQ = D // n_ho
    OQ = G * hd // n_ho
    OC = OQ // 3
    scale = hd ** -0.5
    j = lax.axis_index('ho')
    tp = lax.axis_index('tp')
    X = lax.div(tp, CORES)
    c = lax.rem(tp, CORES)
    Q = CHIPS - 1 - X
    V = X + 1 - 2 * lax.rem(X, 2)
    O = CHIPS - 1 - V
    near = (Q, V)

    def pos(Y):
        return 2 * lax.rem(lax.div(Y + 1, 2), 2) + lax.div(Y, 2)

    pX, pQ, pV, pO = pos(X), pos(Q), pos(V), pos(O)
    pN = (pQ, pV)
    hp = lax.div(pX, 2)
    to_near = ({'tp': Q * CORES + c}, {'tp': V * CORES + c})
    to_partner = {'tp': X * CORES + (1 - c)}
    up = lax.rem(j + 1, n_ho)
    down = lax.rem(j + n_ho - 1, n_ho)

    def rc(src, dst, ss, rs, dev):
        return pltpu.make_async_remote_copy(src_ref=src, dst_ref=dst, send_sem=ss, recv_sem=rs,
                                            device_id=dev, device_id_type=MESH)

    def lc(src, dst, sem):
        return pltpu.make_async_copy(src, dst, sem)

    def rows_of(p):
        return pl.ds(pl.multiple_of((p * CORES + c) * BR, BR), BR)

    def d_pr(par, h):
        return rc(PB.at[par, h, :, 1 - c], PR.at[par, h], s_prs.at[par, h], s_prr.at[par, h], to_partner)

    def d_pr_home(par, h):
        return rc(PB.at[par, h, pl.ds(hp * 2, 2), 1 - c], PR.at[par, h, pl.ds(hp * 2, 2)],
                  s_prs.at[par, h], s_prr.at[par, h], to_partner)

    def d_a(par, e, heavy=False):
        return rc(PB.at[par, e, pO, c], AR.at[par, e], s_as.at[par, e], s_ar.at[par, e], to_near[0 if heavy else e])

    def d_b(par, s, e):
        return rc(PB.at[par, e, pN[e], c], BC.at[s, e, e], s_bs.at[s, e], s_br.at[s, e], to_near[e])

    def d_c(par, s, e):
        return rc(PB.at[par, 1 - e, pN[e], c], BC.at[s, e, 1 - e], s_cs.at[s, e], s_cr.at[s, e], to_near[e])

    def h_part(s, p, half):
        return H.at[s, rows_of(p), pl.ds(half * DH, DH)]

    def d_g(s, e, half):
        return rc(h_part(s, pX, half), h_part(s, pX, half), s_gs.at[s, e, half], s_gr.at[s, e, half], to_near[e])

    def d_r(s, e):
        return rc(h_part(s, pN[e], e), h_part(s, pN[e], e), s_rs.at[s, e], s_rr.at[s, e], to_near[1 - e])

    def d_d(s, p):
        return rc(H.at[s, rows_of(p)], H.at[s, rows_of(p)], s_ds.at[s], s_dr.at[s], to_partner)

    def d_d_all(s, blocks):
        return rc(H.at[s, pl.ds(0, blocks * BR)], H.at[s, pl.ds(0, blocks * BR)], s_ds.at[s], s_dr.at[s], to_partner)

    def quarter(s):
        return pl.ds(pl.multiple_of(s * HS, HS), HS)

    def d_kv(l, f, pr, s, dev):
        return rc(KV.at[f, :, quarter(s)], KVR.at[l, pr, :, quarter(s)], s_kvs.at[f], s_kvr.at[l, pr], dev)

    def d_kv_all(l, f, pr):
        return rc(KV.at[f], KVR.at[l, pr, :, pl.ds(0, T)], s_kvs.at[f], s_kvr.at[l, pr], to_partner)

    E_OUT, E_IN0, E_A, E_IN1, E_B, E_IN2, E_C, E_IN3 = range(8)

    def d_e(step):
        src, dst, dev = ((E_OUT, E_IN0, to_partner), (E_A, E_IN1, to_near[1]), (E_B, E_IN2, to_near[0]),
                         (E_C, E_IN3, to_partner))[step]
        return rc(EX.at[src], EX.at[dst], s_es.at[step], s_er.at[step], dev)

    def cache_copy(l, pr):
        return lc(ZB.at[pr, pl.ds(0, T + 1)], (cb if pr else ca).at[pl.ds(l * (T + 1), T + 1)], s_ko.at[pr])

    def piece(l, k, wide, r):
        par = lax.rem(l, 2)
        if wide:
            return WQF.at[par, k, pl.ds(pl.multiple_of(r * DQ, DQ), DQ), :]
        return WOF.at[par, pl.ds(pl.multiple_of(r * OQ + (k - (G + 2)) * OC, OC), OC), :]

    def fetched(k, wide):
        return XSQ.at[k] if wide else XSO.at[k - (G + 2)]

    def d_fetch(l, k, wide):
        if wide:
            src = wq.at[l, k, pl.ds(pl.multiple_of(j * DQ, DQ), DQ), :]
        else:
            src = wo.at[l, pl.ds(pl.multiple_of(j * OQ + (k - (G + 2)) * OC, OC), OC), :]
        return lc(src, fetched(k, wide), s_ps.at[k])

    def d_x(l, k, wide):
        return rc(fetched(k, wide), piece(l, k, wide, j), s_xs.at[k], s_xr.at[k], to_near[1])

    def d_up(l, k, wide, r):
        return rc(piece(l, k, wide, r), piece(l, k, wide, r), s_us.at[k], s_ur.at[k], {'ho': up})

    def d_down(l, k, wide, r):
        return rc(piece(l, k, wide, r), piece(l, k, wide, r), s_ls.at[k], s_lr.at[k], {'ho': down})

    def d_on(l, k, wide, r, dev):
        return rc(piece(l, k, wide, r), piece(l, k, wide, r), s_ys.at[k], s_yr.at[k], dev)

    def wa_copies(l):
        out = [lc(wq.at[l, i], WQ.at[:, pl.ds(i * hd, hd)], s_wa.at[i]) for i in range(G + 2)]
        return out + [lc(wo.at[l], WO, s_wa.at[G + 2])]

    def wm_copies(l):
        return [lc(src.at[l], dst, s_wm.at[i]) for i, (src, dst) in enumerate(((wg, WG), (wu, WU), (wd, WD)))]

    def prompt_copies(s):
        return [lc(p.at[j, pl.ds(s * HS, HS)], H.at[s, pl.ds(i * HS, HS)], s_in.at[s, i]) for i, p in enumerate((pa, pb))]

    def out_copies(s):
        return [lc(H.at[s, pl.ds(i * HS, HS)], o.at[pl.ds(s * HS, HS)], s_out.at[s, i]) for i, o in enumerate((oa, ob))]

    small = [lc(src, dst, s_sm.at[i])
             for i, (src, dst) in enumerate(((g1h, g1), (g2h, g2), (fa, FT.at[0]), (fb, FT.at[1])))]

    barrier = pltpu.get_barrier_semaphore()
    met = [to_partner, to_near[0], to_near[1], {'ho': up}, {'ho': down},
           {'ho': up, 'tp': V * CORES + c}, {'ho': down, 'tp': V * CORES + c}]
    for dev in met:
        pl.semaphore_signal(barrier, inc=1, device_id=dev, device_id_type=MESH)

    for w in prompt_copies(0) + small + [d_fetch(1, k, True) for k in range(3)] + wa_copies(0):
        w.start()

    def normed(xf, gain):
        ms = jnp.mean(xf * xf, axis=-1, keepdims=True)
        return xf * lax.rsqrt(ms + 1e-5) * gain

    def decode_norm(gain):
        h = normed(DY[...], gain)
        H[STREAMS - 1, TS:TS + DEC, :] = jnp.concatenate([h, jnp.zeros_like(h)], axis=0).astype(BF16)

    for w in small:
        w.wait()
    DY[...] = jnp.zeros(DY.shape, F32)
    for i in BOTH:
        DY[i:i + 1, :] = FT[i].astype(F32)
    decode_norm(g1[0:1, :])
    pl.semaphore_wait(barrier, len(met))

    def slot(it, _):
        n = it - 1
        m1, m2, m3, mc = n - 1, n - 2, n - 3, n + 1

        def state(m):
            live = jnp.logical_and(m >= 0, m < NS)
            r = lax.rem(m + 16, 8)
            full_rs = jnp.logical_or(m < 8, r >= 4)
            full_ag = jnp.logical_or(r < 4, m >= NS - STREAMS)
            return live, full_rs, full_ag

        def when(*conds):
            out = conds[0]
            for x in conds[1:]:
                out = jnp.logical_and(out, x)
            return pl.when(out)

        live_n, frs_n, _ = state(n)
        live_1, frs_1, fag_1 = state(m1)
        live_2, _, fag_2 = state(m2)
        live_3, _, fag_3 = state(m3)
        live_c, frs_c, _ = state(mc)
        heavy = jnp.logical_and(n >= 0, n < STREAMS)
        par_n, par_1 = lax.rem(n + 8, 2), lax.rem(m1 + 8, 2)
        s_n, s_1, s_2, s_3 = (lax.rem(m + 8, STREAMS) for m in (n, m1, m2, m3))

        def pieces(t, fn, first=0):
            r = lax.rem(t + 8, 8)

            @when(t == first)
            def _():
                for k in range(3):
                    fn(1, k, True)

            @when(t >= 0, r == 0, lax.div(t, 8) + 1 < L)
            def _():
                for k in (3, 4):
                    fn(lax.div(t, 8) + 1, k, True)

            @when(t >= 0, r >= 1, r <= 3, lax.div(t, 8) + 1 < L)
            def _():
                fn(lax.div(t, 8) + 1, 4 + r, False)

            @when(t >= 0, r >= 5, lax.div(t, 8) + 2 < L)
            def _():
                fn(lax.div(t, 8) + 2, r - 5, True)

        def by_parity(k, even, odd):
            if isinstance(k, int):
                (odd if k % 2 else even)()
            else:
                when(lax.rem(k, 2) == 0)(even)
                when(lax.rem(k, 2) == 1)(odd)

        def arrived(l, k, wide):
            opposite = lax.rem(j + 2, n_ho)
            d_on(l, k, wide, opposite, {'ho': up}).wait_recv()
            d_on(l, k, wide, opposite, {'ho': up}).wait_send()

        def pass_on(l, k, wide):
            d_up(l, k, wide, j).wait_recv()
            d_down(l, k, wide, j).wait_recv()
            by_parity(k, lambda: d_on(l, k, wide, down, {'ho': up}).start(),
                      lambda: d_on(l, k, wide, up, {'ho': down}).start())
            d_up(l, k, wide, j).wait_send()
            d_down(l, k, wide, j).wait_send()

        def spread(l, k, wide):
            d_x(l, k, wide).wait_recv()
            d_up(l, k, wide, j).start()
            d_down(l, k, wide, j).start()
            d_x(l, k, wide).wait_send()

        def send_over(l, k, wide):
            d_fetch(l, k, wide).wait()
            d_x(l, k, wide).start()

        pieces(n, send_over, -1)
        pieces(n + 1, lambda l, k, wide: d_fetch(l, k, wide).start(), -1)

        def add(h, p):
            PB[par_n, h, p, c] = PB[par_n, h, p, c] + PR[par_n, h, p]

        @when(live_n, frs_n)
        def _():
            for h in BOTH:
                d_pr(par_n, h).wait_recv()
            for e in BOTH:
                add(e, pO)

            @when(jnp.logical_not(heavy))
            def _():
                for e in BOTH:
                    d_a(par_n, e).start()
                for e in BOTH:
                    add(e, pN[e])
                for e in BOTH:
                    d_b(par_n, s_n, e).start()
                for e in BOTH:
                    add(1 - e, pN[e])

            @when(heavy)
            def _():
                for e in BOTH:
                    d_a(par_n, e, True).start()
                for e in BOTH:
                    add(e, pQ)
                d_b(par_n, s_n, 0).start()
                d_c(par_n, s_n, 0).start()
                for e in BOTH:
                    add(e, pV)

            for e in BOTH:
                add(e, pX)

        @when(live_n, jnp.logical_not(frs_n))
        def _():
            for h in BOTH:
                d_pr_home(par_n, h).wait_recv()
            for h in BOTH:
                add(h, pQ)
            d_b(par_n, s_n, 0).start()
            d_c(par_n, s_n, 0).start()
            for h in BOTH:
                add(h, pX)

        @when(live_1)
        def _():
            l = lax.div(m1, 8)
            is_attn = lax.rem(lax.div(m1, 4), 2) == 0
            last = m1 >= NS - STREAMS
            d_b(par_1, s_1, 0).wait_recv()
            d_c(par_1, s_1, 0).wait_recv()

            @when(frs_1)
            def _():
                d_b(par_1, s_1, 1).wait_recv()
                d_c(par_1, s_1, 1).wait_recv()

            x_new = []
            ms = jnp.zeros((BR, 1), F32)
            for h in BOTH:
                second = jnp.where(frs_1, BC[s_1, 1, h].astype(F32), 0.0)
                total = PB[par_1, h, pX, c].astype(F32) + (BC[s_1, 0, h].astype(F32) + second)
                cols = slice(h * DH, (h + 1) * DH)
                x = XR[s_1, :, cols].astype(F32) + total.astype(BF16).astype(F32)
                x = x.astype(BF16)
                XR[s_1, :, cols] = x
                x = x.astype(F32)
                ms = ms + jnp.sum(x * x, axis=-1, keepdims=True)
                x_new.append(x)
            inv = lax.rsqrt(ms * (1.0 / D) + 1e-5)
            nl = jnp.minimum(l + 1, L - 1)
            for h in BOTH:
                cols = slice(h * DH, (h + 1) * DH)
                gain = jnp.where(is_attn, g2[pl.ds(l, 1), cols], g1[pl.ds(nl, 1), cols])
                hn = x_new[h] * inv * gain
                H[s_1, rows_of(pX), cols] = jnp.where(last, x_new[h], hn).astype(BF16)

            d_g(s_1, 0, 0).start()

            @when(fag_1)
            def _():
                d_g(s_1, 1, 1).start()

            d_g(s_1, 0, 1).start()

            @when(fag_1)
            def _():
                d_g(s_1, 1, 0).start()

            d_d(s_1, pX).start()

        @when(live_1)
        def _():
            d_b(par_1, s_1, 0).wait_send()
            d_c(par_1, s_1, 0).wait_send()

            @when(frs_1)
            def _():
                for h in BOTH:
                    d_pr(par_1, h).wait_send()
                for e in BOTH:
                    d_a(par_1, e).wait_send()
                d_b(par_1, s_1, 1).wait_send()
                d_c(par_1, s_1, 1).wait_send()

            @when(jnp.logical_not(frs_1))
            def _():
                for h in BOTH:
                    d_pr_home(par_1, h).wait_send()

        for full, blocks in ((True, CHIPS), (False, CHIPS // 2)):
            @when(live_3, fag_3 if full else jnp.logical_not(fag_3))
            def _():
                d_d_all(s_3, blocks).wait_recv()
                d_d_all(s_3, blocks).wait_send()

        for s in range(STREAMS):
            @when(m3 == NS - STREAMS + s)
            def _():
                for w in out_copies(s):
                    w.start()

        pieces(n - 4, arrived)
        pieces(n - 1, spread)

        @when(n == 0)
        def _():
            def zero(l, _):
                for pr in BOTH:
                    for kv in BOTH:
                        KVR[l, pr, kv, T:T + PAD, :] = jnp.zeros((PAD, hd), BF16)
                return 0

            lax.fori_loop(0, L, zero, 0)

        r8 = lax.rem(mc, 8)
        rows8 = lax.broadcasted_iota(jnp.int32, (8, hd), 0)

        def half_cols(half, k):
            return pl.ds(pl.multiple_of(half * DH + k * hd, hd), hd)

        def decode_send():
            for slot_, half in ((E_OUT, 1 - c), (E_A, c)):
                for t in range(NT4):
                    acc = DP[:, half_cols(half, 4 * t)]
                    for q in range(1, 4):
                        acc = acc + pltpu.roll(DP[:, half_cols(half, 4 * t + q)], 2 * q, axis=0)
                    EX[slot_, t] = acc
            d_e(0).start()

        def sum_cores():
            d_e(0).wait_recv()
            d_e(0).wait_send()
            EX[E_A] = EX[E_A] + EX[E_IN0]
            d_e(1).start()

        def sum_pair():
            d_e(1).wait_recv()
            d_e(1).wait_send()
            EX[E_B] = EX[E_A] + EX[E_IN1]
            d_e(2).start()

        def sum_all():
            d_e(2).wait_recv()
            d_e(2).wait_send()
            EX[E_C] = EX[E_B] + EX[E_IN2]
            d_e(3).start()

        def decode_update():
            d_e(3).wait_recv()
            d_e(3).wait_send()
            for slot_, half in ((E_C, c), (E_IN3, 1 - c)):
                for t in range(NT4):
                    block = EX[slot_, t]
                    for q in range(4):
                        part = block if q == 0 else pltpu.roll(block, 8 - 2 * q, axis=0)
                        cols = half_cols(half, 4 * t + q)
                        DY[:, cols] = DY[:, cols] + jnp.where(rows8 < 2, part, 0.0)
            lq = lax.div(mc, 8)

            @when(r8 == 7)
            def _():
                decode_norm(g2[pl.ds(lq, 1), :])

            @when(r8 == 3, mc < NS)
            def _():
                decode_norm(g1[pl.ds(jnp.minimum(lq, L - 1), 1), :])

        when(r8 == 0, mc > 0)(sum_cores)
        when(jnp.logical_or(r8 == 7, jnp.logical_and(r8 == 3, mc > 8)))(decode_update)

        par_c = lax.rem(mc, 2)
        sc = lax.rem(mc, STREAMS)
        lq_c = jnp.minimum(lax.div(mc, 8), L - 1)
        attn_c = jnp.logical_and(live_c, r8 < 4)
        mlp_c = jnp.logical_and(live_c, r8 >= 4)

        for s in range(STREAMS):
            @when(mc == s)
            def _():
                for w in prompt_copies(s):
                    w.wait()

                def first_rows(i, _):
                    rows = pl.ds(pl.multiple_of(i * BR, BR), BR)
                    hn = normed(H[s, rows, :].astype(F32), g1[0:1, :])
                    H[s, rows, :] = hn.astype(BF16)
                    return 0

                XR[s] = H[s, rows_of(pX), :]
                lax.fori_loop(0, n_tp, first_rows, 0)

        NQKV = (G + 2) * hd

        def qkv_tiles(fn):
            c0 = 0
            while c0 < NQKV:
                c1 = min(c0 + 2 * hd, NQKV)
                fn(c0, c1)
                c0 = c1

        @when(attn_c)
        def _():
            @when(sc == 0)
            def _():
                for w in wa_copies(lq_c)[:-1]:
                    w.wait()

                @when(mc == 0)
                def _():
                    for s in range(1, STREAMS):
                        for w in prompt_copies(s):
                            w.start()
                    for w in wm_copies(0):
                        w.start()

            @when(mc < 8)
            def _():
                def go(c0, c1):
                    QS[:, c0:c1] = jnp.dot(H[sc], WQ[:, c0:c1], preferred_element_type=F32).astype(BF16)

                qkv_tiles(go)

            @when(mc >= 8)
            def _():
                home = pl.ds(pl.multiple_of(hp * HS, HS), HS)
                lpar = lax.rem(lq_c, 2)

                def go(c0, c1):
                    other = jnp.concatenate([WQF[lpar, i] for i in range(c0 // hd, c1 // hd)], axis=1)
                    for f, w in enumerate((WQ[:, c0:c1], other)):
                        QS[f * HS:(f + 1) * HS, c0:c1] = jnp.dot(
                            H[sc, home, :], w, preferred_element_type=F32).astype(BF16)

                qkv_tiles(go)

                @when(sc == STREAMS - 1)
                def _():
                    def dec(c0, c1):
                        QS[TS:TS + DEC, c0:c1] = jnp.dot(
                            H[STREAMS - 1, TS:TS + DEC, :], WQ[:, c0:c1], preferred_element_type=F32).astype(BF16)

                    qkv_tiles(dec)

            for f in BOTH:
                for kv in BOTH:
                    KV[f, kv, quarter(sc), :] = QS[f * HS:(f + 1) * HS, (G + kv) * hd:(G + kv + 1) * hd]

            @when(mc < 8)
            def _():
                for f in BOTH:
                    d_kv(lq_c, f, f, sc, {'ho': up}).start()

            @when(mc >= 8)
            def _():
                d_kv(lq_c, 0, hp, sc, {'ho': up}).start()
                d_kv(lq_c, 1, hp, sc, {'ho': up, 'tp': V * CORES + c}).start()

            for s in range(STREAMS):
                @when(sc == s)
                def _():
                    keys = (s + 1) * HS

                    def attn_tile(i, _):
                        g = lax.div(i, CORES)
                        f = lax.rem(i, CORES)
                        rows = pl.ds(pl.multiple_of(f * HS, HS), HS)
                        cols = pl.ds(pl.multiple_of(g * hd, hd), hd)
                        scores = lax.dot_general(QS[rows, cols], KV[f, 0, 0:keys, :], (((1,), (1,)), ((), ())),
                                                 preferred_element_type=F32) * scale
                        qpos = s * HS + lax.broadcasted_iota(jnp.int32, (HS, keys), 0)
                        kpos = lax.broadcasted_iota(jnp.int32, (HS, keys), 1)
                        scores = jnp.where(qpos >= kpos, scores, -1e30)
                        e = jnp.exp(scores - jnp.max(scores, axis=-1, keepdims=True))
                        p = (e / jnp.sum(e, axis=-1, keepdims=True)).astype(BF16)
                        OS[rows, cols] = jnp.dot(p, KV[f, 1, 0:keys, :], preferred_element_type=F32).astype(BF16)
                        return 0

                    lax.fori_loop(0, CORES * G, attn_tile, 0)

        rows_of_mlp = ((TS, sc < STREAMS - 1), (TS + DEC, sc == STREAMS - 1))
        UT, NT = tile_of(F, 512), tile_of(DH, 512)

        @when(mlp_c)
        def _():
            @when(sc == 0)
            def _():
                for w in wm_copies(lq_c):
                    w.wait()

            for rows, these in rows_of_mlp:
                @when(these)
                def _():
                    def gate_up(i, _):
                        cols = pl.ds(pl.multiple_of(i * UT, UT), UT)
                        gate = jnp.dot(H[sc, 0:rows], WG[:, cols], preferred_element_type=F32)
                        up_ = jnp.dot(H[sc, 0:rows], WU[:, cols], preferred_element_type=F32)
                        US[0:rows, cols] = (gate * (1.0 / (1.0 + jnp.exp(-gate))) * up_).astype(BF16)
                        return 0

                    lax.fori_loop(0, F // UT, gate_up, 0)

        @when(live_n, frs_n, jnp.logical_not(heavy))
        def _():
            for e in BOTH:
                d_a(par_n, e).wait_recv()
                PB[par_n, e, pN[1 - e], c] = PB[par_n, e, pN[1 - e], c] + AR[par_n, e]
            for e in BOTH:
                d_c(par_n, s_n, 1 - e).start()

        @when(heavy)
        def _():
            for e in BOTH:
                d_a(par_n, e, True).wait_recv()
                PB[par_n, e, pV, c] = PB[par_n, e, pV, c] + AR[par_n, e]
            d_c(par_n, s_n, 1).start()
            d_b(par_n, s_n, 1).start()

        @when(live_c, r8 == 4)
        def _():
            for pr in BOTH:
                d_kv_all(lq_c, pr, pr).wait_send()
            for pr in BOTH:
                d_kv_all(lq_c, pr, pr).wait_recv()
            rows = lax.broadcasted_iota(jnp.int32, (DEC, hd), 0)
            outs = []
            for pr in BOTH:
                @when(lq_c > 0)
                def _():
                    cache_copy(lq_c - 1, pr).wait()

                both = jnp.zeros((DEC, hd), F32)
                for kv in BOTH:
                    new = QS[TS:TS + DEC, (G + kv) * hd:(G + kv + 1) * hd].astype(F32)
                    new = jnp.sum(jnp.where(rows == pr, new, 0.0), axis=0, keepdims=True)
                    KVR[lq_c, pr, kv, T:T + DEC, :] = jnp.where(rows == 0, new, 0.0).astype(BF16)
                    both = jnp.where(rows == kv, new, both)
                    Z32[pl.ds(kv, T, stride=2), :] = KVR[lq_c, pr, kv, 0:T, :].astype(F32)
                ZB[pr, 0:T] = Z32[...].astype(BF16).reshape(T, 2, hd)
                ZB[pr, T:T + DEC // 2] = both.astype(BF16).reshape(DEC // 2, 2, hd)
                cache_copy(lq_c, pr).start()
                q = jnp.concatenate([QS[TS:TS + DEC, g * hd:(g + 1) * hd] for g in range(G)], axis=0)
                scores = lax.dot_general(q, KVR[lq_c, pr, 0], (((1,), (1,)), ((), ())), preferred_element_type=F32) * scale
                kpos = lax.broadcasted_iota(jnp.int32, (G * DEC, T + PAD), 1)
                scores = jnp.where(kpos <= T, scores, -1e30)
                e = jnp.exp(scores - jnp.max(scores, axis=-1, keepdims=True))
                p = (e / jnp.sum(e, axis=-1, keepdims=True)).astype(BF16)
                outs.append(jnp.dot(p, KVR[lq_c, pr, 1], preferred_element_type=F32))
            picked = []
            for g in range(G):
                rest = jnp.where(rows == 1, outs[1][g * DEC:(g + 1) * DEC], 0.0)
                picked.append(jnp.where(rows == 0, outs[0][g * DEC:(g + 1) * DEC], rest).astype(BF16))
            od = jnp.concatenate(picked, axis=1)

            for t in range(D // NT):
                part = jnp.dot(od, WO[:, t * NT:(t + 1) * NT], preferred_element_type=F32)
                DP[:, t * NT:(t + 1) * NT] = part[0:8]
            decode_send()

            @when(lax.div(mc, 8) + 1 < L)
            def _():
                for w in wa_copies(lax.div(mc, 8) + 1):
                    w.start()

        when(r8 == 1, mc > 8)(sum_pair)
        when(r8 == 2, mc > 8)(sum_all)

        @when(live_2)
        def _():
            d_g(s_2, 0, 1).wait_recv()

            @when(jnp.logical_not(fag_2))
            def _():
                d_g(s_2, 0, 0).wait_recv()

            d_d(s_2, pQ).start()

            @when(fag_2)
            def _():
                d_g(s_2, 1, 0).wait_recv()
                d_d(s_2, pV).start()
                for e in BOTH:
                    d_r(s_2, e).wait_recv()
                d_d(s_2, pO).start()
                for half in BOTH:
                    d_g(s_2, 1, half).wait_send()
                for e in BOTH:
                    d_r(s_2, e).wait_send()

            for half in BOTH:
                d_g(s_2, 0, half).wait_send()


        def at_cols(t):
            return pl.ds(pl.multiple_of(t * NT, NT), NT)

        @when(attn_c, sc == 0)
        def _():
            wa_copies(lq_c)[-1].wait()

        @when(attn_c, mc < 8)
        def _():
            for h in BOTH:
                def out_tile(t, _):
                    cols = pl.ds(pl.multiple_of(h * DH + t * NT, NT), NT)
                    val = jnp.dot(OS[...], WO[:, cols], preferred_element_type=F32)
                    PB[par_c, h, :, :, :, at_cols(t)] = val.astype(BF16).reshape(CHIPS, CORES, BR, NT)
                    return 0

                lax.fori_loop(0, DH // NT, out_tile, 0)
                d_pr(par_c, h).start()

        @when(attn_c, mc >= 8)
        def _():
            for h in BOTH:
                def out_tile(t, _):
                    cols = pl.ds(pl.multiple_of(h * DH + t * NT, NT), NT)
                    val = jnp.dot(OS[0:HS, :], WO[:, cols], preferred_element_type=F32)
                    val = val + jnp.dot(OS[HS:TS, :], WOF[lax.rem(lq_c, 2), :, cols], preferred_element_type=F32)
                    PB[par_c, h, pl.ds(hp * 2, 2), :, :, at_cols(t)] = val.astype(BF16).reshape(2, CORES, BR, NT)
                    return 0

                lax.fori_loop(0, DH // NT, out_tile, 0)
                d_pr_home(par_c, h).start()

        for rows, these in rows_of_mlp:
            @when(mlp_c, these)
            def _():
                for h in BOTH:
                    def down_tile(t, _):
                        cols = pl.ds(pl.multiple_of(h * DH + t * NT, NT), NT)
                        val = jnp.dot(US[0:rows, :], WD[:, cols], preferred_element_type=F32)
                        PB[par_c, h, :, :, :, at_cols(t)] = val[0:TS].astype(BF16).reshape(CHIPS, CORES, BR, NT)
                        if rows > TS:
                            DP[:, cols] = val[TS:TS + 8]
                        return 0

                    lax.fori_loop(0, DH // NT, down_tile, 0)
                    d_pr(par_c, h).start()

        @when(n < NS + 2)
        def _():
            for e in BOTH:
                pl.semaphore_signal(s_sync.at[e], inc=1, device_id=to_near[e], device_id_type=MESH)

        @when(live_1, fag_1)
        def _():
            for e in BOTH:
                d_g(s_1, e, e).wait_recv()
                d_r(s_1, e).start()

        when(r8 == 4)(sum_cores)
        when(r8 == 5)(sum_pair)
        when(r8 == 6)(sum_all)

        @when(live_c, r8 == 7)
        def _():
            decode_send()

            @when(lax.div(mc, 8) + 1 < L)
            def _():
                for w in wm_copies(lax.div(mc, 8) + 1):
                    w.start()

        pieces(n - 2, pass_on)

        @when(n >= 0)
        def _():
            for e in BOTH:
                pl.semaphore_wait(s_sync.at[e], 1)

        return 0

    lax.fori_loop(0, NS + 4, slot, 0)

    for i, ref in enumerate((fin_a, fin_b)):
        ref[...] = DY[i:i + 1, :]
    for pr in BOTH:
        cache_copy(L - 1, pr).wait()
    for s in range(STREAMS):
        for w in out_copies(s):
            w.wait()


def device_specs():
    row, whole, last = P(('pairs', 'ho')), P(), P(None, None, 'tp')
    in_specs = (P('pairs'), P('pairs'), row, row, last, P(None, 'tp'), last, last, P(None, 'tp'), whole, whole)
    cache = P(('pairs', 'ho'), None, None, None, 'tp')
    out_specs = (row, row, row, row, cache, cache)
    return in_specs, out_specs


def solution(mesh):
    n_ho, n_tp = mesh.shape['ho'], mesh.shape['tp']
    in_specs, out_specs = device_specs()

    def per_device(prompt_a, prompt_b, first_a, first_b, w_qkv, w_out, w_gate, w_up, w_down, norm_attn, norm_mlp):
        L, D = w_qkv.shape[0], w_qkv.shape[1]
        G, hd = w_out.shape[2], w_out.shape[3]
        F = w_gate.shape[2]
        T = prompt_a.shape[1]
        TS, DH = T // 2, D // 2
        BR = TS // n_tp
        wq = jnp.swapaxes(w_qkv[:, :, 0], 1, 2)
        wo = w_out.reshape(L, G * hd, D)
        any_spec = pl.BlockSpec(memory_space=pl.ANY)
        hbm_spec = pl.BlockSpec(memory_space=pltpu.HBM)
        vmem_spec = pl.BlockSpec(memory_space=pltpu.VMEM)
        dma = pltpu.SemaphoreType.DMA
        two, four, eight = (2, 2), (STREAMS,), (8,)
        by_stream = four + two[:1]
        flops = 2 * L * 2 * T * D * (wq.shape[1] * hd + G * hd + 3 * F)
        outs = pl.pallas_call(
            functools.partial(body, (n_ho, n_tp, L, T, D, G, hd, F)),
            name='serve',
            out_shape=(
                jax.ShapeDtypeStruct((T + DEC, D), BF16), jax.ShapeDtypeStruct((T + DEC, D), BF16),
                jax.ShapeDtypeStruct((1, D), F32), jax.ShapeDtypeStruct((1, D), F32),
                jax.ShapeDtypeStruct((L * (T + 1), 2, hd), BF16), jax.ShapeDtypeStruct((L * (T + 1), 2, hd), BF16)),
            in_specs=[hbm_spec] * 11,
            out_specs=(any_spec, any_spec, vmem_spec, vmem_spec, any_spec, any_spec),
            scratch_shapes=[
                pltpu.VMEM((STREAMS, TS + DEC, D), BF16),
                pltpu.VMEM((2, 2, CHIPS, CORES, BR, DH), BF16),
                pltpu.VMEM((2, 2, CHIPS, BR, DH), BF16),
                pltpu.VMEM((2, 2, BR, DH), BF16),
                pltpu.VMEM((STREAMS, 2, 2, BR, DH), BF16),
                pltpu.VMEM((STREAMS, BR, D), BF16),
                pltpu.VMEM((TS + DEC, (G + 2) * hd), BF16),
                pltpu.VMEM((2, 2, T, hd), BF16),
                pltpu.VMEM((TS, G * hd), BF16),
                pltpu.VMEM((TS + DEC, F), BF16),
                pltpu.VMEM((L, 2, 2, T + PAD, hd), BF16),
                pltpu.VMEM((D, (G + 2) * hd), BF16),
                pltpu.VMEM((G * hd, D), BF16),
                pltpu.VMEM((2, G + 2, D, hd), BF16),
                pltpu.VMEM((2, G * hd, D), BF16),
                pltpu.VMEM((G + 2, D // n_ho, hd), BF16),
                pltpu.VMEM((3, G * hd // n_ho // 3, D), BF16),
                pltpu.VMEM((D, F), BF16),
                pltpu.VMEM((D, F), BF16),
                pltpu.VMEM((F, D), BF16),
                pltpu.VMEM((L, D), F32),
                pltpu.VMEM((L, D), F32),
                pltpu.VMEM((2, 1, D), BF16),
                pltpu.VMEM((8, D), F32),
                pltpu.VMEM((8, D), F32),
                pltpu.VMEM((8, DH // (4 * hd), 8, hd), F32),
                pltpu.VMEM((2 * T, hd), F32),
                pltpu.VMEM((2, T + 8, 2, hd), BF16),
                *map(dma, (two, two, two, two)),
                *map(dma, (by_stream, by_stream, by_stream, by_stream)),
                *map(dma, (by_stream + two[:1], by_stream + two[:1], by_stream, by_stream)),
                *map(dma, (four, four)),
                *map(dma, (two[:1], (L,) + two[:1])),
                *map(dma, ((G + 3,), eight, (3,))),
                *map(dma, (by_stream, by_stream, two[:1])),
                *map(dma, (four, four, four)),
                *map(dma, (eight,) * 8),
                pltpu.SemaphoreType.REGULAR((2,)),
            ],
            compiler_params=pltpu.CompilerParams(
                collective_id=0, has_side_effects=True, vmem_limit_bytes=60 << 20),
            cost_estimate=pl.CostEstimate(flops=flops, bytes_accessed=flops // T, transcendentals=0),
        )(prompt_a, prompt_b, first_a, first_b, wq, wo, w_gate, w_up, w_down, norm_attn, norm_mlp)
        out_a, out_b, fin_a, fin_b, cache_a, cache_b = outs

        def cache(rows):
            return jnp.swapaxes(rows.reshape(L, T + 1, 2, hd), 1, 2)[None, :, :, :, None]

        return (out_a[None, :T], out_b[None, :T], fin_a, fin_b, cache(cache_a), cache(cache_b))

    return jax.shard_map(per_device, mesh=mesh, in_specs=in_specs, out_specs=out_specs, check_vma=False)
```
